32 devices in a mesh: fsdp: 8 (over z, y), model: 4 (over x, core).
Axes of the slice: x: 2, y: 2, z: 4, core: 2. Of those that a mesh axis runs over, the one named last changes fastest.
Arguments:
- x_in: bfloat16 [16, 128, 2048], P('fsdp', 'model')
- grad_out: bfloat16 [16, 128, 2048], P('fsdp', 'model')
- gain_attn: float32 [2048], replicated
- gain_mlp: float32 [2048], replicated
- w_qkv: bfloat16 [2048, 6144], P('fsdp', 'model')
- w_out: bfloat16 [2048, 2048], P('model', 'fsdp')
- w_gate: bfloat16 [2048, 8192], P('fsdp', 'model')
- w_up: bfloat16 [2048, 8192], P('fsdp', 'model')
- w_down: bfloat16 [8192, 2048], P('model', 'fsdp')
- rope_cos: float32 [128, 64], replicated
- rope_sin: float32 [128, 64], replicated
Outputs:
- output 1: bfloat16 [16, 128, 2048], P('fsdp', 'model')
- output 2: bfloat16 [16, 128, 2048], P('fsdp', 'model')
- output 3: float32 [2048], replicated
- output 4: float32 [2048], replicated
- output 5: float32 [2048, 6144], P('fsdp', 'model')
- output 6: float32 [2048, 2048], P('model', 'fsdp')
- output 7: float32 [2048, 8192], P('fsdp', 'model')
- output 8: float32 [2048, 8192], P('fsdp', 'model')
- output 9: float32 [8192, 2048], P('model', 'fsdp')
All inputs are finite; a program needn't handle non-finite values.
Results may differ from the reference program's by a relative error of at most 0.0159797.
Values are sent between devices in bfloat16 or wider.
A program may use at most 1 GiB of HBM per device.

```python
import jax
import jax.numpy as jnp
from jax import lax

BATCH = 16
SEQ_LEN = 128
D_MODEL = 2048
D_FF = 8192
HEADS = 16
KV_HEADS = 16
HEAD_DIM = 128
GROUP_SIZE = HEADS // KV_HEADS
QKV_COLS = KV_HEADS * (GROUP_SIZE + 2) * HEAD_DIM
NORM_EPS = 1e-5
ROPE_BASE = 500000.0


def rope_tables(key):
    step_key, offset_key = jax.random.split(key)
    steps = jax.random.randint(step_key, (SEQ_LEN,), 1, 4)
    offset = jax.random.randint(offset_key, (), 0, 1024)
    positions = (jnp.cumsum(steps) + offset).astype(jnp.float32)
    freqs = ROPE_BASE ** (-jnp.arange(0, HEAD_DIM, 2).astype(jnp.float32) / HEAD_DIM)
    angles = positions[:, None] * freqs[None, :]
    return jnp.cos(angles), jnp.sin(angles)


def normal_weight(key, rows, cols):
    return (jax.random.normal(key, (rows, cols), jnp.float32) * rows ** -0.5).astype(jnp.bfloat16)


def setup_inputs(seed: int = 0) -> dict:
    keys = jax.random.split(jax.random.key(seed), 10)
    act_shape = (BATCH, SEQ_LEN, D_MODEL)
    rope_cos, rope_sin = rope_tables(keys[9])
    return {
        'x_in': jax.random.normal(keys[0], act_shape, jnp.float32).astype(jnp.bfloat16),
        'grad_out': jax.random.normal(keys[1], act_shape, jnp.float32).astype(jnp.bfloat16),
        'gain_attn': 1.0 + 0.3 * jax.random.normal(keys[2], (D_MODEL,), jnp.float32),
        'gain_mlp': 1.0 + 0.3 * jax.random.normal(keys[3], (D_MODEL,), jnp.float32),
        'w_qkv': normal_weight(keys[4], D_MODEL, QKV_COLS),
        'w_out': normal_weight(keys[5], HEADS * HEAD_DIM, D_MODEL),
        'w_gate': normal_weight(keys[6], D_MODEL, D_FF),
        'w_up': normal_weight(keys[7], D_MODEL, D_FF),
        'w_down': normal_weight(keys[8], D_FF, D_MODEL),
        'rope_cos': rope_cos,
        'rope_sin': rope_sin,
    }


def rms_norm(x_f32, gain):
    inv_rms = lax.rsqrt(jnp.mean(x_f32 * x_f32, axis=-1, keepdims=True) + NORM_EPS)
    return (x_f32 * inv_rms * gain).astype(jnp.bfloat16)


def rotate(tensor, cos_t, sin_t):
    half = HEAD_DIM // 2
    first = tensor[..., :half]
    second = tensor[..., half:]
    return jnp.concatenate([first * cos_t - second * sin_t, second * cos_t + first * sin_t], axis=-1)


def matmul(left, right):
    return jnp.dot(left.astype(jnp.float32), right.astype(jnp.float32))


def layer_seq(x_seq, params, rope_cos, rope_sin):
    gain_attn, gain_mlp, w_qkv, w_out, w_gate, w_up, w_down = params
    x_f32 = x_seq.astype(jnp.float32)
    h_attn = rms_norm(x_f32, gain_attn)
    qkv = matmul(h_attn, w_qkv).reshape(SEQ_LEN, KV_HEADS, GROUP_SIZE + 2, HEAD_DIM)
    query = rotate(qkv[:, :, :GROUP_SIZE], rope_cos[:, None, None, :], rope_sin[:, None, None, :]).astype(jnp.bfloat16)
    key_rot = rotate(qkv[:, :, GROUP_SIZE], rope_cos[:, None, :], rope_sin[:, None, :]).astype(jnp.bfloat16)
    value = qkv[:, :, GROUP_SIZE + 1].astype(jnp.bfloat16)
    scores = jnp.einsum('qkgd,tkd->kgqt', query.astype(jnp.float32), key_rot.astype(jnp.float32)) * HEAD_DIM ** -0.5
    pos_ids = jnp.arange(SEQ_LEN)
    scores = jnp.where(pos_ids[:, None] >= pos_ids[None, :], scores, -1e30)
    attn_prob = jax.nn.softmax(scores, axis=-1).astype(jnp.bfloat16)
    attn = jnp.einsum('kgqt,tkd->qkgd', attn_prob.astype(jnp.float32), value.astype(jnp.float32)).astype(jnp.bfloat16)
    attn_proj = matmul(attn.reshape(SEQ_LEN, HEADS * HEAD_DIM), w_out).astype(jnp.bfloat16)
    mid_f32 = (x_f32 + attn_proj.astype(jnp.float32)).astype(jnp.bfloat16).astype(jnp.float32)
    h_mlp = rms_norm(mid_f32, gain_mlp)
    gate = matmul(h_mlp, w_gate)
    up_proj = matmul(h_mlp, w_up)
    gated_act = (jax.nn.silu(gate) * up_proj).astype(jnp.bfloat16)
    mlp_out = matmul(gated_act, w_down).astype(jnp.bfloat16)
    return (mid_f32 + mlp_out.astype(jnp.float32)).astype(jnp.bfloat16)


def reference(x_in, grad_out, gain_attn, gain_mlp, w_qkv, w_out, w_gate, w_up, w_down, rope_cos, rope_sin):
    params = tuple(weight.astype(jnp.float32) for weight in (gain_attn, gain_mlp, w_qkv, w_out, w_gate, w_up, w_down))

    def layer_fn(x_seq, param_set):
        return layer_seq(x_seq, param_set, rope_cos, rope_sin)

    def seq_step(accum, seq_pair):
        x_seq, dy_seq = seq_pair
        y_seq, vjp_fn = jax.vjp(layer_fn, x_seq, params)
        dx_seq, dparams = vjp_fn(dy_seq)
        return jax.tree.map(jnp.add, accum, dparams), (y_seq, dx_seq)

    zero_grads = jax.tree.map(jnp.zeros_like, params)
    grads, (y_out, dx_in) = lax.scan(seq_step, zero_grads, (x_in, grad_out))
    return (y_out, dx_in, grads[0], grads[1], grads[2], grads[3], grads[4], grads[5], grads[6])
```

```python
import functools

import jax
import jax.numpy as jnp
from jax import lax
from jax.experimental import pallas as pl
from jax.experimental.pallas import tpu as pltpu
from jax.sharding import PartitionSpec as P

NORM_EPS = 1e-5
MESH = pl.DeviceIdType.MESH


def rms_scale(x_f32, gain):
    inv_rms = lax.rsqrt(jnp.mean(x_f32 * x_f32, axis=-1, keepdims=True) + NORM_EPS)
    return x_f32 * inv_rms * gain


def rotate(tensor, cos_t, sin_t):
    half = tensor.shape[-1] // 2
    first = tensor[..., :half]
    second = tensor[..., half:]
    return jnp.concatenate([first * cos_t - second * sin_t, second * cos_t + first * sin_t], axis=-1)


def rotate_back(cotangent, cos_t, sin_t):
    half = cotangent.shape[-1] // 2
    first = cotangent[..., :half]
    second = cotangent[..., half:]
    return jnp.concatenate([first * cos_t + second * sin_t, second * cos_t - first * sin_t], axis=-1)


def ring_place(index):
    z, y = index // 2, index % 2
    return z + y * (7 - 2 * z)


def ring_device(place):
    y = place // 4
    return 2 * (place + y * (7 - 2 * place)) + y


def ring_kernel(dims, *refs):
    count = len(dims)
    ins, outs = refs[:count], refs[count:2 * count]
    send_sem, recv_sem, local_sem = refs[2 * count:]
    me = lax.axis_index('fsdp')
    place = ring_place(me)
    targets = (ring_device((place + 1) % 8), ring_device((place + 7) % 8))

    barrier = pltpu.get_barrier_semaphore()
    for target in targets:
        pl.semaphore_signal(barrier, inc=1, device_id={'fsdp': target}, device_id_type=MESH)
    pl.semaphore_wait(barrier, 2)

    def piece(idx, owner, way):
        rows, cols = ins[idx].shape
        half = rows // 2
        if dims[idx] == 0:
            start = pl.multiple_of(owner * rows + way * half, half)
            return outs[idx].at[pl.ds(start, half), :]
        return outs[idx].at[pl.ds(way * half, half), pl.ds(pl.multiple_of(owner * cols, cols), cols)]

    def send(idx, way, step):
        owner = ring_device((place + (8 - step if way == 0 else step)) % 8)
        dst = piece(idx, owner, way)
        half = ins[idx].shape[0] // 2
        src = ins[idx].at[pl.ds(way * half, half), :] if step == 0 else dst
        return pltpu.make_async_remote_copy(
            src_ref=src, dst_ref=dst, send_sem=send_sem.at[idx, way, step], recv_sem=recv_sem.at[idx, way, step],
            device_id={'fsdp': targets[way]}, device_id_type=MESH)

    def landed(idx, way, step):
        owner = ring_device((place + (7 - step if way == 0 else step + 1)) % 8)
        dst = piece(idx, owner, way)
        return pltpu.make_async_remote_copy(
            src_ref=dst, dst_ref=dst, send_sem=send_sem.at[idx, way, step], recv_sem=recv_sem.at[idx, way, step],
            device_id={'fsdp': targets[way]}, device_id_type=MESH)

    def own(idx, way):
        half = ins[idx].shape[0] // 2
        return pltpu.make_async_copy(ins[idx].at[pl.ds(way * half, half), :], piece(idx, me, way), local_sem.at[idx, way])

    for step in range(7):
        for idx in range(count):
            for way in range(2):
                if step > 0:
                    landed(idx, way, step - 1).wait_recv()
                send(idx, way, step).start()
                if step == 0:
                    own(idx, way).start()
    for idx in range(count):
        for way in range(2):
            landed(idx, way, 6).wait_recv()
            own(idx, way).wait()
            for step in range(7):
                send(idx, way, step).wait_send()


def ring_gather(arrays, dims, collective_id):
    shapes = []
    for array, dim in zip(arrays, dims):
        shape = list(array.shape)
        shape[dim] *= 8
        shapes.append(jax.ShapeDtypeStruct(tuple(shape), array.dtype))
    count = len(arrays)
    return pl.pallas_call(
        functools.partial(ring_kernel, tuple(dims)),
        out_shape=shapes,
        in_specs=[pl.BlockSpec(memory_space=pl.ANY)] * count,
        out_specs=[pl.BlockSpec(memory_space=pl.ANY)] * count,
        scratch_shapes=[pltpu.SemaphoreType.DMA((count, 2, 7)), pltpu.SemaphoreType.DMA((count, 2, 7)),
                        pltpu.SemaphoreType.DMA((count, 2))],
        compiler_params=pltpu.CompilerParams(collective_id=collective_id, has_side_effects=True),
        name=f'ring_gather_{collective_id}',
    )(*arrays)


def solution(mesh):
    act_spec = P('fsdp', 'model', None)
    rows_spec = P('fsdp', 'model')
    cols_spec = P('model', 'fsdp')
    f32 = jnp.float32
    bf16 = jnp.bfloat16

    def gather_seq(tensor):
        return lax.all_gather(tensor, 'model', axis=1, tiled=True)

    def scatter_seq(tensor):
        return lax.psum_scatter(tensor, 'model', scatter_dimension=1, tiled=True)

    def device_fn(x_loc, dy_loc, gain_attn, gain_mlp, wqkv_sh, wout_sh, wgate_sh, wup_sh, wdown_sh, rope_cos, rope_sin):
        head_dim = 2 * rope_cos.shape[1]
        seq_full = rope_cos.shape[0]
        local_heads = wout_sh.shape[0] // head_dim
        local_kv = (wqkv_sh.shape[1] // head_dim - local_heads) // 2
        group_size = local_heads // local_kv
        rows = x_loc.shape[0]
        tokens = rows * seq_full
        scale = head_dim ** -0.5
        pos_ids = jnp.arange(seq_full)
        causal = pos_ids[:, None] >= pos_ids[None, :]
        cos_q = rope_cos[:, None, None, :]
        sin_q = rope_sin[:, None, None, :]
        cos_k = rope_cos[:, None, :]
        sin_k = rope_sin[:, None, :]

        w_qkv, w_out, w_gate, w_up, w_down = ring_gather(
            [wqkv_sh, wout_sh, wgate_sh, wup_sh, wdown_sh], [0, 1, 0, 0, 1], 0)

        x_f32 = x_loc.astype(f32)
        h_attn_f, norm_back_attn = jax.vjp(rms_scale, x_f32, gain_attn)
        h_attn_loc = h_attn_f.astype(bf16)
        h_attn = gather_seq(h_attn_loc)
        dy_full = gather_seq(dy_loc)
        qkv = jnp.einsum('bsd,dc->bsc', h_attn, w_qkv, preferred_element_type=f32)
        qkv = qkv.reshape(rows, seq_full, local_kv, group_size + 2, head_dim)
        query = rotate(qkv[:, :, :, :group_size], cos_q, sin_q).astype(bf16)
        key_rot = rotate(qkv[:, :, :, group_size], cos_k, sin_k).astype(bf16)
        value = qkv[:, :, :, group_size + 1].astype(bf16)
        scores = jnp.einsum('bqkgd,btkd->bkgqt', query, key_rot, preferred_element_type=f32) * scale
        attn_prob = jax.nn.softmax(jnp.where(causal, scores, -1e30), axis=-1)
        prob_bf = attn_prob.astype(bf16)
        attn = jnp.einsum('bkgqt,btkd->bqkgd', prob_bf, value, preferred_element_type=f32)
        attn_flat = attn.astype(bf16).reshape(rows, seq_full, local_heads * head_dim)
        attn_red = scatter_seq(jnp.einsum('bsh,hd->bsd', attn_flat, w_out, preferred_element_type=f32))
        mid_f32 = (x_f32 + attn_red.astype(bf16).astype(f32)).astype(bf16).astype(f32)
        h_mlp_f, norm_back_mlp = jax.vjp(rms_scale, mid_f32, gain_mlp)
        h_mlp_loc = h_mlp_f.astype(bf16)
        h_mlp = gather_seq(h_mlp_loc)
        gate = jnp.einsum('bsd,df->bsf', h_mlp, w_gate, preferred_element_type=f32)
        up_proj = jnp.einsum('bsd,df->bsf', h_mlp, w_up, preferred_element_type=f32)
        sig_gate = jax.nn.sigmoid(gate)
        silu_gate = gate * sig_gate
        gated_act = (silu_gate * up_proj).astype(bf16)
        mlp_red = scatter_seq(jnp.einsum('bsf,fd->bsd', gated_act, w_down, preferred_element_type=f32))
        y_loc = (mid_f32 + mlp_red.astype(bf16).astype(f32)).astype(bf16)

        d_act = jnp.einsum('bsd,fd->bsf', dy_full, w_down, preferred_element_type=f32).astype(bf16).astype(f32)
        d_gate = (d_act * up_proj * sig_gate * (1.0 + gate * (1.0 - sig_gate))).astype(bf16)
        d_up = (d_act * silu_gate).astype(bf16)
        dh_mlp = scatter_seq(jnp.einsum('bsf,df->bsd', d_gate, w_gate, preferred_element_type=f32)
                             + jnp.einsum('bsf,df->bsd', d_up, w_up, preferred_element_type=f32))
        d_mid_norm, d_gain_mlp = norm_back_mlp(dh_mlp.astype(bf16).astype(f32))
        d_mid = (dy_loc.astype(f32) + d_mid_norm).astype(bf16)

        d_mid_full = gather_seq(d_mid)
        d_attn = jnp.einsum('bsd,hd->bsh', d_mid_full, w_out, preferred_element_type=f32).astype(bf16)
        d_attn = d_attn.reshape(rows, seq_full, local_kv, group_size, head_dim)
        d_prob = jnp.einsum('bqkgd,btkd->bkgqt', d_attn, value, preferred_element_type=f32)
        d_value = jnp.einsum('bkgqt,bqkgd->btkd', prob_bf, d_attn, preferred_element_type=f32)
        row_dot = jnp.sum(d_prob * attn_prob, axis=-1, keepdims=True)
        d_scores = (attn_prob * (d_prob - row_dot) * scale).astype(bf16)
        d_query = jnp.einsum('bkgqt,btkd->bqkgd', d_scores, key_rot, preferred_element_type=f32)
        d_key = jnp.einsum('bkgqt,bqkgd->btkd', d_scores, query, preferred_element_type=f32)
        d_qkv = jnp.concatenate([rotate_back(d_query, cos_q, sin_q),
                                 rotate_back(d_key, cos_k, sin_k)[:, :, :, None],
                                 d_value[:, :, :, None]], axis=3)
        d_qkv = d_qkv.astype(bf16).reshape(rows, seq_full, -1)
        dh_attn = scatter_seq(jnp.einsum('bsc,dc->bsd', d_qkv, w_qkv, preferred_element_type=f32))
        d_x_norm, d_gain_attn = norm_back_attn(dh_attn.astype(bf16).astype(f32))
        dx_loc = (d_mid.astype(f32) + d_x_norm).astype(bf16)
        gain_grads = lax.psum((d_gain_attn, d_gain_mlp), ('fsdp', 'model'))

        fsdp_size = 8
        width = x_loc.shape[2] // fsdp_size
        pos_loc = x_loc.shape[1]
        packed = jnp.stack([h_attn_loc, h_mlp_loc, dy_loc, d_mid], axis=0)
        packed = packed.reshape(4, rows, pos_loc, fsdp_size, width).transpose(3, 0, 1, 2, 4)
        packed = lax.all_to_all(packed, 'fsdp', 0, 0, tiled=True)
        packed = lax.all_gather(packed, 'model', axis=0)
        packed = packed.transpose(2, 1, 3, 0, 4, 5).reshape(4, fsdp_size * tokens, width)

        d_qkv_all, attn_all, d_gate_all, d_up_all, act_all = ring_gather(
            [d_qkv.reshape(tokens, -1), attn_flat.reshape(tokens, -1), d_gate.reshape(tokens, -1),
             d_up.reshape(tokens, -1), gated_act.reshape(tokens, -1)], [0, 0, 0, 0, 0], 1)

        def pair(left, right):
            return lax.dot_general(left, right, (((0,), (0,)), ((), ())), preferred_element_type=f32)

        return (y_loc, dx_loc, gain_grads[0], gain_grads[1],
                pair(packed[0], d_qkv_all), pair(attn_all, packed[3]),
                pair(packed[1], d_gate_all), pair(packed[1], d_up_all), pair(act_all, packed[2]))

    in_specs = (act_spec, act_spec, P(), P(), rows_spec, cols_spec, rows_spec, rows_spec, cols_spec, P(), P())
    out_specs = (act_spec, act_spec, P(), P(), rows_spec, cols_spec, rows_spec, rows_spec, cols_spec)
    return jax.shard_map(device_fn, mesh=mesh, in_specs=in_specs, out_specs=out_specs, check_vma=False)
```

```python
import functools

import jax
import jax.numpy as jnp
from jax import lax
from jax.experimental import pallas as pl
from jax.experimental.pallas import tpu as pltpu
from jax.sharding import PartitionSpec as P

NORM_EPS = 1e-5
MESH = pl.DeviceIdType.MESH


def rms_scale(x_f32, gain):
    inv_rms = lax.rsqrt(jnp.mean(x_f32 * x_f32, axis=-1, keepdims=True) + NORM_EPS)
    return x_f32 * inv_rms * gain


def rotate(tensor, cos_t, sin_t):
    half = tensor.shape[-1] // 2
    first = tensor[..., :half]
    second = tensor[..., half:]
    return jnp.concatenate([first * cos_t - second * sin_t, second * cos_t + first * sin_t], axis=-1)


def rotate_back(cotangent, cos_t, sin_t):
    half = cotangent.shape[-1] // 2
    first = cotangent[..., :half]
    second = cotangent[..., half:]
    return jnp.concatenate([first * cos_t + second * sin_t, second * cos_t - first * sin_t], axis=-1)


def ring_place(index):
    z, y = index // 2, index % 2
    return z + y * (7 - 2 * z)


def ring_device(place):
    y = place // 4
    return 2 * (place + y * (7 - 2 * place)) + y


def ring_kernel(dims, slices, sums, *refs):
    count = len(dims)
    total = count + slices + sums
    ins, outs = refs[:total], refs[total:2 * total]
    send_sem, recv_sem, local_sem, slice_send, slice_recv, slice_local, sum_send, sum_recv, sum_local = refs[2 * total:]
    me = lax.axis_index('fsdp')
    me_model = lax.axis_index('model')
    me_all = 4 * me + me_model
    place = ring_place(me)
    targets = (ring_device((place + 1) % 8), ring_device((place + 7) % 8))

    barrier = pltpu.get_barrier_semaphore()
    if sums:
        for hop in range(1, 32):
            peer = (me_all + hop) % 32
            pl.semaphore_signal(barrier, inc=1, device_id={'fsdp': peer // 4, 'model': peer % 4}, device_id_type=MESH)
        pl.semaphore_wait(barrier, 31)
    elif slices:
        for hop in range(1, 8):
            pl.semaphore_signal(barrier, inc=1, device_id={'fsdp': (me + hop) % 8}, device_id_type=MESH)
        pl.semaphore_wait(barrier, 7)
    else:
        for target in targets:
            pl.semaphore_signal(barrier, inc=1, device_id={'fsdp': target}, device_id_type=MESH)
        pl.semaphore_wait(barrier, 2)

    def piece(idx, owner, way):
        rows, cols = ins[idx].shape
        half = rows // 2
        if dims[idx] == 0:
            start = pl.multiple_of(owner * rows + way * half, half)
            return outs[idx].at[pl.ds(start, half), :]
        return outs[idx].at[pl.ds(way * half, half), pl.ds(pl.multiple_of(owner * cols, cols), cols)]

    def send(idx, way, step):
        owner = ring_device((place + (8 - step if way == 0 else step)) % 8)
        dst = piece(idx, owner, way)
        half = ins[idx].shape[0] // 2
        src = ins[idx].at[pl.ds(way * half, half), :] if step == 0 else dst
        return pltpu.make_async_remote_copy(
            src_ref=src, dst_ref=dst, send_sem=send_sem.at[idx, way, step], recv_sem=recv_sem.at[idx, way, step],
            device_id={'fsdp': targets[way]}, device_id_type=MESH)

    def landed(idx, way, step):
        owner = ring_device((place + (7 - step if way == 0 else step + 1)) % 8)
        dst = piece(idx, owner, way)
        return pltpu.make_async_remote_copy(
            src_ref=dst, dst_ref=dst, send_sem=send_sem.at[idx, way, step], recv_sem=recv_sem.at[idx, way, step],
            device_id={'fsdp': targets[way]}, device_id_type=MESH)

    def own(idx, way):
        half = ins[idx].shape[0] // 2
        return pltpu.make_async_copy(ins[idx].at[pl.ds(way * half, half), :], piece(idx, me, way), local_sem.at[idx, way])

    def columns(idx, peer):
        src = ins[count + idx]
        width = src.shape[2] // 8
        return src.at[:, :, pl.ds(pl.multiple_of(peer * width, width), width)]

    def slice_out(idx, hop):
        peer = (me + hop) % 8
        return pltpu.make_async_remote_copy(
            src_ref=columns(idx, peer), dst_ref=outs[count + idx].at[me], send_sem=slice_send.at[idx, hop],
            recv_sem=slice_recv.at[idx, hop], device_id={'fsdp': peer}, device_id_type=MESH)

    def slice_in(idx, hop):
        slot = outs[count + idx].at[(me + 8 - hop) % 8]
        return pltpu.make_async_remote_copy(
            src_ref=slot, dst_ref=slot, send_sem=slice_send.at[idx, hop], recv_sem=slice_recv.at[idx, hop],
            device_id={'fsdp': (me + hop) % 8}, device_id_type=MESH)

    def slice_own(idx):
        return pltpu.make_async_copy(columns(idx, me), outs[count + idx].at[me], slice_local.at[idx])

    def sum_copy(idx, hop, incoming):
        peer = (me_all + hop) % 32
        slot = outs[count + slices + idx].at[(me_all + 32 - hop) % 32 if incoming else me_all]
        return pltpu.make_async_remote_copy(
            src_ref=slot if incoming else ins[count + slices + idx], dst_ref=slot, send_sem=sum_send.at[idx, hop],
            recv_sem=sum_recv.at[idx, hop], device_id={'fsdp': peer // 4, 'model': peer % 4}, device_id_type=MESH)

    def sum_own(idx):
        return pltpu.make_async_copy(ins[count + slices + idx], outs[count + slices + idx].at[me_all], sum_local.at[idx])

    for step in range(7):
        for idx in range(count):
            for way in range(2):
                if step > 0:
                    landed(idx, way, step - 1).wait_recv()
                send(idx, way, step).start()
        if step == 0:
            for idx in range(slices):
                slice_own(idx).start()
                for hop in range(1, 8):
                    slice_out(idx, hop).start()
            for idx in range(sums):
                sum_own(idx).start()
                for hop in range(1, 32):
                    sum_copy(idx, hop, False).start()
            for idx in range(count):
                for way in range(2):
                    own(idx, way).start()
    for idx in range(count):
        for way in range(2):
            landed(idx, way, 6).wait_recv()
            own(idx, way).wait()
            for step in range(7):
                send(idx, way, step).wait_send()
    for idx in range(slices):
        slice_own(idx).wait()
        for hop in range(1, 8):
            slice_in(idx, hop).wait_recv()
            slice_out(idx, hop).wait_send()
    for idx in range(sums):
        sum_own(idx).wait()
        for hop in range(1, 32):
            sum_copy(idx, hop, True).wait_recv()
            sum_copy(idx, hop, False).wait_send()


def ring_gather(collective_id, arrays, dims, slices=(), sums=()):
    shapes = []
    sent = 0
    for array, dim in zip(arrays, dims):
        shape = list(array.shape)
        shape[dim] *= 8
        shapes.append(jax.ShapeDtypeStruct(tuple(shape), array.dtype))
        sent += 7 * array.size * 2
    for array in slices:
        shapes.append(jax.ShapeDtypeStruct((8,) + array.shape[:2] + (array.shape[2] // 8,), array.dtype))
    for array in sums:
        shapes.append(jax.ShapeDtypeStruct((32,) + array.shape, array.dtype))
    count, n_slices, n_sums = len(arrays), len(slices), len(sums)
    dma = pltpu.SemaphoreType.DMA
    return pl.pallas_call(
        functools.partial(ring_kernel, tuple(dims), n_slices, n_sums),
        out_shape=shapes,
        in_specs=[pl.BlockSpec(memory_space=pl.ANY)] * len(shapes),
        out_specs=[pl.BlockSpec(memory_space=pl.ANY)] * len(shapes),
        scratch_shapes=[dma((count, 2, 7)), dma((count, 2, 7)), dma((count, 2)),
                        dma((max(n_slices, 1), 8)), dma((max(n_slices, 1), 8)), dma((max(n_slices, 1),)),
                        dma((max(n_sums, 1), 32)), dma((max(n_sums, 1), 32)), dma((max(n_sums, 1),))],
        compiler_params=pltpu.CompilerParams(collective_id=collective_id, has_side_effects=True),
        cost_estimate=pl.CostEstimate(flops=sent * 3000, bytes_accessed=2 * sent, transcendentals=0),
        name=f'ring_gather_{collective_id}',
    )(*arrays, *slices, *sums)


def after(values, *deps):
    return lax.optimization_barrier((tuple(values), deps))[0]


def solution(mesh):
    act_spec = P('fsdp', 'model', None)
    rows_spec = P('fsdp', 'model')
    cols_spec = P('model', 'fsdp')
    f32 = jnp.float32
    bf16 = jnp.bfloat16

    def gather_seq(tensor):
        return lax.all_gather(tensor, 'model', axis=1, tiled=True)

    def scatter_seq(tensor):
        return lax.psum_scatter(tensor, 'model', scatter_dimension=1, tiled=True)

    def device_fn(x_loc, dy_loc, gain_attn, gain_mlp, wqkv_sh, wout_sh, wgate_sh, wup_sh, wdown_sh, rope_cos, rope_sin):
        head_dim = 2 * rope_cos.shape[1]
        seq_full = rope_cos.shape[0]
        local_heads = wout_sh.shape[0] // head_dim
        local_kv = (wqkv_sh.shape[1] // head_dim - local_heads) // 2
        group_size = local_heads // local_kv
        rows = x_loc.shape[0]
        tokens = rows * seq_full
        scale = head_dim ** -0.5
        pos_ids = jnp.arange(seq_full)
        causal = pos_ids[:, None] >= pos_ids[None, :]
        cos_q = rope_cos[:, None, None, :]
        sin_q = rope_sin[:, None, None, :]
        cos_k = rope_cos[:, None, :]
        sin_k = rope_sin[:, None, :]

        x_f32 = x_loc.astype(f32)
        h_attn_f, norm_back_attn = jax.vjp(rms_scale, x_f32, gain_attn)
        h_attn_loc = h_attn_f.astype(bf16)
        h_attn = gather_seq(h_attn_loc)
        dy_full = gather_seq(dy_loc)
        w_qkv, w_out, h_attn_cols, dy_cols = ring_gather(0, [wqkv_sh, wout_sh], [0, 1], [h_attn_loc, dy_loc])
        qkv = jnp.einsum('bsd,dc->bsc', h_attn, w_qkv, preferred_element_type=f32)
        qkv = qkv.reshape(rows, seq_full, local_kv, group_size + 2, head_dim)
        query = rotate(qkv[:, :, :, :group_size], cos_q, sin_q).astype(bf16)
        key_rot = rotate(qkv[:, :, :, group_size], cos_k, sin_k).astype(bf16)
        value = qkv[:, :, :, group_size + 1].astype(bf16)
        scores = jnp.einsum('bqkgd,btkd->bkgqt', query, key_rot, preferred_element_type=f32) * scale
        attn_prob = jax.nn.softmax(jnp.where(causal, scores, -1e30), axis=-1)
        prob_bf = attn_prob.astype(bf16)
        attn = jnp.einsum('bkgqt,btkd->bqkgd', prob_bf, value, preferred_element_type=f32)
        attn_flat = attn.astype(bf16).reshape(rows, seq_full, local_heads * head_dim)
        attn_part = jnp.einsum('bsh,hd->bsd', attn_flat, w_out, preferred_element_type=f32)
        attn_red = scatter_seq(attn_part)
        w_gate, w_up = ring_gather(1, after([wgate_sh, wup_sh], attn_part), [0, 0])
        attn_red, = after([attn_red], w_gate)
        mid_f32 = (x_f32 + attn_red.astype(bf16).astype(f32)).astype(bf16).astype(f32)
        h_mlp_f, norm_back_mlp = jax.vjp(rms_scale, mid_f32, gain_mlp)
        h_mlp_loc = h_mlp_f.astype(bf16)
        h_mlp = gather_seq(h_mlp_loc)
        wdown_sh, h_mlp_src = after([wdown_sh, h_mlp_loc])
        w_down, h_mlp_cols = ring_gather(2, [wdown_sh], [1], [h_mlp_src])
        h_mlp, = after([h_mlp], w_down)
        gate = jnp.einsum('bsd,df->bsf', h_mlp, w_gate, preferred_element_type=f32)
        up_proj = jnp.einsum('bsd,df->bsf', h_mlp, w_up, preferred_element_type=f32)
        sig_gate = jax.nn.sigmoid(gate)
        silu_gate = gate * sig_gate
        gated_act = (silu_gate * up_proj).astype(bf16)
        mlp_part = jnp.einsum('bsf,fd->bsd', gated_act, w_down, preferred_element_type=f32)

        d_act = jnp.einsum('bsd,fd->bsf', dy_full, w_down, preferred_element_type=f32).astype(bf16).astype(f32)
        d_gate = (d_act * up_proj * sig_gate * (1.0 + gate * (1.0 - sig_gate))).astype(bf16)
        d_up = (d_act * silu_gate).astype(bf16)
        dh_part = (jnp.einsum('bsf,df->bsd', d_gate, w_gate, preferred_element_type=f32)
                   + jnp.einsum('bsf,df->bsd', d_up, w_up, preferred_element_type=f32))
        dh_mlp = scatter_seq(dh_part)
        mlp_red = scatter_seq(mlp_part)
        act_all, = ring_gather(3, after([gated_act.reshape(tokens, -1)], dh_part, mlp_part), [0])
        dh_mlp, mlp_red = after([dh_mlp, mlp_red], act_all)
        y_loc = (mid_f32 + mlp_red.astype(bf16).astype(f32)).astype(bf16)
        d_mid_norm, d_gain_mlp = norm_back_mlp(dh_mlp.astype(bf16).astype(f32))
        d_mid = (dy_loc.astype(f32) + d_mid_norm).astype(bf16)

        d_mid_full = gather_seq(d_mid)
        flat_gate, flat_attn, d_mid_src = after([d_gate.reshape(tokens, -1), attn_flat.reshape(tokens, -1), d_mid])
        d_gate_all, attn_all, d_mid_cols = ring_gather(4, [flat_gate, flat_attn], [0, 0], [d_mid_src])
        d_mid_full, = after([d_mid_full], d_gate_all)
        d_attn = jnp.einsum('bsd,hd->bsh', d_mid_full, w_out, preferred_element_type=f32).astype(bf16)
        d_attn = d_attn.reshape(rows, seq_full, local_kv, group_size, head_dim)
        d_prob = jnp.einsum('bqkgd,btkd->bkgqt', d_attn, value, preferred_element_type=f32)
        d_value = jnp.einsum('bkgqt,bqkgd->btkd', prob_bf, d_attn, preferred_element_type=f32)
        row_dot = jnp.sum(d_prob * attn_prob, axis=-1, keepdims=True)
        d_scores = (attn_prob * (d_prob - row_dot) * scale).astype(bf16)
        d_query = jnp.einsum('bkgqt,btkd->bqkgd', d_scores, key_rot, preferred_element_type=f32)
        d_key = jnp.einsum('bkgqt,bqkgd->btkd', d_scores, query, preferred_element_type=f32)
        d_qkv = jnp.concatenate([rotate_back(d_query, cos_q, sin_q),
                                 rotate_back(d_key, cos_k, sin_k)[:, :, :, None],
                                 d_value[:, :, :, None]], axis=3)
        d_qkv = d_qkv.astype(bf16).reshape(rows, seq_full, -1)
        dh_attn_part = jnp.einsum('bsc,dc->bsd', d_qkv, w_qkv, preferred_element_type=f32)
        dh_attn = scatter_seq(dh_attn_part)
        d_up_all, = ring_gather(5, after([d_up.reshape(tokens, -1)], dh_attn_part), [0])
        dh_attn, = after([dh_attn], d_up_all)
        d_x_norm, d_gain_attn = norm_back_attn(dh_attn.astype(bf16).astype(f32))
        dx_loc = (d_mid.astype(f32) + d_x_norm).astype(bf16)
        gains = jnp.stack([d_gain_attn, d_gain_mlp]).reshape(16, -1)
        flat_qkv, gains = after([d_qkv.reshape(tokens, -1), gains])
        d_qkv_all, gains_all = ring_gather(6, [flat_qkv], [0], (), [gains])
        gain_grads = jnp.sum(gains_all, axis=0).reshape(2, -1)

        def spread(pieces):
            pieces = lax.all_gather(pieces, 'model', axis=0)
            return pieces.transpose(1, 2, 0, 3, 4).reshape(8 * tokens, -1)

        h_attn_cols, dy_cols, h_mlp_cols, d_mid_cols = map(spread, (h_attn_cols, dy_cols, h_mlp_cols, d_mid_cols))

        def pair(left, right):
            return lax.dot_general(left, right, (((0,), (0,)), ((), ())), preferred_element_type=f32)

        return (y_loc, dx_loc, gain_grads[0], gain_grads[1],
                pair(h_attn_cols, d_qkv_all), pair(attn_all, d_mid_cols),
                pair(h_mlp_cols, d_gate_all), pair(h_mlp_cols, d_up_all), pair(act_all, dy_cols))

    in_specs = (act_spec, act_spec, P(), P(), rows_spec, cols_spec, rows_spec, rows_spec, cols_spec, P(), P())
    out_specs = (act_spec, act_spec, P(), P(), rows_spec, cols_spec, rows_spec, rows_spec, cols_spec)
    return jax.shard_map(device_fn, mesh=mesh, in_specs=in_specs, out_specs=out_specs, check_vma=False)
```

```python
import functools

import jax
import jax.numpy as jnp
from jax import lax
from jax.experimental import pallas as pl
from jax.experimental.pallas import tpu as pltpu
from jax.sharding import PartitionSpec as P

NORM_EPS = 1e-5
MESH = pl.DeviceIdType.MESH


def rms_scale(x_f32, gain):
    inv_rms = lax.rsqrt(jnp.mean(x_f32 * x_f32, axis=-1, keepdims=True) + NORM_EPS)
    return x_f32 * inv_rms * gain


def rotate(tensor, cos_t, sin_t):
    half = tensor.shape[-1] // 2
    first = tensor[..., :half]
    second = tensor[..., half:]
    return jnp.concatenate([first * cos_t - second * sin_t, second * cos_t + first * sin_t], axis=-1)


def rotate_back(cotangent, cos_t, sin_t):
    half = cotangent.shape[-1] // 2
    first = cotangent[..., :half]
    second = cotangent[..., half:]
    return jnp.concatenate([first * cos_t + second * sin_t, second * cos_t - first * sin_t], axis=-1)


def ring_place(index):
    z, y = index // 2, index % 2
    return z + y * (7 - 2 * z)


def ring_device(place):
    y = place // 4
    return 2 * (place + y * (7 - 2 * place)) + y


def ring_kernel(dims, spans, slices, sums, *refs):
    count = len(dims)
    total = count + slices + sums
    ins, outs = refs[:total], refs[total:2 * total]
    mix = refs[2 * total] if sums else None
    send_sem, recv_sem, local_sem, slice_send, slice_recv, slice_local, mix_send, mix_recv, mix_local = refs[-9:]
    me = lax.axis_index('fsdp')
    me_model = lax.axis_index('model')
    place = ring_place(me)
    targets = (ring_device((place + 1) % 8), ring_device((place + 7) % 8))

    barrier = pltpu.get_barrier_semaphore()
    peers = [(me + hop) % 8 for hop in range(1, 8)] if slices else targets
    for peer in peers:
        pl.semaphore_signal(barrier, inc=1, device_id={'fsdp': peer}, device_id_type=MESH)
    if sums:
        for hop in range(1, 4):
            pl.semaphore_signal(barrier, inc=1, device_id={'model': (me_model + hop) % 4}, device_id_type=MESH)
    pl.semaphore_wait(barrier, len(peers) + 3 * sums)

    def piece(idx, owner, way):
        if idx == count:
            return outs[count + slices].at[owner, pl.ds(2 * way, 2)]
        half = spans[idx][1] // 2
        cols = ins[idx].shape[1]
        if dims[idx] == 0:
            start = pl.multiple_of(owner * (2 * half) + way * half, half)
            return outs[idx].at[pl.ds(start, half), :]
        return outs[idx].at[pl.ds(way * half, half), pl.ds(pl.multiple_of(owner * cols, cols), cols)]

    def source(idx, way):
        if idx == count:
            return mix.at[pl.ds(2 * way, 2)]
        start, length = spans[idx]
        return ins[idx].at[pl.ds(start + way * (length // 2), length // 2), :]

    def send(idx, way, step):
        owner = ring_device((place + (8 - step if way == 0 else step)) % 8)
        dst = piece(idx, owner, way)
        return pltpu.make_async_remote_copy(
            src_ref=source(idx, way) if step == 0 else dst, dst_ref=dst, send_sem=send_sem.at[idx, way, step],
            recv_sem=recv_sem.at[idx, way, step], device_id={'fsdp': targets[way]}, device_id_type=MESH)

    def landed(idx, way, step):
        owner = ring_device((place + (7 - step if way == 0 else step + 1)) % 8)
        dst = piece(idx, owner, way)
        return pltpu.make_async_remote_copy(
            src_ref=dst, dst_ref=dst, send_sem=send_sem.at[idx, way, step], recv_sem=recv_sem.at[idx, way, step],
            device_id={'fsdp': targets[way]}, device_id_type=MESH)

    def own(idx, way):
        return pltpu.make_async_copy(source(idx, way), piece(idx, me, way), local_sem.at[idx, way])

    def columns(idx, peer):
        src = ins[count + idx]
        width = src.shape[2] // 8
        return src.at[:, :, pl.ds(pl.multiple_of(peer * width, width), width)]

    def slice_out(idx, hop):
        peer = (me + hop) % 8
        return pltpu.make_async_remote_copy(
            src_ref=columns(idx, peer), dst_ref=outs[count + idx].at[me], send_sem=slice_send.at[idx, hop],
            recv_sem=slice_recv.at[idx, hop], device_id={'fsdp': peer}, device_id_type=MESH)

    def slice_in(idx, hop):
        slot = outs[count + idx].at[(me + 8 - hop) % 8]
        return pltpu.make_async_remote_copy(
            src_ref=slot, dst_ref=slot, send_sem=slice_send.at[idx, hop], recv_sem=slice_recv.at[idx, hop],
            device_id={'fsdp': (me + hop) % 8}, device_id_type=MESH)

    def slice_own(idx):
        return pltpu.make_async_copy(columns(idx, me), outs[count + idx].at[me], slice_local.at[idx])

    def mix_copy(hop, incoming):
        slot = mix.at[(me_model + 4 - hop) % 4 if incoming else me_model]
        return pltpu.make_async_remote_copy(
            src_ref=slot if incoming else ins[count + slices], dst_ref=slot, send_sem=mix_send.at[hop],
            recv_sem=mix_recv.at[hop], device_id={'model': (me_model + hop) % 4}, device_id_type=MESH)

    def mix_own():
        return pltpu.make_async_copy(ins[count + slices], mix.at[me_model], mix_local)

    if sums:
        mix_own().start()
        for hop in range(1, 4):
            mix_copy(hop, False).start()
    for step in range(7):
        for idx in range(count + sums):
            for way in range(2):
                if step > 0:
                    landed(idx, way, step - 1).wait_recv()
                elif idx == count and way == 0:
                    mix_own().wait()
                    for hop in range(1, 4):
                        mix_copy(hop, True).wait_recv()
                        mix_copy(hop, False).wait_send()
                send(idx, way, step).start()
        if step == 0:
            for idx in range(slices):
                slice_own(idx).start()
                for hop in range(1, 8):
                    slice_out(idx, hop).start()
            for idx in range(count + sums):
                for way in range(2):
                    own(idx, way).start()
    for idx in range(count + sums):
        for way in range(2):
            landed(idx, way, 6).wait_recv()
            own(idx, way).wait()
            for step in range(7):
                send(idx, way, step).wait_send()
    for idx in range(slices):
        slice_own(idx).wait()
        for hop in range(1, 8):
            slice_in(idx, hop).wait_recv()
            slice_out(idx, hop).wait_send()


def ring_gather(collective_id, arrays, dims, slices=(), sums=(), spans=None):
    shapes = []
    sent = 0
    spans = spans or [(0, array.shape[0]) for array in arrays]
    for array, dim, span in zip(arrays, dims, spans):
        rows, cols = span[1], array.shape[1]
        shapes.append(jax.ShapeDtypeStruct((8 * rows, cols) if dim == 0 else (rows, 8 * cols), array.dtype))
        sent += 7 * rows * cols * 2
    for array in slices:
        shapes.append(jax.ShapeDtypeStruct((8,) + array.shape[:2] + (array.shape[2] // 8,), array.dtype))
    for array in sums:
        shapes.append(jax.ShapeDtypeStruct((8, 4) + array.shape, array.dtype))
    n_in = len(shapes)
    for array in sums:
        shapes.append(jax.ShapeDtypeStruct((4,) + array.shape, array.dtype))
    count, n_slices, n_sums = len(arrays), len(slices), len(sums)
    dma = pltpu.SemaphoreType.DMA
    return pl.pallas_call(
        functools.partial(ring_kernel, tuple(dims), tuple(spans), n_slices, n_sums),
        out_shape=shapes,
        in_specs=[pl.BlockSpec(memory_space=pl.ANY)] * n_in,
        out_specs=[pl.BlockSpec(memory_space=pl.ANY)] * len(shapes),
        scratch_shapes=[dma((count + n_sums, 2, 7)), dma((count + n_sums, 2, 7)), dma((count + n_sums, 2)),
                        dma((max(n_slices, 1), 8)), dma((max(n_slices, 1), 8)), dma((max(n_slices, 1),)),
                        dma((4,)), dma((4,)), dma],
        compiler_params=pltpu.CompilerParams(collective_id=collective_id, has_side_effects=True),
        cost_estimate=pl.CostEstimate(flops=sent * 3000, bytes_accessed=2 * sent, transcendentals=0),
        name=f'ring_gather_{collective_id}',
    )(*arrays, *slices, *sums)


TILE = 512


def mlp_kernel(gate_sh, up_sh, down_a, down_b, h_ref, dy_ref, act_ref, d_gate_ref, d_up_ref, y_part_ref, dh_part_ref,
               w_gate, w_up, w_down, gate_acc, up_acc, d_act, send_sem, recv_sem, local_sem, down_sem):
    f32, bf16 = jnp.float32, jnp.bfloat16
    me = lax.axis_index('fsdp')
    place = ring_place(me)
    targets = (ring_device((place + 1) % 8), ring_device((place + 7) % 8))
    barrier = pltpu.get_barrier_semaphore()
    for target in targets:
        pl.semaphore_signal(barrier, inc=1, device_id={'fsdp': target}, device_id_type=MESH)
    pl.semaphore_wait(barrier, 2)
    shards, weights, accs = (gate_sh, up_sh), (w_gate, w_up), (gate_acc, up_acc)
    rows, width = gate_sh.shape
    half = rows // 2

    def start_of(owner, way):
        return pl.multiple_of(owner * rows + way * half, half)

    def send(idx, way, step):
        owner = ring_device((place + (8 - step if way == 0 else step)) % 8)
        dst = weights[idx].at[pl.ds(start_of(owner, way), half), :]
        src = shards[idx].at[pl.ds(way * half, half), :] if isinstance(step, int) and step == 0 else dst
        return pltpu.make_async_remote_copy(
            src_ref=src, dst_ref=dst, send_sem=send_sem.at[idx, way, step], recv_sem=recv_sem.at[idx, way, step],
            device_id={'fsdp': targets[way]}, device_id_type=MESH)

    def landed(idx, way, step):
        owner = ring_device((place + (7 - step if way == 0 else step + 1)) % 8)
        dst = weights[idx].at[pl.ds(start_of(owner, way), half), :]
        return pltpu.make_async_remote_copy(
            src_ref=dst, dst_ref=dst, send_sem=send_sem.at[idx, way, step], recv_sem=recv_sem.at[idx, way, step],
            device_id={'fsdp': targets[way]}, device_id_type=MESH)

    def own(idx, way):
        return pltpu.make_async_copy(shards[idx].at[pl.ds(way * half, half), :],
                                     weights[idx].at[pl.ds(start_of(me, way), half), :], local_sem.at[idx, way])

    def fetch_down(part):
        src = (down_a, down_b)[part]
        return pltpu.make_async_copy(src, w_down.at[pl.ds(part * src.shape[0], src.shape[0]), :], down_sem.at[part])

    def accumulate(step):
        for way in range(2):
            start = start_of(ring_device((place + (8 - step if way == 0 else step)) % 8), way)
            h_block = h_ref[:, pl.ds(start, half)]
            for idx in range(2):
                @pl.loop(0, width // TILE)
                def _(tile):
                    cols = pl.ds(pl.multiple_of(tile * TILE, TILE), TILE)
                    accs[idx][:, cols] += jnp.dot(h_block, weights[idx][pl.ds(start, half), cols],
                                                  preferred_element_type=f32)

    def across(left, right):
        return lax.dot_general(left, right, (((1,), (1,)), ((), ())), preferred_element_type=f32)

    for idx in range(2):
        for way in range(2):
            send(idx, way, 0).start()
    for part in range(2):
        fetch_down(part).start()
    for idx in range(2):
        for way in range(2):
            own(idx, way).start()
    for acc in accs:
        acc[...] = jnp.zeros_like(acc)
    for part in range(2):
        fetch_down(part).wait()

    @pl.loop(0, width // TILE)
    def _(tile):
        cols = pl.ds(pl.multiple_of(tile * TILE, TILE), TILE)
        d_act[:, cols] = across(dy_ref[...], w_down[cols, :]).astype(bf16)

    for idx in range(2):
        for way in range(2):
            own(idx, way).wait()
    accumulate(0)

    @pl.loop(1, 7)
    def _(step):
        for idx in range(2):
            for way in range(2):
                landed(idx, way, step - 1).wait_recv()
                send(idx, way, step).start()
        accumulate(step)

    for idx in range(2):
        for way in range(2):
            landed(idx, way, 6).wait_recv()
    accumulate(7)

    @pl.loop(0, width // 256)
    def _(tile):
        cols = pl.ds(pl.multiple_of(tile * 256, 256), 256)
        gate, up_proj = gate_acc[:, cols], up_acc[:, cols]
        d_val = d_act[:, cols].astype(f32)
        sig_gate = jax.nn.sigmoid(gate)
        silu_gate = gate * sig_gate
        act_ref[:, cols] = (silu_gate * up_proj).astype(bf16)
        d_gate_ref[:, cols] = (d_val * up_proj * sig_gate * (1.0 + gate * (1.0 - sig_gate))).astype(bf16)
        d_up_ref[:, cols] = (d_val * silu_gate).astype(bf16)

    @pl.loop(0, width // TILE)
    def _(tile):
        cols = pl.ds(pl.multiple_of(tile * TILE, TILE), TILE)
        dh_part_ref[:, cols] = across(d_gate_ref[...], w_gate[cols, :]) + across(d_up_ref[...], w_up[cols, :])
        y_part_ref[:, cols] = jnp.dot(act_ref[...], w_down[:, cols], preferred_element_type=f32)

    for idx in range(2):
        for way in range(2):
            for step in range(7):
                send(idx, way, step).wait_send()


def ring_mlp(collective_id, gate_sh, up_sh, down_a, down_b, h_full, dy_full):
    tokens, d_model = h_full.shape
    width = gate_sh.shape[1]
    sent = 14 * gate_sh.size * 2
    dma = pltpu.SemaphoreType.DMA
    vmem = pl.BlockSpec(memory_space=pltpu.VMEM)
    hbm = pl.BlockSpec(memory_space=pl.ANY)
    hidden = jax.ShapeDtypeStruct((tokens, width), jnp.bfloat16)
    partial_sum = jax.ShapeDtypeStruct((tokens, d_model), jnp.float32)
    return pl.pallas_call(
        mlp_kernel,
        out_shape=[hidden, hidden, hidden, partial_sum, partial_sum],
        in_specs=[hbm, hbm, hbm, hbm, vmem, vmem],
        out_specs=[vmem] * 5,
        scratch_shapes=[pltpu.VMEM((d_model, width), jnp.bfloat16), pltpu.VMEM((d_model, width), jnp.bfloat16),
                        pltpu.VMEM((width, d_model), jnp.bfloat16), pltpu.VMEM((tokens, width), jnp.float32),
                        pltpu.VMEM((tokens, width), jnp.float32), pltpu.VMEM((tokens, width), jnp.bfloat16),
                        dma((2, 2, 7)), dma((2, 2, 7)), dma((2, 2)), dma((2,))],
        compiler_params=pltpu.CompilerParams(collective_id=collective_id, has_side_effects=True,
                                             vmem_limit_bytes=60 * 1024 * 1024),
        cost_estimate=pl.CostEstimate(flops=sent * 3000, bytes_accessed=2 * sent, transcendentals=0),
        name=f'ring_mlp_{collective_id}',
    )(gate_sh, up_sh, down_a, down_b, h_full, dy_full)


def after(values, *deps):
    return lax.optimization_barrier((tuple(values), deps))[0]


def solution(mesh):
    act_spec = P('fsdp', 'model', None)
    rows_spec = P('fsdp', 'model')
    cols_spec = P('model', 'fsdp')
    f32 = jnp.float32
    bf16 = jnp.bfloat16

    def gather_seq(tensor):
        return lax.all_gather(tensor, 'model', axis=1, tiled=True)

    def scatter_seq(tensor):
        return lax.psum_scatter(tensor, 'model', scatter_dimension=1, tiled=True)

    def device_fn(x_loc, dy_loc, gain_attn, gain_mlp, wqkv_sh, wout_sh, wgate_sh, wup_sh, wdown_sh, rope_cos, rope_sin):
        head_dim = 2 * rope_cos.shape[1]
        seq_full = rope_cos.shape[0]
        local_heads = wout_sh.shape[0] // head_dim
        local_kv = (wqkv_sh.shape[1] // head_dim - local_heads) // 2
        group_size = local_heads // local_kv
        rows = x_loc.shape[0]
        tokens = rows * seq_full
        scale = head_dim ** -0.5
        pos_ids = jnp.arange(seq_full)
        causal = pos_ids[:, None] >= pos_ids[None, :]
        cos_q = rope_cos[:, None, None, :]
        sin_q = rope_sin[:, None, None, :]
        cos_k = rope_cos[:, None, :]
        sin_k = rope_sin[:, None, :]

        x_f32 = x_loc.astype(f32)
        h_attn_f, norm_back_attn = jax.vjp(rms_scale, x_f32, gain_attn)
        h_attn_loc = h_attn_f.astype(bf16)
        h_attn = gather_seq(h_attn_loc)
        dy_full = gather_seq(dy_loc)
        w_qkv, w_out, h_attn_cols, dy_cols = ring_gather(0, [wqkv_sh, wout_sh], [0, 1], [h_attn_loc, dy_loc])
        qkv = jnp.einsum('bsd,dc->bsc', h_attn, w_qkv, preferred_element_type=f32)
        qkv = qkv.reshape(rows, seq_full, local_kv, group_size + 2, head_dim)
        query = rotate(qkv[:, :, :, :group_size], cos_q, sin_q).astype(bf16)
        key_rot = rotate(qkv[:, :, :, group_size], cos_k, sin_k).astype(bf16)
        value = qkv[:, :, :, group_size + 1].astype(bf16)
        scores = jnp.einsum('bqkgd,btkd->bkgqt', query, key_rot, preferred_element_type=f32) * scale
        attn_prob = jax.nn.softmax(jnp.where(causal, scores, -1e30), axis=-1)
        prob_bf = attn_prob.astype(bf16)
        attn = jnp.einsum('bkgqt,btkd->bqkgd', prob_bf, value, preferred_element_type=f32)
        attn_flat = attn.astype(bf16).reshape(rows, seq_full, local_heads * head_dim)
        attn_part = jnp.einsum('bsh,hd->bsd', attn_flat, w_out, preferred_element_type=f32)
        attn_red = scatter_seq(attn_part)
        half_down = wdown_sh.shape[0] // 2
        down_a, = ring_gather(1, after([wdown_sh], attn_part), [1], spans=[(0, half_down)])
        attn_red, = after([attn_red], down_a)
        mid_f32 = (x_f32 + attn_red.astype(bf16).astype(f32)).astype(bf16).astype(f32)
        h_mlp_f, norm_back_mlp = jax.vjp(rms_scale, mid_f32, gain_mlp)
        h_mlp_loc = h_mlp_f.astype(bf16)
        h_mlp = gather_seq(h_mlp_loc)
        wdown_sh, h_mlp_src = after([wdown_sh, h_mlp_loc])
        down_b, h_mlp_cols = ring_gather(2, [wdown_sh], [1], [h_mlp_src], spans=[(half_down, half_down)])
        h_mlp, = after([h_mlp], down_b)
        gated_act, d_gate, d_up, mlp_part, dh_part = ring_mlp(
            7, wgate_sh, wup_sh, down_a, down_b, h_mlp.reshape(tokens, -1), dy_full.reshape(tokens, -1))
        mlp_part = mlp_part.reshape(rows, seq_full, -1)
        dh_part = dh_part.reshape(rows, seq_full, -1)
        dh_mlp = scatter_seq(dh_part)
        mlp_red = scatter_seq(mlp_part)
        act_all, = ring_gather(3, [gated_act], [0])
        dh_mlp, mlp_red = after([dh_mlp, mlp_red], act_all)
        y_loc = (mid_f32 + mlp_red.astype(bf16).astype(f32)).astype(bf16)
        d_mid_norm, d_gain_mlp = norm_back_mlp(dh_mlp.astype(bf16).astype(f32))
        d_mid = (dy_loc.astype(f32) + d_mid_norm).astype(bf16)

        d_mid_full = gather_seq(d_mid)
        flat_gate, flat_attn, d_mid_src = after([d_gate, attn_flat.reshape(tokens, -1), d_mid])
        d_gate_all, attn_all, d_mid_cols = ring_gather(4, [flat_gate, flat_attn], [0, 0], [d_mid_src])
        d_mid_full, = after([d_mid_full], d_gate_all)
        d_attn = jnp.einsum('bsd,hd->bsh', d_mid_full, w_out, preferred_element_type=f32).astype(bf16)
        d_attn = d_attn.reshape(rows, seq_full, local_kv, group_size, head_dim)
        d_prob = jnp.einsum('bqkgd,btkd->bkgqt', d_attn, value, preferred_element_type=f32)
        d_value = jnp.einsum('bkgqt,bqkgd->btkd', prob_bf, d_attn, preferred_element_type=f32)
        row_dot = jnp.sum(d_prob * attn_prob, axis=-1, keepdims=True)
        d_scores = (attn_prob * (d_prob - row_dot) * scale).astype(bf16)
        d_query = jnp.einsum('bkgqt,btkd->bqkgd', d_scores, key_rot, preferred_element_type=f32)
        d_key = jnp.einsum('bkgqt,bqkgd->btkd', d_scores, query, preferred_element_type=f32)
        d_qkv = jnp.concatenate([rotate_back(d_query, cos_q, sin_q),
                                 rotate_back(d_key, cos_k, sin_k)[:, :, :, None],
                                 d_value[:, :, :, None]], axis=3)
        d_qkv = d_qkv.astype(bf16).reshape(rows, seq_full, -1)
        dh_attn_part = jnp.einsum('bsc,dc->bsd', d_qkv, w_qkv, preferred_element_type=f32)
        dh_attn = scatter_seq(dh_attn_part)
        d_up_all, = ring_gather(5, after([d_up], dh_attn_part), [0])
        dh_attn, = after([dh_attn], d_up_all)
        d_x_norm, d_gain_attn = norm_back_attn(dh_attn.astype(bf16).astype(f32))
        dx_loc = (d_mid.astype(f32) + d_x_norm).astype(bf16)
        gains = jnp.stack([d_gain_attn, d_gain_mlp]).reshape(16, -1)
        flat_qkv, gains = after([d_qkv.reshape(tokens, -1), gains])
        d_qkv_all, gains_all, _ = ring_gather(6, [flat_qkv], [0], (), [gains])
        gain_grads = jnp.sum(gains_all, axis=(0, 1)).reshape(2, -1)

        def spread(pieces):
            pieces = lax.all_gather(pieces, 'model', axis=0)
            return pieces.transpose(1, 2, 0, 3, 4).reshape(8 * tokens, -1)

        h_attn_cols, dy_cols, h_mlp_cols, d_mid_cols = map(spread, (h_attn_cols, dy_cols, h_mlp_cols, d_mid_cols))

        def pair(left, right):
            return lax.dot_general(left, right, (((0,), (0,)), ((), ())), preferred_element_type=f32)

        return (y_loc, dx_loc, gain_grads[0], gain_grads[1],
                pair(h_attn_cols, d_qkv_all), pair(attn_all, d_mid_cols),
                pair(h_mlp_cols, d_gate_all), pair(h_mlp_cols, d_up_all), pair(act_all, dy_cols))

    in_specs = (act_spec, act_spec, P(), P(), rows_spec, cols_spec, rows_spec, rows_spec, cols_spec, P(), P())
    out_specs = (act_spec, act_spec, P(), P(), rows_spec, cols_spec, rows_spec, rows_spec, cols_spec)
    return jax.shard_map(device_fn, mesh=mesh, in_specs=in_specs, out_specs=out_specs, check_vma=False)
```

```python
import functools

import jax
import jax.numpy as jnp
from jax import lax
from jax.experimental import pallas as pl
from jax.experimental.pallas import tpu as pltpu
from jax.sharding import PartitionSpec as P

NORM_EPS = 1e-5
MESH = pl.DeviceIdType.MESH


def rms_scale(x_f32, gain):
    inv_rms = lax.rsqrt(jnp.mean(x_f32 * x_f32, axis=-1, keepdims=True) + NORM_EPS)
    return x_f32 * inv_rms * gain


def rotate(tensor, cos_t, sin_t):
    half = tensor.shape[-1] // 2
    first = tensor[..., :half]
    second = tensor[..., half:]
    return jnp.concatenate([first * cos_t - second * sin_t, second * cos_t + first * sin_t], axis=-1)


def rotate_back(cotangent, cos_t, sin_t):
    half = cotangent.shape[-1] // 2
    first = cotangent[..., :half]
    second = cotangent[..., half:]
    return jnp.concatenate([first * cos_t + second * sin_t, second * cos_t - first * sin_t], axis=-1)


def ring_place(index):
    z, y = index // 2, index % 2
    return z + y * (7 - 2 * z)


def ring_device(place):
    y = place // 4
    return 2 * (place + y * (7 - 2 * place)) + y


def ring_kernel(dims, spans, slices, kinds, sums, *refs):
    count = len(dims)
    first_model = count + slices
    last = first_model + len(kinds)
    total = last + sums
    ins, outs = refs[:total], refs[total:2 * total]
    mix = refs[2 * total] if sums else None
    (send_sem, recv_sem, local_sem, slice_send, slice_recv, slice_local, mix_send, mix_recv, mix_local,
     model_send, model_recv, model_local) = refs[-12:]
    me = lax.axis_index('fsdp')
    me_model = lax.axis_index('model')
    place = ring_place(me)
    targets = (ring_device((place + 1) % 8), ring_device((place + 7) % 8))

    barrier = pltpu.get_barrier_semaphore()
    peers = [(me + hop) % 8 for hop in range(1, 8)] if slices else targets
    for peer in peers:
        pl.semaphore_signal(barrier, inc=1, device_id={'fsdp': peer}, device_id_type=MESH)
    if sums or kinds:
        for hop in range(1, 4):
            pl.semaphore_signal(barrier, inc=1, device_id={'model': (me_model + hop) % 4}, device_id_type=MESH)
    pl.semaphore_wait(barrier, len(peers) + (3 if sums or kinds else 0))

    def piece(idx, owner, way):
        if idx == count:
            return outs[last].at[owner, pl.ds(2 * way, 2)]
        half = spans[idx][1] // 2
        cols = ins[idx].shape[1]
        if dims[idx] == 0:
            start = pl.multiple_of(owner * (2 * half) + way * half, half)
            return outs[idx].at[pl.ds(start, half), :]
        return outs[idx].at[pl.ds(way * half, half), pl.ds(pl.multiple_of(owner * cols, cols), cols)]

    def source(idx, way):
        if idx == count:
            return mix.at[pl.ds(2 * way, 2)]
        start, length = spans[idx]
        return ins[idx].at[pl.ds(start + way * (length // 2), length // 2), :]

    def send(idx, way, step):
        owner = ring_device((place + (8 - step if way == 0 else step)) % 8)
        dst = piece(idx, owner, way)
        return pltpu.make_async_remote_copy(
            src_ref=source(idx, way) if step == 0 else dst, dst_ref=dst, send_sem=send_sem.at[idx, way, step],
            recv_sem=recv_sem.at[idx, way, step], device_id={'fsdp': targets[way]}, device_id_type=MESH)

    def landed(idx, way, step):
        owner = ring_device((place + (7 - step if way == 0 else step + 1)) % 8)
        dst = piece(idx, owner, way)
        return pltpu.make_async_remote_copy(
            src_ref=dst, dst_ref=dst, send_sem=send_sem.at[idx, way, step], recv_sem=recv_sem.at[idx, way, step],
            device_id={'fsdp': targets[way]}, device_id_type=MESH)

    def own(idx, way):
        return pltpu.make_async_copy(source(idx, way), piece(idx, me, way), local_sem.at[idx, way])

    def columns(idx, peer):
        src = ins[count + idx]
        width = src.shape[2] // 8
        return src.at[:, :, pl.ds(pl.multiple_of(peer * width, width), width)]

    def slice_out(idx, hop):
        peer = (me + hop) % 8
        return pltpu.make_async_remote_copy(
            src_ref=columns(idx, peer), dst_ref=outs[count + idx].at[me], send_sem=slice_send.at[idx, hop],
            recv_sem=slice_recv.at[idx, hop], device_id={'fsdp': peer}, device_id_type=MESH)

    def slice_in(idx, hop):
        slot = outs[count + idx].at[(me + 8 - hop) % 8]
        return pltpu.make_async_remote_copy(
            src_ref=slot, dst_ref=slot, send_sem=slice_send.at[idx, hop], recv_sem=slice_recv.at[idx, hop],
            device_id={'fsdp': (me + hop) % 8}, device_id_type=MESH)

    def slice_own(idx):
        return pltpu.make_async_copy(columns(idx, me), outs[count + idx].at[me], slice_local.at[idx])

    def mix_copy(hop, incoming):
        slot = mix.at[(me_model + 4 - hop) % 4 if incoming else me_model]
        return pltpu.make_async_remote_copy(
            src_ref=slot if incoming else ins[last], dst_ref=slot, send_sem=mix_send.at[hop],
            recv_sem=mix_recv.at[hop], device_id={'model': (me_model + hop) % 4}, device_id_type=MESH)

    def mix_own():
        return pltpu.make_async_copy(ins[last], mix.at[me_model], mix_local)

    def model_src(idx, peer):
        src = ins[first_model + idx]
        if kinds[idx] != 'sum':
            return src
        block = src.shape[1] // 4
        return src.at[:, pl.ds(pl.multiple_of(peer * block, block), block), :]

    def model_dst(idx, member):
        dst = outs[first_model + idx]
        if kinds[idx] == 'sum':
            return dst.at[member]
        if kinds[idx] == 'cols':
            return dst.at[:, :, member]
        block = dst.shape[1] // 4
        return dst.at[:, pl.ds(pl.multiple_of(member * block, block), block), :]

    def model_out(idx, hop):
        peer = (me_model + hop) % 4
        return pltpu.make_async_remote_copy(
            src_ref=model_src(idx, peer), dst_ref=model_dst(idx, me_model), send_sem=model_send.at[idx, hop],
            recv_sem=model_recv.at[idx, hop], device_id={'model': peer}, device_id_type=MESH)

    def model_in(idx, hop):
        slot = model_dst(idx, (me_model + 4 - hop) % 4)
        return pltpu.make_async_remote_copy(
            src_ref=slot, dst_ref=slot, send_sem=model_send.at[idx, hop], recv_sem=model_recv.at[idx, hop],
            device_id={'model': (me_model + hop) % 4}, device_id_type=MESH)

    def model_own(idx):
        return pltpu.make_async_copy(model_src(idx, me_model), model_dst(idx, me_model), model_local.at[idx])

    if sums:
        mix_own().start()
        for hop in range(1, 4):
            mix_copy(hop, False).start()
    for step in range(7):
        for idx in range(count + sums):
            for way in range(2):
                if step > 0:
                    landed(idx, way, step - 1).wait_recv()
                elif idx == count and way == 0:
                    mix_own().wait()
                    for hop in range(1, 4):
                        mix_copy(hop, True).wait_recv()
                        mix_copy(hop, False).wait_send()
                send(idx, way, step).start()
        if step == 0:
            for idx in range(slices):
                slice_own(idx).start()
                for hop in range(1, 8):
                    slice_out(idx, hop).start()
            for idx in range(len(kinds)):
                for hop in range(1, 4):
                    model_out(idx, hop).start()
                model_own(idx).start()
            for idx in range(count + sums):
                for way in range(2):
                    own(idx, way).start()
    for idx in range(count + sums):
        for way in range(2):
            landed(idx, way, 6).wait_recv()
            own(idx, way).wait()
            for step in range(7):
                send(idx, way, step).wait_send()
    for idx in range(slices):
        slice_own(idx).wait()
        for hop in range(1, 8):
            slice_in(idx, hop).wait_recv()
            slice_out(idx, hop).wait_send()
    for idx in range(len(kinds)):
        model_own(idx).wait()
        for hop in range(1, 4):
            model_in(idx, hop).wait_recv()
            model_out(idx, hop).wait_send()


def ring_gather(collective_id, arrays, dims, slices=(), model=(), sums=(), spans=None):
    shapes = []
    sent = 0
    spans = spans or [(0, array.shape[0]) for array in arrays]
    for array, dim, span in zip(arrays, dims, spans):
        rows, cols = span[1], array.shape[1]
        shapes.append(jax.ShapeDtypeStruct((8 * rows, cols) if dim == 0 else (rows, 8 * cols), array.dtype))
        sent += 7 * rows * cols * 2
    for array in slices:
        shapes.append(jax.ShapeDtypeStruct((8,) + array.shape[:2] + (array.shape[2] // 8,), array.dtype))
    for kind, array in model:
        if kind == 'sum':
            shape = (4, array.shape[0], array.shape[1] // 4, array.shape[2])
        elif kind == 'cols':
            shape = array.shape[:2] + (4,) + array.shape[2:]
        else:
            shape = (array.shape[0], 4 * array.shape[1], array.shape[2])
        shapes.append(jax.ShapeDtypeStruct(shape, array.dtype))
    for array in sums:
        shapes.append(jax.ShapeDtypeStruct((8, 4) + array.shape, array.dtype))
    n_in = len(shapes)
    for array in sums:
        shapes.append(jax.ShapeDtypeStruct((4,) + array.shape, array.dtype))
    count, n_slices, n_sums = len(arrays), len(slices), len(sums)
    dma = pltpu.SemaphoreType.DMA
    return pl.pallas_call(
        functools.partial(ring_kernel, tuple(dims), tuple(spans), n_slices, tuple(kind for kind, _ in model), n_sums),
        out_shape=shapes,
        in_specs=[pl.BlockSpec(memory_space=pl.ANY)] * n_in,
        out_specs=[pl.BlockSpec(memory_space=pl.ANY)] * len(shapes),
        scratch_shapes=[dma((count + n_sums, 2, 7)), dma((count + n_sums, 2, 7)), dma((count + n_sums, 2)),
                        dma((max(n_slices, 1), 8)), dma((max(n_slices, 1), 8)), dma((max(n_slices, 1),)),
                        dma((4,)), dma((4,)), dma, dma((max(len(model), 1), 4)), dma((max(len(model), 1), 4)),
                        dma((max(len(model), 1),))],
        compiler_params=pltpu.CompilerParams(collective_id=collective_id, has_side_effects=True),
        cost_estimate=pl.CostEstimate(flops=sent * 3000, bytes_accessed=2 * sent, transcendentals=0),
        name=f'ring_gather_{collective_id}',
    )(*arrays, *slices, *[array for _, array in model], *sums)


TILE = 512


def mlp_kernel(gate_sh, up_sh, down_a, down_b, h_ref, dy_ref, act_ref, d_gate_ref, d_up_ref, y_part_ref, dh_part_ref,
               w_gate, w_up, w_down, gate_acc, up_acc, d_act, send_sem, recv_sem, local_sem, down_sem):
    f32, bf16 = jnp.float32, jnp.bfloat16
    me = lax.axis_index('fsdp')
    place = ring_place(me)
    targets = (ring_device((place + 1) % 8), ring_device((place + 7) % 8))
    barrier = pltpu.get_barrier_semaphore()
    for target in targets:
        pl.semaphore_signal(barrier, inc=1, device_id={'fsdp': target}, device_id_type=MESH)
    pl.semaphore_wait(barrier, 2)
    shards, weights, accs = (gate_sh, up_sh), (w_gate, w_up), (gate_acc, up_acc)
    rows, width = gate_sh.shape
    half = rows // 2

    def start_of(owner, way):
        return pl.multiple_of(owner * rows + way * half, half)

    def send(idx, way, step):
        owner = ring_device((place + (8 - step if way == 0 else step)) % 8)
        dst = weights[idx].at[pl.ds(start_of(owner, way), half), :]
        src = shards[idx].at[pl.ds(way * half, half), :] if isinstance(step, int) and step == 0 else dst
        return pltpu.make_async_remote_copy(
            src_ref=src, dst_ref=dst, send_sem=send_sem.at[idx, way, step], recv_sem=recv_sem.at[idx, way, step],
            device_id={'fsdp': targets[way]}, device_id_type=MESH)

    def landed(idx, way, step):
        owner = ring_device((place + (7 - step if way == 0 else step + 1)) % 8)
        dst = weights[idx].at[pl.ds(start_of(owner, way), half), :]
        return pltpu.make_async_remote_copy(
            src_ref=dst, dst_ref=dst, send_sem=send_sem.at[idx, way, step], recv_sem=recv_sem.at[idx, way, step],
            device_id={'fsdp': targets[way]}, device_id_type=MESH)

    def own(idx, way):
        return pltpu.make_async_copy(shards[idx].at[pl.ds(way * half, half), :],
                                     weights[idx].at[pl.ds(start_of(me, way), half), :], local_sem.at[idx, way])

    def fetch_down(part):
        src = (down_a, down_b)[part]
        return pltpu.make_async_copy(src, w_down.at[pl.ds(part * src.shape[0], src.shape[0]), :], down_sem.at[part])

    def accumulate(step):
        for way in range(2):
            start = start_of(ring_device((place + (8 - step if way == 0 else step)) % 8), way)
            h_block = h_ref[:, pl.ds(start, half)]
            for idx in range(2):
                @pl.loop(0, width // TILE)
                def _(tile):
                    cols = pl.ds(pl.multiple_of(tile * TILE, TILE), TILE)
                    accs[idx][:, cols] += jnp.dot(h_block, weights[idx][pl.ds(start, half), cols],
                                                  preferred_element_type=f32)

    def across(left, right):
        return lax.dot_general(left, right, (((1,), (1,)), ((), ())), preferred_element_type=f32)

    for idx in range(2):
        for way in range(2):
            send(idx, way, 0).start()
    for part in range(2):
        fetch_down(part).start()
    for idx in range(2):
        for way in range(2):
            own(idx, way).start()
    for acc in accs:
        acc[...] = jnp.zeros_like(acc)
    for part in range(2):
        fetch_down(part).wait()

    @pl.loop(0, width // TILE)
    def _(tile):
        cols = pl.ds(pl.multiple_of(tile * TILE, TILE), TILE)
        d_act[:, cols] = across(dy_ref[...], w_down[cols, :]).astype(bf16)

    for idx in range(2):
        for way in range(2):
            own(idx, way).wait()
    accumulate(0)

    @pl.loop(1, 7)
    def _(step):
        for idx in range(2):
            for way in range(2):
                landed(idx, way, step - 1).wait_recv()
                send(idx, way, step).start()
        accumulate(step)

    for idx in range(2):
        for way in range(2):
            landed(idx, way, 6).wait_recv()
    accumulate(7)

    @pl.loop(0, width // 256)
    def _(tile):
        cols = pl.ds(pl.multiple_of(tile * 256, 256), 256)
        gate, up_proj = gate_acc[:, cols], up_acc[:, cols]
        d_val = d_act[:, cols].astype(f32)
        sig_gate = jax.nn.sigmoid(gate)
        silu_gate = gate * sig_gate
        act_ref[:, cols] = (silu_gate * up_proj).astype(bf16)
        d_gate_ref[:, cols] = (d_val * up_proj * sig_gate * (1.0 + gate * (1.0 - sig_gate))).astype(bf16)
        d_up_ref[:, cols] = (d_val * silu_gate).astype(bf16)

    @pl.loop(0, width // TILE)
    def _(tile):
        cols = pl.ds(pl.multiple_of(tile * TILE, TILE), TILE)
        dh_part_ref[:, cols] = across(d_gate_ref[...], w_gate[cols, :]) + across(d_up_ref[...], w_up[cols, :])
        y_part_ref[:, cols] = jnp.dot(act_ref[...], w_down[:, cols], preferred_element_type=f32)

    for idx in range(2):
        for way in range(2):
            for step in range(7):
                send(idx, way, step).wait_send()


def ring_mlp(collective_id, gate_sh, up_sh, down_a, down_b, h_full, dy_full):
    tokens, d_model = h_full.shape
    width = gate_sh.shape[1]
    sent = 14 * gate_sh.size * 2
    dma = pltpu.SemaphoreType.DMA
    vmem = pl.BlockSpec(memory_space=pltpu.VMEM)
    hbm = pl.BlockSpec(memory_space=pl.ANY)
    hidden = jax.ShapeDtypeStruct((tokens, width), jnp.bfloat16)
    partial_sum = jax.ShapeDtypeStruct((tokens, d_model), jnp.float32)
    return pl.pallas_call(
        mlp_kernel,
        out_shape=[hidden, hidden, hidden, partial_sum, partial_sum],
        in_specs=[hbm, hbm, hbm, hbm, vmem, vmem],
        out_specs=[vmem] * 5,
        scratch_shapes=[pltpu.VMEM((d_model, width), jnp.bfloat16), pltpu.VMEM((d_model, width), jnp.bfloat16),
                        pltpu.VMEM((width, d_model), jnp.bfloat16), pltpu.VMEM((tokens, width), jnp.float32),
                        pltpu.VMEM((tokens, width), jnp.float32), pltpu.VMEM((tokens, width), jnp.bfloat16),
                        dma((2, 2, 7)), dma((2, 2, 7)), dma((2, 2)), dma((2,))],
        compiler_params=pltpu.CompilerParams(collective_id=collective_id, has_side_effects=True,
                                             vmem_limit_bytes=60 * 1024 * 1024),
        cost_estimate=pl.CostEstimate(flops=sent * 3000, bytes_accessed=2 * sent, transcendentals=0),
        name=f'ring_mlp_{collective_id}',
    )(gate_sh, up_sh, down_a, down_b, h_full, dy_full)


def add_blocks(blocks):
    return (blocks[0] + blocks[1]) + (blocks[2] + blocks[3])


def solution(mesh):
    act_spec = P('fsdp', 'model', None)
    rows_spec = P('fsdp', 'model')
    cols_spec = P('model', 'fsdp')
    f32 = jnp.float32
    bf16 = jnp.bfloat16

    def device_fn(x_loc, dy_loc, gain_attn, gain_mlp, wqkv_sh, wout_sh, wgate_sh, wup_sh, wdown_sh, rope_cos, rope_sin):
        head_dim = 2 * rope_cos.shape[1]
        seq_full = rope_cos.shape[0]
        local_heads = wout_sh.shape[0] // head_dim
        local_kv = (wqkv_sh.shape[1] // head_dim - local_heads) // 2
        group_size = local_heads // local_kv
        rows = x_loc.shape[0]
        tokens = rows * seq_full
        scale = head_dim ** -0.5
        pos_ids = jnp.arange(seq_full)
        causal = pos_ids[:, None] >= pos_ids[None, :]
        cos_q = rope_cos[:, None, None, :]
        sin_q = rope_sin[:, None, None, :]
        cos_k = rope_cos[:, None, :]
        sin_k = rope_sin[:, None, :]

        x_f32 = x_loc.astype(f32)
        h_attn_f, norm_back_attn = jax.vjp(rms_scale, x_f32, gain_attn)
        h_attn_loc = h_attn_f.astype(bf16)
        w_qkv, w_out, h_attn_cols, dy_cols, h_attn, dy_full = ring_gather(
            0, [wqkv_sh, wout_sh], [0, 1], [h_attn_loc, dy_loc], [('seq', h_attn_loc), ('seq', dy_loc)])
        qkv = jnp.einsum('bsd,dc->bsc', h_attn, w_qkv, preferred_element_type=f32)
        qkv = qkv.reshape(rows, seq_full, local_kv, group_size + 2, head_dim)
        query = rotate(qkv[:, :, :, :group_size], cos_q, sin_q).astype(bf16)
        key_rot = rotate(qkv[:, :, :, group_size], cos_k, sin_k).astype(bf16)
        value = qkv[:, :, :, group_size + 1].astype(bf16)
        scores = jnp.einsum('bqkgd,btkd->bkgqt', query, key_rot, preferred_element_type=f32) * scale
        attn_prob = jax.nn.softmax(jnp.where(causal, scores, -1e30), axis=-1)
        prob_bf = attn_prob.astype(bf16)
        attn = jnp.einsum('bkgqt,btkd->bqkgd', prob_bf, value, preferred_element_type=f32)
        attn_flat = attn.astype(bf16).reshape(rows, seq_full, local_heads * head_dim)
        attn_part = jnp.einsum('bsh,hd->bsd', attn_flat, w_out, preferred_element_type=f32)
        half_down = wdown_sh.shape[0] // 2
        down_a, attn_red = ring_gather(1, [wdown_sh], [1], (), [('sum', attn_part)], spans=[(0, half_down)])
        attn_red = add_blocks(attn_red)
        mid_f32 = (x_f32 + attn_red.astype(bf16).astype(f32)).astype(bf16).astype(f32)
        h_mlp_f, norm_back_mlp = jax.vjp(rms_scale, mid_f32, gain_mlp)
        h_mlp_loc = h_mlp_f.astype(bf16)
        down_b, h_mlp_cols, h_mlp, h_attn_cols, dy_cols = ring_gather(
            2, [wdown_sh], [1], [h_mlp_loc], [('seq', h_mlp_loc), ('cols', h_attn_cols), ('cols', dy_cols)],
            spans=[(half_down, half_down)])
        gated_act, d_gate, d_up, mlp_part, dh_part = ring_mlp(
            7, wgate_sh, wup_sh, down_a, down_b, h_mlp.reshape(tokens, -1), dy_full.reshape(tokens, -1))
        mlp_part = mlp_part.reshape(rows, seq_full, -1)
        dh_part = dh_part.reshape(rows, seq_full, -1)
        act_all, dh_mlp, mlp_red, h_mlp_cols = ring_gather(
            3, [gated_act], [0], (), [('sum', dh_part), ('sum', mlp_part), ('cols', h_mlp_cols)])
        dh_mlp, mlp_red = add_blocks(dh_mlp), add_blocks(mlp_red)
        y_loc = (mid_f32 + mlp_red.astype(bf16).astype(f32)).astype(bf16)
        d_mid_norm, d_gain_mlp = norm_back_mlp(dh_mlp.astype(bf16).astype(f32))
        d_mid = (dy_loc.astype(f32) + d_mid_norm).astype(bf16)

        d_gate_all, attn_all, d_mid_cols, d_mid_full = ring_gather(
            4, [d_gate, attn_flat.reshape(tokens, -1)], [0, 0], [d_mid], [('seq', d_mid)])
        d_attn = jnp.einsum('bsd,hd->bsh', d_mid_full, w_out, preferred_element_type=f32).astype(bf16)
        d_attn = d_attn.reshape(rows, seq_full, local_kv, group_size, head_dim)
        d_prob = jnp.einsum('bqkgd,btkd->bkgqt', d_attn, value, preferred_element_type=f32)
        d_value = jnp.einsum('bkgqt,bqkgd->btkd', prob_bf, d_attn, preferred_element_type=f32)
        row_dot = jnp.sum(d_prob * attn_prob, axis=-1, keepdims=True)
        d_scores = (attn_prob * (d_prob - row_dot) * scale).astype(bf16)
        d_query = jnp.einsum('bkgqt,btkd->bqkgd', d_scores, key_rot, preferred_element_type=f32)
        d_key = jnp.einsum('bkgqt,bqkgd->btkd', d_scores, query, preferred_element_type=f32)
        d_qkv = jnp.concatenate([rotate_back(d_query, cos_q, sin_q),
                                 rotate_back(d_key, cos_k, sin_k)[:, :, :, None],
                                 d_value[:, :, :, None]], axis=3)
        d_qkv = d_qkv.astype(bf16).reshape(rows, seq_full, -1)
        dh_attn_part = jnp.einsum('bsc,dc->bsd', d_qkv, w_qkv, preferred_element_type=f32)
        d_up_all, dh_attn, d_mid_cols = ring_gather(
            5, [d_up], [0], (), [('sum', dh_attn_part), ('cols', d_mid_cols)])
        dh_attn = add_blocks(dh_attn)
        d_x_norm, d_gain_attn = norm_back_attn(dh_attn.astype(bf16).astype(f32))
        dx_loc = (d_mid.astype(f32) + d_x_norm).astype(bf16)
        gains = jnp.stack([d_gain_attn, d_gain_mlp]).reshape(16, -1)
        d_qkv_all, gains_all, _ = ring_gather(6, [d_qkv.reshape(tokens, -1)], [0], sums=[gains])
        gain_grads = jnp.sum(gains_all, axis=(0, 1)).reshape(2, -1)
        h_attn_cols, dy_cols, h_mlp_cols, d_mid_cols = [
            cols.reshape(8 * tokens, -1) for cols in (h_attn_cols, dy_cols, h_mlp_cols, d_mid_cols)]

        def pair(left, right):
            return lax.dot_general(left, right, (((0,), (0,)), ((), ())), preferred_element_type=f32)

        return (y_loc, dx_loc, gain_grads[0], gain_grads[1],
                pair(h_attn_cols, d_qkv_all), pair(attn_all, d_mid_cols),
                pair(h_mlp_cols, d_gate_all), pair(h_mlp_cols, d_up_all), pair(act_all, dy_cols))

    in_specs = (act_spec, act_spec, P(), P(), rows_spec, cols_spec, rows_spec, rows_spec, cols_spec, P(), P())
    out_specs = (act_spec, act_spec, P(), P(), rows_spec, cols_spec, rows_spec, rows_spec, cols_spec)
    return jax.shard_map(device_fn, mesh=mesh, in_specs=in_specs, out_specs=out_specs, check_vma=False)
```

```python
import functools

import jax
import jax.numpy as jnp
from jax import lax
from jax.experimental import pallas as pl
from jax.experimental.pallas import tpu as pltpu
from jax.sharding import PartitionSpec as P

NORM_EPS = 1e-5
MESH = pl.DeviceIdType.MESH


def rms_scale(x_f32, gain):
    inv_rms = lax.rsqrt(jnp.mean(x_f32 * x_f32, axis=-1, keepdims=True) + NORM_EPS)
    return x_f32 * inv_rms * gain


def rotate(tensor, cos_t, sin_t):
    half = tensor.shape[-1] // 2
    first = tensor[..., :half]
    second = tensor[..., half:]
    return jnp.concatenate([first * cos_t - second * sin_t, second * cos_t + first * sin_t], axis=-1)


def rotate_back(cotangent, cos_t, sin_t):
    half = cotangent.shape[-1] // 2
    first = cotangent[..., :half]
    second = cotangent[..., half:]
    return jnp.concatenate([first * cos_t + second * sin_t, second * cos_t - first * sin_t], axis=-1)


def ring_place(index):
    z, y = index // 2, index % 2
    return z + y * (7 - 2 * z)


def ring_device(place):
    y = place // 4
    return 2 * (place + y * (7 - 2 * place)) + y


def ring_kernel(dims, spans, slices, kinds, sums, *refs):
    count = len(dims)
    first_model = count + slices
    last = first_model + len(kinds)
    total = last + sums
    ins, outs = refs[:total], refs[total:2 * total]
    mix = refs[2 * total] if sums else None
    (send_sem, recv_sem, local_sem, slice_send, slice_recv, slice_local, mix_send, mix_recv, mix_local,
     model_send, model_recv, model_local) = refs[-12:]
    me = lax.axis_index('fsdp')
    me_model = lax.axis_index('model')
    place = ring_place(me)
    targets = (ring_device((place + 1) % 8), ring_device((place + 7) % 8))

    barrier = pltpu.get_barrier_semaphore()
    peers = [(me + hop) % 8 for hop in range(1, 8)] if slices else targets
    for peer in peers:
        pl.semaphore_signal(barrier, inc=1, device_id={'fsdp': peer}, device_id_type=MESH)
    if sums or kinds:
        for hop in range(1, 4):
            pl.semaphore_signal(barrier, inc=1, device_id={'model': (me_model + hop) % 4}, device_id_type=MESH)
    pl.semaphore_wait(barrier, len(peers) + (3 if sums or kinds else 0))

    def piece(idx, owner, way):
        if idx == count:
            return outs[last].at[owner, pl.ds(2 * way, 2)]
        half = spans[idx][1] // 2
        cols = ins[idx].shape[1]
        if dims[idx] == 0:
            start = pl.multiple_of(owner * (2 * half) + way * half, half)
            return outs[idx].at[pl.ds(start, half), :]
        return outs[idx].at[pl.ds(way * half, half), pl.ds(pl.multiple_of(owner * cols, cols), cols)]

    def source(idx, way):
        if idx == count:
            return mix.at[pl.ds(2 * way, 2)]
        start, length = spans[idx]
        return ins[idx].at[pl.ds(start + way * (length // 2), length // 2), :]

    def send(idx, way, step):
        owner = ring_device((place + (8 - step if way == 0 else step)) % 8)
        dst = piece(idx, owner, way)
        return pltpu.make_async_remote_copy(
            src_ref=source(idx, way) if step == 0 else dst, dst_ref=dst, send_sem=send_sem.at[idx, way, step],
            recv_sem=recv_sem.at[idx, way, step], device_id={'fsdp': targets[way]}, device_id_type=MESH)

    def landed(idx, way, step):
        owner = ring_device((place + (7 - step if way == 0 else step + 1)) % 8)
        dst = piece(idx, owner, way)
        return pltpu.make_async_remote_copy(
            src_ref=dst, dst_ref=dst, send_sem=send_sem.at[idx, way, step], recv_sem=recv_sem.at[idx, way, step],
            device_id={'fsdp': targets[way]}, device_id_type=MESH)

    def own(idx, way):
        return pltpu.make_async_copy(source(idx, way), piece(idx, me, way), local_sem.at[idx, way])

    def columns(idx, peer):
        src = ins[count + idx]
        width = src.shape[2] // 8
        return src.at[:, :, pl.ds(pl.multiple_of(peer * width, width), width)]

    def slice_out(idx, hop):
        peer = (me + hop) % 8
        return pltpu.make_async_remote_copy(
            src_ref=columns(idx, peer), dst_ref=outs[count + idx].at[me], send_sem=slice_send.at[idx, hop],
            recv_sem=slice_recv.at[idx, hop], device_id={'fsdp': peer}, device_id_type=MESH)

    def slice_in(idx, hop):
        slot = outs[count + idx].at[(me + 8 - hop) % 8]
        return pltpu.make_async_remote_copy(
            src_ref=slot, dst_ref=slot, send_sem=slice_send.at[idx, hop], recv_sem=slice_recv.at[idx, hop],
            device_id={'fsdp': (me + hop) % 8}, device_id_type=MESH)

    def slice_own(idx):
        return pltpu.make_async_copy(columns(idx, me), outs[count + idx].at[me], slice_local.at[idx])

    def mix_copy(hop, incoming):
        slot = mix.at[(me_model + 4 - hop) % 4 if incoming else me_model]
        return pltpu.make_async_remote_copy(
            src_ref=slot if incoming else ins[last], dst_ref=slot, send_sem=mix_send.at[hop],
            recv_sem=mix_recv.at[hop], device_id={'model': (me_model + hop) % 4}, device_id_type=MESH)

    def mix_own():
        return pltpu.make_async_copy(ins[last], mix.at[me_model], mix_local)

    def model_src(idx, peer):
        src = ins[first_model + idx]
        if kinds[idx] != 'sum':
            return src
        block = src.shape[1] // 4
        return src.at[:, pl.ds(pl.multiple_of(peer * block, block), block), :]

    def model_dst(idx, member):
        dst = outs[first_model + idx]
        if kinds[idx] == 'sum':
            return dst.at[member]
        if kinds[idx] == 'cols':
            return dst.at[:, :, member]
        block = dst.shape[1] // 4
        return dst.at[:, pl.ds(pl.multiple_of(member * block, block), block), :]

    def model_out(idx, hop):
        peer = (me_model + hop) % 4
        return pltpu.make_async_remote_copy(
            src_ref=model_src(idx, peer), dst_ref=model_dst(idx, me_model), send_sem=model_send.at[idx, hop],
            recv_sem=model_recv.at[idx, hop], device_id={'model': peer}, device_id_type=MESH)

    def model_in(idx, hop):
        slot = model_dst(idx, (me_model + 4 - hop) % 4)
        return pltpu.make_async_remote_copy(
            src_ref=slot, dst_ref=slot, send_sem=model_send.at[idx, hop], recv_sem=model_recv.at[idx, hop],
            device_id={'model': (me_model + hop) % 4}, device_id_type=MESH)

    def model_own(idx):
        return pltpu.make_async_copy(model_src(idx, me_model), model_dst(idx, me_model), model_local.at[idx])

    if sums:
        mix_own().start()
        for hop in range(1, 4):
            mix_copy(hop, False).start()
    for step in range(7):
        for idx in range(count + sums):
            for way in range(2):
                if step > 0:
                    landed(idx, way, step - 1).wait_recv()
                elif idx == count and way == 0:
                    mix_own().wait()
                    for hop in range(1, 4):
                        mix_copy(hop, True).wait_recv()
                        mix_copy(hop, False).wait_send()
                send(idx, way, step).start()
        if step == 0:
            for idx in range(slices):
                slice_own(idx).start()
                for hop in range(1, 8):
                    slice_out(idx, hop).start()
            for idx in range(len(kinds)):
                for hop in range(1, 4):
                    model_out(idx, hop).start()
                model_own(idx).start()
            for idx in range(count + sums):
                for way in range(2):
                    own(idx, way).start()
    for idx in range(count + sums):
        for way in range(2):
            landed(idx, way, 6).wait_recv()
            own(idx, way).wait()
            for step in range(7):
                send(idx, way, step).wait_send()
    for idx in range(slices):
        slice_own(idx).wait()
        for hop in range(1, 8):
            slice_in(idx, hop).wait_recv()
            slice_out(idx, hop).wait_send()
    for idx in range(len(kinds)):
        model_own(idx).wait()
        for hop in range(1, 4):
            model_in(idx, hop).wait_recv()
            model_out(idx, hop).wait_send()


def ring_gather(collective_id, arrays, dims, slices=(), model=(), sums=(), spans=None):
    shapes = []
    sent = 0
    spans = spans or [(0, array.shape[0]) for array in arrays]
    for array, dim, span in zip(arrays, dims, spans):
        rows, cols = span[1], array.shape[1]
        shapes.append(jax.ShapeDtypeStruct((8 * rows, cols) if dim == 0 else (rows, 8 * cols), array.dtype))
        sent += 7 * rows * cols * 2
    for array in slices:
        shapes.append(jax.ShapeDtypeStruct((8,) + array.shape[:2] + (array.shape[2] // 8,), array.dtype))
    for kind, array in model:
        if kind == 'sum':
            shape = (4, array.shape[0], array.shape[1] // 4, array.shape[2])
        elif kind == 'cols':
            shape = array.shape[:2] + (4,) + array.shape[2:]
        else:
            shape = (array.shape[0], 4 * array.shape[1], array.shape[2])
        shapes.append(jax.ShapeDtypeStruct(shape, array.dtype))
    for array in sums:
        shapes.append(jax.ShapeDtypeStruct((8, 4) + array.shape, array.dtype))
    n_in = len(shapes)
    for array in sums:
        shapes.append(jax.ShapeDtypeStruct((4,) + array.shape, array.dtype))
    count, n_slices, n_sums = len(arrays), len(slices), len(sums)
    dma = pltpu.SemaphoreType.DMA
    return pl.pallas_call(
        functools.partial(ring_kernel, tuple(dims), tuple(spans), n_slices, tuple(kind for kind, _ in model), n_sums),
        out_shape=shapes,
        in_specs=[pl.BlockSpec(memory_space=pl.ANY)] * n_in,
        out_specs=[pl.BlockSpec(memory_space=pl.ANY)] * len(shapes),
        scratch_shapes=[dma((count + n_sums, 2, 7)), dma((count + n_sums, 2, 7)), dma((count + n_sums, 2)),
                        dma((max(n_slices, 1), 8)), dma((max(n_slices, 1), 8)), dma((max(n_slices, 1),)),
                        dma((4,)), dma((4,)), dma, dma((max(len(model), 1), 4)), dma((max(len(model), 1), 4)),
                        dma((max(len(model), 1),))],
        compiler_params=pltpu.CompilerParams(collective_id=collective_id, has_side_effects=True),
        cost_estimate=pl.CostEstimate(flops=sent * 3000, bytes_accessed=2 * sent, transcendentals=0),
        name=f'ring_gather_{collective_id}',
    )(*arrays, *slices, *[array for _, array in model], *sums)


TILE = 512


def mlp_kernel(down_sh, gate_sh, up_sh, attn_part, cols_a, cols_b, x_ref, gain_ref, dy_ref,
               act_ref, d_gate_ref, d_up_ref, y_part_ref, dh_part_ref, mid_ref, h_cols, all_a, all_b,
               w_down, w_gate, w_up, gate_acc, up_acc, d_act, h_full, h_loc, blocks,
               send_sem, recv_sem, local_sem, block_send, block_recv, block_local, h_send, h_recv, h_local,
               slice_send, slice_recv, slice_local, cols_send, cols_recv, cols_local):
    f32, bf16 = jnp.float32, jnp.bfloat16
    me = lax.axis_index('fsdp')
    me_model = lax.axis_index('model')
    place = ring_place(me)
    targets = (ring_device((place + 1) % 8), ring_device((place + 7) % 8))
    barrier = pltpu.get_barrier_semaphore()
    for hop in range(1, 8):
        pl.semaphore_signal(barrier, inc=1, device_id={'fsdp': (me + hop) % 8}, device_id_type=MESH)
    for hop in range(1, 4):
        pl.semaphore_signal(barrier, inc=1, device_id={'model': (me_model + hop) % 4}, device_id_type=MESH)
    pl.semaphore_wait(barrier, 10)
    shards, weights, accs = (down_sh, gate_sh, up_sh), (w_down, w_gate, w_up), (None, gate_acc, up_acc)
    rows, width = gate_sh.shape
    half = rows // 2
    tall = down_sh.shape[0] // 2
    block_rows = x_ref.shape[1]
    slice_width = h_cols.shape[3]

    def start_of(owner, way):
        return pl.multiple_of(owner * rows + way * half, half)

    def piece(idx, owner, way):
        if idx == 0:
            return w_down.at[pl.ds(way * tall, tall), pl.ds(pl.multiple_of(owner * rows, rows), rows)]
        return weights[idx].at[pl.ds(start_of(owner, way), half), :]

    def source(idx, way):
        size = shards[idx].shape[0] // 2
        return shards[idx].at[pl.ds(way * size, size), :]

    def owner_at(way, step):
        return ring_device((place + (8 - step if way == 0 else step)) % 8)

    def send(idx, way, step):
        dst = piece(idx, owner_at(way, step), way)
        return pltpu.make_async_remote_copy(
            src_ref=source(idx, way) if isinstance(step, int) and step == 0 else dst, dst_ref=dst,
            send_sem=send_sem.at[idx, way, step], recv_sem=recv_sem.at[idx, way, step],
            device_id={'fsdp': targets[way]}, device_id_type=MESH)

    def landed(idx, way, step):
        dst = piece(idx, owner_at(way, step + 1), way)
        return pltpu.make_async_remote_copy(
            src_ref=dst, dst_ref=dst, send_sem=send_sem.at[idx, way, step], recv_sem=recv_sem.at[idx, way, step],
            device_id={'fsdp': targets[way]}, device_id_type=MESH)

    def own(idx, way):
        return pltpu.make_async_copy(source(idx, way), piece(idx, me, way), local_sem.at[idx, way])

    def to_member(src, dst, send_sems, recv_sems, hop):
        return pltpu.make_async_remote_copy(
            src_ref=src, dst_ref=dst, send_sem=send_sems, recv_sem=recv_sems,
            device_id={'model': (me_model + hop) % 4}, device_id_type=MESH)

    def block_of(member):
        return attn_part.at[:, pl.ds(pl.multiple_of(member * block_rows, block_rows), block_rows), :]

    def block_out(hop):
        return to_member(block_of((me_model + hop) % 4), blocks.at[me_model], block_send.at[hop], block_recv.at[hop], hop)

    def block_in(hop):
        slot = blocks.at[(me_model + 4 - hop) % 4]
        return to_member(slot, slot, block_send.at[hop], block_recv.at[hop], hop)

    def block_own():
        return pltpu.make_async_copy(block_of(me_model), blocks.at[me_model], block_local)

    def h_slot(member):
        return h_full.at[:, pl.ds(pl.multiple_of(member * block_rows, block_rows), block_rows), :]

    def h_out(hop):
        return to_member(h_loc, h_slot(me_model), h_send.at[hop], h_recv.at[hop], hop)

    def h_in(hop):
        slot = h_slot((me_model + 4 - hop) % 4)
        return to_member(slot, slot, h_send.at[hop], h_recv.at[hop], hop)

    def columns(peer):
        return h_loc.at[:, :, pl.ds(pl.multiple_of(peer * slice_width, slice_width), slice_width)]

    def slice_copy(hop, incoming):
        peer = (me + hop) % 8
        slot = h_cols.at[(me + 8 - hop) % 8 if incoming else me]
        return pltpu.make_async_remote_copy(
            src_ref=slot if incoming else columns(peer), dst_ref=slot, send_sem=slice_send.at[hop],
            recv_sem=slice_recv.at[hop], device_id={'fsdp': peer}, device_id_type=MESH)

    def slice_own():
        return pltpu.make_async_copy(columns(me), h_cols.at[me], slice_local)

    cols_in, cols_all = (cols_a, cols_b), (all_a, all_b)

    def cols_copy(idx, hop, incoming):
        slot = cols_all[idx].at[:, :, (me_model + 4 - hop) % 4 if incoming else me_model]
        return to_member(slot if incoming else cols_in[idx], slot, cols_send.at[idx, hop], cols_recv.at[idx, hop], hop)

    def cols_own(idx):
        return pltpu.make_async_copy(cols_in[idx], cols_all[idx].at[:, :, me_model], cols_local.at[idx])

    def accumulate(step):
        for way in range(2):
            start = start_of(owner_at(way, step), way)
            h_block = h_full[:, :, pl.ds(start, half)].reshape(dy_ref.shape[0], half)
            for idx in (1, 2):
                @pl.loop(0, width // TILE)
                def _(tile):
                    cols = pl.ds(pl.multiple_of(tile * TILE, TILE), TILE)
                    accs[idx][:, cols] += jnp.dot(h_block, weights[idx][pl.ds(start, half), cols],
                                                  preferred_element_type=f32)

    def across(left, right):
        return lax.dot_general(left, right, (((1,), (1,)), ((), ())), preferred_element_type=f32)

    for way in range(2):
        send(0, way, 0).start()
    for hop in range(1, 4):
        block_out(hop).start()
    block_own().start()
    for idx in range(3):
        for way in range(2):
            own(idx, way).start()
    for idx in range(2):
        for hop in range(1, 4):
            cols_copy(idx, hop, False).start()
        cols_own(idx).start()
    gate_acc[...] = jnp.zeros_like(gate_acc)
    up_acc[...] = jnp.zeros_like(up_acc)

    for step in range(1, 7):
        for way in range(2):
            landed(0, way, step - 1).wait_recv()
            send(0, way, step).start()
        if step == 2:
            block_own().wait()
            for hop in range(1, 4):
                block_in(hop).wait_recv()
                block_out(hop).wait_send()

            @pl.loop(0, block_rows // 16)
            def _(group):
                at = pl.ds(pl.multiple_of(group * 16, 16), 16)
                for seq in range(x_ref.shape[0]):
                    total = (blocks[0, seq, at, :] + blocks[1, seq, at, :]) + (blocks[2, seq, at, :] + blocks[3, seq, at, :])
                    mid = (x_ref[seq, at, :].astype(f32) + total.astype(bf16).astype(f32)).astype(bf16)
                    mid_ref[seq, at, :] = mid
                    mid = mid.astype(f32)
                    inv_rms = lax.rsqrt(jnp.mean(mid * mid, axis=-1, keepdims=True) + NORM_EPS)
                    h_loc[seq, at, :] = (mid * inv_rms * gain_ref[...]).astype(bf16)
        if step == 3:
            for hop in range(1, 4):
                h_out(hop).start()
            pltpu.make_async_copy(h_loc, h_slot(me_model), h_local).start()
            slice_own().start()
            for hop in range(1, 8):
                slice_copy(hop, False).start()
    for idx in (1, 2):
        for way in range(2):
            send(idx, way, 0).start()
    pltpu.make_async_copy(h_loc, h_slot(me_model), h_local).wait()
    for hop in range(1, 4):
        h_in(hop).wait_recv()
    for way in range(2):
        landed(0, way, 6).wait_recv()
        own(0, way).wait()

    @pl.loop(0, width // TILE)
    def _(tile):
        cols = pl.ds(pl.multiple_of(tile * TILE, TILE), TILE)
        d_act[:, cols] = across(dy_ref[...], w_down[cols, :]).astype(bf16)

    for idx in (1, 2):
        for way in range(2):
            own(idx, way).wait()
    accumulate(0)

    @pl.loop(1, 7)
    def _(step):
        for idx in (1, 2):
            for way in range(2):
                landed(idx, way, step - 1).wait_recv()
                send(idx, way, step).start()
        accumulate(step)

    for idx in (1, 2):
        for way in range(2):
            landed(idx, way, 6).wait_recv()
    accumulate(7)

    @pl.loop(0, width // 256)
    def _(tile):
        cols = pl.ds(pl.multiple_of(tile * 256, 256), 256)
        gate, up_proj = gate_acc[:, cols], up_acc[:, cols]
        d_val = d_act[:, cols].astype(f32)
        sig_gate = jax.nn.sigmoid(gate)
        silu_gate = gate * sig_gate
        act_ref[:, cols] = (silu_gate * up_proj).astype(bf16)
        d_gate_ref[:, cols] = (d_val * up_proj * sig_gate * (1.0 + gate * (1.0 - sig_gate))).astype(bf16)
        d_up_ref[:, cols] = (d_val * silu_gate).astype(bf16)

    @pl.loop(0, width // TILE)
    def _(tile):
        cols = pl.ds(pl.multiple_of(tile * TILE, TILE), TILE)
        dh_part_ref[:, cols] = across(d_gate_ref[...], w_gate[cols, :]) + across(d_up_ref[...], w_up[cols, :])
        y_part_ref[:, cols] = jnp.dot(act_ref[...], w_down[:, cols], preferred_element_type=f32)

    for idx in range(3):
        for way in range(2):
            for step in range(7):
                send(idx, way, step).wait_send()
    slice_own().wait()
    for hop in range(1, 8):
        slice_copy(hop, True).wait_recv()
        slice_copy(hop, False).wait_send()
    for hop in range(1, 4):
        h_out(hop).wait_send()
    for idx in range(2):
        cols_own(idx).wait()
        for hop in range(1, 4):
            cols_copy(idx, hop, True).wait_recv()
            cols_copy(idx, hop, False).wait_send()


def ring_mlp(collective_id, down_sh, gate_sh, up_sh, attn_part, cols_a, cols_b, x_loc, gain, dy_full):
    tokens, d_model = dy_full.shape
    width = gate_sh.shape[1]
    sent = 21 * gate_sh.size * 2
    dma = pltpu.SemaphoreType.DMA
    vmem = pl.BlockSpec(memory_space=pltpu.VMEM)
    hbm = pl.BlockSpec(memory_space=pl.ANY)
    bf16, f32 = jnp.bfloat16, jnp.float32
    hidden = jax.ShapeDtypeStruct((tokens, width), bf16)
    partial_sum = jax.ShapeDtypeStruct((tokens, d_model), f32)
    sliced = jax.ShapeDtypeStruct(cols_a.shape, bf16)
    spread = jax.ShapeDtypeStruct(cols_a.shape[:2] + (4,) + cols_a.shape[2:], bf16)
    return pl.pallas_call(
        mlp_kernel,
        out_shape=[hidden, hidden, hidden, partial_sum, partial_sum, jax.ShapeDtypeStruct(x_loc.shape, bf16),
                   sliced, spread, spread],
        in_specs=[hbm] * 6 + [vmem] * 3,
        out_specs=[vmem] * 6 + [hbm] * 3,
        scratch_shapes=[pltpu.VMEM((width, d_model), bf16), pltpu.VMEM((d_model, width), bf16),
                        pltpu.VMEM((d_model, width), bf16), pltpu.VMEM((tokens, width), f32),
                        pltpu.VMEM((tokens, width), f32), pltpu.VMEM((tokens, width), bf16),
                        pltpu.VMEM(attn_part.shape, bf16), pltpu.VMEM(x_loc.shape, bf16),
                        pltpu.VMEM((4,) + x_loc.shape, f32),
                        dma((3, 2, 7)), dma((3, 2, 7)), dma((3, 2)), dma((4,)), dma((4,)), dma, dma((4,)), dma((4,)), dma,
                        dma((8,)), dma((8,)), dma, dma((2, 4)), dma((2, 4)), dma((2,))],
        compiler_params=pltpu.CompilerParams(collective_id=collective_id, has_side_effects=True,
                                             vmem_limit_bytes=60 * 1024 * 1024),
        cost_estimate=pl.CostEstimate(flops=sent * 3000, bytes_accessed=2 * sent, transcendentals=0),
        name=f'ring_mlp_{collective_id}',
    )(down_sh, gate_sh, up_sh, attn_part, cols_a, cols_b, x_loc, gain, dy_full)


def add_blocks(blocks):
    return (blocks[0] + blocks[1]) + (blocks[2] + blocks[3])


def solution(mesh):
    act_spec = P('fsdp', 'model', None)
    rows_spec = P('fsdp', 'model')
    cols_spec = P('model', 'fsdp')
    f32 = jnp.float32
    bf16 = jnp.bfloat16

    def device_fn(x_loc, dy_loc, gain_attn, gain_mlp, wqkv_sh, wout_sh, wgate_sh, wup_sh, wdown_sh, rope_cos, rope_sin):
        head_dim = 2 * rope_cos.shape[1]
        seq_full = rope_cos.shape[0]
        local_heads = wout_sh.shape[0] // head_dim
        local_kv = (wqkv_sh.shape[1] // head_dim - local_heads) // 2
        group_size = local_heads // local_kv
        rows = x_loc.shape[0]
        tokens = rows * seq_full
        scale = head_dim ** -0.5
        pos_ids = jnp.arange(seq_full)
        causal = pos_ids[:, None] >= pos_ids[None, :]
        cos_q = rope_cos[:, None, None, :]
        sin_q = rope_sin[:, None, None, :]
        cos_k = rope_cos[:, None, :]
        sin_k = rope_sin[:, None, :]

        x_f32 = x_loc.astype(f32)
        h_attn_f, norm_back_attn = jax.vjp(rms_scale, x_f32, gain_attn)
        h_attn_loc = h_attn_f.astype(bf16)
        w_qkv, w_out, h_attn_cols, dy_cols, h_attn, dy_full = ring_gather(
            0, [wqkv_sh, wout_sh], [0, 1], [h_attn_loc, dy_loc], [('seq', h_attn_loc), ('seq', dy_loc)])
        qkv = jnp.einsum('bsd,dc->bsc', h_attn, w_qkv, preferred_element_type=f32)
        qkv = qkv.reshape(rows, seq_full, local_kv, group_size + 2, head_dim)
        query = rotate(qkv[:, :, :, :group_size], cos_q, sin_q).astype(bf16)
        key_rot = rotate(qkv[:, :, :, group_size], cos_k, sin_k).astype(bf16)
        value = qkv[:, :, :, group_size + 1].astype(bf16)
        scores = jnp.einsum('bqkgd,btkd->bkgqt', query, key_rot, preferred_element_type=f32) * scale
        attn_prob = jax.nn.softmax(jnp.where(causal, scores, -1e30), axis=-1)
        prob_bf = attn_prob.astype(bf16)
        attn = jnp.einsum('bkgqt,btkd->bqkgd', prob_bf, value, preferred_element_type=f32)
        attn_flat = attn.astype(bf16).reshape(rows, seq_full, local_heads * head_dim)
        attn_part = jnp.einsum('bsh,hd->bsd', attn_flat, w_out, preferred_element_type=f32)
        gated_act, d_gate, d_up, mlp_part, dh_part, mid, h_mlp_cols, h_attn_cols, dy_cols = ring_mlp(
            1, wdown_sh, wgate_sh, wup_sh, attn_part, h_attn_cols, dy_cols, x_loc, gain_mlp.reshape(1, -1),
            dy_full.reshape(tokens, -1))
        mid_f32 = mid.astype(f32)
        _, norm_back_mlp = jax.vjp(rms_scale, mid_f32, gain_mlp)
        mlp_part = mlp_part.reshape(rows, seq_full, -1)
        dh_part = dh_part.reshape(rows, seq_full, -1)
        act_all, dh_mlp, mlp_red, h_mlp_cols = ring_gather(
            3, [gated_act], [0], (), [('sum', dh_part), ('sum', mlp_part), ('cols', h_mlp_cols)])
        dh_mlp, mlp_red = add_blocks(dh_mlp), add_blocks(mlp_red)
        y_loc = (mid_f32 + mlp_red.astype(bf16).astype(f32)).astype(bf16)
        d_mid_norm, d_gain_mlp = norm_back_mlp(dh_mlp.astype(bf16).astype(f32))
        d_mid = (dy_loc.astype(f32) + d_mid_norm).astype(bf16)

        d_gate_all, attn_all, d_mid_cols, d_mid_full = ring_gather(
            4, [d_gate, attn_flat.reshape(tokens, -1)], [0, 0], [d_mid], [('seq', d_mid)])
        d_attn = jnp.einsum('bsd,hd->bsh', d_mid_full, w_out, preferred_element_type=f32).astype(bf16)
        d_attn = d_attn.reshape(rows, seq_full, local_kv, group_size, head_dim)
        d_prob = jnp.einsum('bqkgd,btkd->bkgqt', d_attn, value, preferred_element_type=f32)
        d_value = jnp.einsum('bkgqt,bqkgd->btkd', prob_bf, d_attn, preferred_element_type=f32)
        row_dot = jnp.sum(d_prob * attn_prob, axis=-1, keepdims=True)
        d_scores = (attn_prob * (d_prob - row_dot) * scale).astype(bf16)
        d_query = jnp.einsum('bkgqt,btkd->bqkgd', d_scores, key_rot, preferred_element_type=f32)
        d_key = jnp.einsum('bkgqt,bqkgd->btkd', d_scores, query, preferred_element_type=f32)
        d_qkv = jnp.concatenate([rotate_back(d_query, cos_q, sin_q),
                                 rotate_back(d_key, cos_k, sin_k)[:, :, :, None],
                                 d_value[:, :, :, None]], axis=3)
        d_qkv = d_qkv.astype(bf16).reshape(rows, seq_full, -1)
        dh_attn_part = jnp.einsum('bsc,dc->bsd', d_qkv, w_qkv, preferred_element_type=f32)
        d_up_all, dh_attn, d_mid_cols = ring_gather(
            5, [d_up], [0], (), [('sum', dh_attn_part), ('cols', d_mid_cols)])
        dh_attn = add_blocks(dh_attn)
        d_x_norm, d_gain_attn = norm_back_attn(dh_attn.astype(bf16).astype(f32))
        dx_loc = (d_mid.astype(f32) + d_x_norm).astype(bf16)
        gains = jnp.stack([d_gain_attn, d_gain_mlp]).reshape(16, -1)
        d_qkv_all, gains_all, _ = ring_gather(6, [d_qkv.reshape(tokens, -1)], [0], sums=[gains])
        gain_grads = jnp.sum(gains_all, axis=(0, 1)).reshape(2, -1)
        h_attn_cols, dy_cols, h_mlp_cols, d_mid_cols = [
            cols.reshape(8 * tokens, -1) for cols in (h_attn_cols, dy_cols, h_mlp_cols, d_mid_cols)]

        def pair(left, right):
            return lax.dot_general(left, right, (((0,), (0,)), ((), ())), preferred_element_type=f32)

        return (y_loc, dx_loc, gain_grads[0], gain_grads[1],
                pair(h_attn_cols, d_qkv_all), pair(attn_all, d_mid_cols),
                pair(h_mlp_cols, d_gate_all), pair(h_mlp_cols, d_up_all), pair(act_all, dy_cols))

    in_specs = (act_spec, act_spec, P(), P(), rows_spec, cols_spec, rows_spec, rows_spec, cols_spec, P(), P())
    out_specs = (act_spec, act_spec, P(), P(), rows_spec, cols_spec, rows_spec, rows_spec, cols_spec)
    return jax.shard_map(device_fn, mesh=mesh, in_specs=in_specs, out_specs=out_specs, check_vma=False)
```

```python
import functools

import jax
import jax.numpy as jnp
from jax import lax
from jax.experimental import pallas as pl
from jax.experimental.pallas import tpu as pltpu
from jax.sharding import PartitionSpec as P

NORM_EPS = 1e-5
MESH = pl.DeviceIdType.MESH


def rms_scale(x_f32, gain):
    inv_rms = lax.rsqrt(jnp.mean(x_f32 * x_f32, axis=-1, keepdims=True) + NORM_EPS)
    return x_f32 * inv_rms * gain


def rotate(tensor, cos_t, sin_t):
    half = tensor.shape[-1] // 2
    first = tensor[..., :half]
    second = tensor[..., half:]
    return jnp.concatenate([first * cos_t - second * sin_t, second * cos_t + first * sin_t], axis=-1)


def ring_place(index):
    z, y = index // 2, index % 2
    return z + y * (7 - 2 * z)


def ring_device(place):
    y = place // 4
    return 2 * (place + y * (7 - 2 * place)) + y


def ring_kernel(dims, spans, slices, kinds, sums, *refs):
    count = len(dims)
    first_model = count + slices
    last = first_model + len(kinds)
    total = last + sums
    ins, outs = refs[:total], refs[total:2 * total]
    mix = refs[2 * total] if sums else None
    (send_sem, recv_sem, local_sem, slice_send, slice_recv, slice_local, mix_send, mix_recv, mix_local,
     model_send, model_recv, model_local) = refs[-12:]
    me = lax.axis_index('fsdp')
    me_model = lax.axis_index('model')
    place = ring_place(me)
    targets = (ring_device((place + 1) % 8), ring_device((place + 7) % 8))

    barrier = pltpu.get_barrier_semaphore()
    peers = [(me + hop) % 8 for hop in range(1, 8)] if slices else targets
    for peer in peers:
        pl.semaphore_signal(barrier, inc=1, device_id={'fsdp': peer}, device_id_type=MESH)
    if sums or kinds:
        for hop in range(1, 4):
            pl.semaphore_signal(barrier, inc=1, device_id={'model': (me_model + hop) % 4}, device_id_type=MESH)
    pl.semaphore_wait(barrier, len(peers) + (3 if sums or kinds else 0))

    def piece(idx, owner, way):
        if idx == count:
            return outs[last].at[owner, pl.ds(2 * way, 2)]
        half = spans[idx][1] // 2
        cols = ins[idx].shape[1]
        if dims[idx] == 0:
            start = pl.multiple_of(owner * (2 * half) + way * half, half)
            return outs[idx].at[pl.ds(start, half), :]
        return outs[idx].at[pl.ds(way * half, half), pl.ds(pl.multiple_of(owner * cols, cols), cols)]

    def source(idx, way):
        if idx == count:
            return mix.at[pl.ds(2 * way, 2)]
        start, length = spans[idx]
        return ins[idx].at[pl.ds(start + way * (length // 2), length // 2), :]

    def send(idx, way, step):
        owner = ring_device((place + (8 - step if way == 0 else step)) % 8)
        dst = piece(idx, owner, way)
        return pltpu.make_async_remote_copy(
            src_ref=source(idx, way) if step == 0 else dst, dst_ref=dst, send_sem=send_sem.at[idx, way, step],
            recv_sem=recv_sem.at[idx, way, step], device_id={'fsdp': targets[way]}, device_id_type=MESH)

    def landed(idx, way, step):
        owner = ring_device((place + (7 - step if way == 0 else step + 1)) % 8)
        dst = piece(idx, owner, way)
        return pltpu.make_async_remote_copy(
            src_ref=dst, dst_ref=dst, send_sem=send_sem.at[idx, way, step], recv_sem=recv_sem.at[idx, way, step],
            device_id={'fsdp': targets[way]}, device_id_type=MESH)

    def own(idx, way):
        return pltpu.make_async_copy(source(idx, way), piece(idx, me, way), local_sem.at[idx, way])

    def columns(idx, peer):
        src = ins[count + idx]
        width = src.shape[2] // 8
        return src.at[:, :, pl.ds(pl.multiple_of(peer * width, width), width)]

    def slice_out(idx, hop):
        peer = (me + hop) % 8
        return pltpu.make_async_remote_copy(
            src_ref=columns(idx, peer), dst_ref=outs[count + idx].at[me], send_sem=slice_send.at[idx, hop],
            recv_sem=slice_recv.at[idx, hop], device_id={'fsdp': peer}, device_id_type=MESH)

    def slice_in(idx, hop):
        slot = outs[count + idx].at[(me + 8 - hop) % 8]
        return pltpu.make_async_remote_copy(
            src_ref=slot, dst_ref=slot, send_sem=slice_send.at[idx, hop], recv_sem=slice_recv.at[idx, hop],
            device_id={'fsdp': (me + hop) % 8}, device_id_type=MESH)

    def slice_own(idx):
        return pltpu.make_async_copy(columns(idx, me), outs[count + idx].at[me], slice_local.at[idx])

    def mix_copy(hop, incoming):
        slot = mix.at[(me_model + 4 - hop) % 4 if incoming else me_model]
        return pltpu.make_async_remote_copy(
            src_ref=slot if incoming else ins[last], dst_ref=slot, send_sem=mix_send.at[hop],
            recv_sem=mix_recv.at[hop], device_id={'model': (me_model + hop) % 4}, device_id_type=MESH)

    def mix_own():
        return pltpu.make_async_copy(ins[last], mix.at[me_model], mix_local)

    def model_src(idx, peer):
        src = ins[first_model + idx]
        if kinds[idx] != 'sum':
            return src
        block = src.shape[1] // 4
        return src.at[:, pl.ds(pl.multiple_of(peer * block, block), block), :]

    def model_dst(idx, member):
        dst = outs[first_model + idx]
        if kinds[idx] == 'sum':
            return dst.at[member]
        if kinds[idx] == 'cols':
            return dst.at[:, :, member]
        block = dst.shape[1] // 4
        return dst.at[:, pl.ds(pl.multiple_of(member * block, block), block), :]

    def model_out(idx, hop):
        peer = (me_model + hop) % 4
        return pltpu.make_async_remote_copy(
            src_ref=model_src(idx, peer), dst_ref=model_dst(idx, me_model), send_sem=model_send.at[idx, hop],
            recv_sem=model_recv.at[idx, hop], device_id={'model': peer}, device_id_type=MESH)

    def model_in(idx, hop):
        slot = model_dst(idx, (me_model + 4 - hop) % 4)
        return pltpu.make_async_remote_copy(
            src_ref=slot, dst_ref=slot, send_sem=model_send.at[idx, hop], recv_sem=model_recv.at[idx, hop],
            device_id={'model': (me_model + hop) % 4}, device_id_type=MESH)

    def model_own(idx):
        return pltpu.make_async_copy(model_src(idx, me_model), model_dst(idx, me_model), model_local.at[idx])

    if sums:
        mix_own().start()
        for hop in range(1, 4):
            mix_copy(hop, False).start()
    for step in range(7):
        for idx in range(count + sums):
            for way in range(2):
                if step > 0:
                    landed(idx, way, step - 1).wait_recv()
                elif idx == count and way == 0:
                    mix_own().wait()
                    for hop in range(1, 4):
                        mix_copy(hop, True).wait_recv()
                        mix_copy(hop, False).wait_send()
                send(idx, way, step).start()
        if step == 0:
            for idx in range(slices):
                slice_own(idx).start()
                for hop in range(1, 8):
                    slice_out(idx, hop).start()
            for idx in range(len(kinds)):
                for hop in range(1, 4):
                    model_out(idx, hop).start()
                model_own(idx).start()
            for idx in range(count + sums):
                for way in range(2):
                    own(idx, way).start()
    for idx in range(count + sums):
        for way in range(2):
            landed(idx, way, 6).wait_recv()
            own(idx, way).wait()
            for step in range(7):
                send(idx, way, step).wait_send()
    for idx in range(slices):
        slice_own(idx).wait()
        for hop in range(1, 8):
            slice_in(idx, hop).wait_recv()
            slice_out(idx, hop).wait_send()
    for idx in range(len(kinds)):
        model_own(idx).wait()
        for hop in range(1, 4):
            model_in(idx, hop).wait_recv()
            model_out(idx, hop).wait_send()


def ring_gather(collective_id, arrays, dims, slices=(), model=(), sums=(), spans=None):
    shapes = []
    sent = 0
    spans = spans or [(0, array.shape[0]) for array in arrays]
    for array, dim, span in zip(arrays, dims, spans):
        rows, cols = span[1], array.shape[1]
        shapes.append(jax.ShapeDtypeStruct((8 * rows, cols) if dim == 0 else (rows, 8 * cols), array.dtype))
        sent += 7 * rows * cols * 2
    for array in slices:
        shapes.append(jax.ShapeDtypeStruct((8,) + array.shape[:2] + (array.shape[2] // 8,), array.dtype))
    for kind, array in model:
        if kind == 'sum':
            shape = (4, array.shape[0], array.shape[1] // 4, array.shape[2])
        elif kind == 'cols':
            shape = array.shape[:2] + (4,) + array.shape[2:]
        else:
            shape = (array.shape[0], 4 * array.shape[1], array.shape[2])
        shapes.append(jax.ShapeDtypeStruct(shape, array.dtype))
    for array in sums:
        shapes.append(jax.ShapeDtypeStruct((8, 4) + array.shape, array.dtype))
    n_in = len(shapes)
    for array in sums:
        shapes.append(jax.ShapeDtypeStruct((4,) + array.shape, array.dtype))
    count, n_slices, n_sums = len(arrays), len(slices), len(sums)
    dma = pltpu.SemaphoreType.DMA
    return pl.pallas_call(
        functools.partial(ring_kernel, tuple(dims), tuple(spans), n_slices, tuple(kind for kind, _ in model), n_sums),
        out_shape=shapes,
        in_specs=[pl.BlockSpec(memory_space=pl.ANY)] * n_in,
        out_specs=[pl.BlockSpec(memory_space=pl.ANY)] * len(shapes),
        scratch_shapes=[dma((count + n_sums, 2, 7)), dma((count + n_sums, 2, 7)), dma((count + n_sums, 2)),
                        dma((max(n_slices, 1), 8)), dma((max(n_slices, 1), 8)), dma((max(n_slices, 1),)),
                        dma((4,)), dma((4,)), dma, dma((max(len(model), 1), 4)), dma((max(len(model), 1), 4)),
                        dma((max(len(model), 1),))],
        compiler_params=pltpu.CompilerParams(collective_id=collective_id, has_side_effects=True),
        cost_estimate=pl.CostEstimate(flops=sent * 3000, bytes_accessed=2 * sent, transcendentals=0),
        name=f'ring_gather_{collective_id}',
    )(*arrays, *slices, *[array for _, array in model], *sums)


TILE = 512


def mlp_kernel(down_sh, gate_sh, up_sh, attn_part, cols_a, cols_b, x_ref, gain_ref, dy_ref,
               act_ref, d_gate_ref, d_up_ref, y_part_ref, dh_part_ref, mid_ref, h_cols, all_a, all_b,
               w_down, w_gate, w_up, gate_acc, up_acc, d_act, h_full, h_loc, blocks,
               send_sem, recv_sem, local_sem, block_send, block_recv, block_local, h_send, h_recv, h_local,
               slice_send, slice_recv, slice_local, cols_send, cols_recv, cols_local):
    f32, bf16 = jnp.float32, jnp.bfloat16
    me = lax.axis_index('fsdp')
    me_model = lax.axis_index('model')
    place = ring_place(me)
    targets = (ring_device((place + 1) % 8), ring_device((place + 7) % 8))
    barrier = pltpu.get_barrier_semaphore()
    for hop in range(1, 8):
        pl.semaphore_signal(barrier, inc=1, device_id={'fsdp': (me + hop) % 8}, device_id_type=MESH)
    for hop in range(1, 4):
        pl.semaphore_signal(barrier, inc=1, device_id={'model': (me_model + hop) % 4}, device_id_type=MESH)
    pl.semaphore_wait(barrier, 10)
    shards, weights, accs = (down_sh, gate_sh, up_sh), (w_down, w_gate, w_up), (None, gate_acc, up_acc)
    rows, width = gate_sh.shape
    half = rows // 2
    tall = down_sh.shape[0] // 2
    block_rows = x_ref.shape[1]
    slice_width = h_cols.shape[3]

    def start_of(owner, way):
        return pl.multiple_of(owner * rows + way * half, half)

    def piece(idx, owner, way):
        if idx == 0:
            return w_down.at[pl.ds(way * tall, tall), pl.ds(pl.multiple_of(owner * rows, rows), rows)]
        return weights[idx].at[pl.ds(start_of(owner, way), half), :]

    def source(idx, way):
        size = shards[idx].shape[0] // 2
        return shards[idx].at[pl.ds(way * size, size), :]

    def owner_at(way, step):
        return ring_device((place + (8 - step if way == 0 else step)) % 8)

    def send(idx, way, step):
        dst = piece(idx, owner_at(way, step), way)
        return pltpu.make_async_remote_copy(
            src_ref=source(idx, way) if isinstance(step, int) and step == 0 else dst, dst_ref=dst,
            send_sem=send_sem.at[idx, way, step], recv_sem=recv_sem.at[idx, way, step],
            device_id={'fsdp': targets[way]}, device_id_type=MESH)

    def landed(idx, way, step):
        dst = piece(idx, owner_at(way, step + 1), way)
        return pltpu.make_async_remote_copy(
            src_ref=dst, dst_ref=dst, send_sem=send_sem.at[idx, way, step], recv_sem=recv_sem.at[idx, way, step],
            device_id={'fsdp': targets[way]}, device_id_type=MESH)

    def own(idx, way):
        return pltpu.make_async_copy(source(idx, way), piece(idx, me, way), local_sem.at[idx, way])

    def to_member(src, dst, send_sems, recv_sems, hop):
        return pltpu.make_async_remote_copy(
            src_ref=src, dst_ref=dst, send_sem=send_sems, recv_sem=recv_sems,
            device_id={'model': (me_model + hop) % 4}, device_id_type=MESH)

    def block_of(member):
        return attn_part.at[:, pl.ds(pl.multiple_of(member * block_rows, block_rows), block_rows), :]

    def block_out(hop):
        return to_member(block_of((me_model + hop) % 4), blocks.at[me_model], block_send.at[hop], block_recv.at[hop], hop)

    def block_in(hop):
        slot = blocks.at[(me_model + 4 - hop) % 4]
        return to_member(slot, slot, block_send.at[hop], block_recv.at[hop], hop)

    def block_own():
        return pltpu.make_async_copy(block_of(me_model), blocks.at[me_model], block_local)

    def h_slot(member):
        return h_full.at[:, pl.ds(pl.multiple_of(member * block_rows, block_rows), block_rows), :]

    def h_out(hop):
        return to_member(h_loc, h_slot(me_model), h_send.at[hop], h_recv.at[hop], hop)

    def h_in(hop):
        slot = h_slot((me_model + 4 - hop) % 4)
        return to_member(slot, slot, h_send.at[hop], h_recv.at[hop], hop)

    def columns(peer):
        return h_loc.at[:, :, pl.ds(pl.multiple_of(peer * slice_width, slice_width), slice_width)]

    def slice_copy(hop, incoming):
        peer = (me + hop) % 8
        slot = h_cols.at[(me + 8 - hop) % 8 if incoming else me]
        return pltpu.make_async_remote_copy(
            src_ref=slot if incoming else columns(peer), dst_ref=slot, send_sem=slice_send.at[hop],
            recv_sem=slice_recv.at[hop], device_id={'fsdp': peer}, device_id_type=MESH)

    def slice_own():
        return pltpu.make_async_copy(columns(me), h_cols.at[me], slice_local)

    cols_in, cols_all = (cols_a, cols_b), (all_a, all_b)

    def cols_copy(idx, hop, incoming):
        slot = cols_all[idx].at[:, :, (me_model + 4 - hop) % 4 if incoming else me_model]
        return to_member(slot if incoming else cols_in[idx], slot, cols_send.at[idx, hop], cols_recv.at[idx, hop], hop)

    def cols_own(idx):
        return pltpu.make_async_copy(cols_in[idx], cols_all[idx].at[:, :, me_model], cols_local.at[idx])

    def accumulate(step):
        for way in range(2):
            start = start_of(owner_at(way, step), way)
            h_block = h_full[:, :, pl.ds(start, half)].reshape(dy_ref.shape[0], half)
            for idx in (1, 2):
                @pl.loop(0, width // TILE)
                def _(tile):
                    cols = pl.ds(pl.multiple_of(tile * TILE, TILE), TILE)
                    accs[idx][:, cols] += jnp.dot(h_block, weights[idx][pl.ds(start, half), cols],
                                                  preferred_element_type=f32)

    def across(left, right):
        return lax.dot_general(left, right, (((1,), (1,)), ((), ())), preferred_element_type=f32)

    for way in range(2):
        send(0, way, 0).start()
    for hop in range(1, 4):
        block_out(hop).start()
    block_own().start()
    for idx in range(3):
        for way in range(2):
            own(idx, way).start()
    for idx in range(2):
        for hop in range(1, 4):
            cols_copy(idx, hop, False).start()
        cols_own(idx).start()
    gate_acc[...] = jnp.zeros_like(gate_acc)
    up_acc[...] = jnp.zeros_like(up_acc)

    for step in range(1, 7):
        for way in range(2):
            landed(0, way, step - 1).wait_recv()
            send(0, way, step).start()
        if step == 2:
            block_own().wait()
            for hop in range(1, 4):
                block_in(hop).wait_recv()
                block_out(hop).wait_send()

            @pl.loop(0, block_rows // 16)
            def _(group):
                at = pl.ds(pl.multiple_of(group * 16, 16), 16)
                for seq in range(x_ref.shape[0]):
                    total = (blocks[0, seq, at, :] + blocks[1, seq, at, :]) + (blocks[2, seq, at, :] + blocks[3, seq, at, :])
                    mid = (x_ref[seq, at, :].astype(f32) + total.astype(bf16).astype(f32)).astype(bf16)
                    mid_ref[seq, at, :] = mid
                    mid = mid.astype(f32)
                    inv_rms = lax.rsqrt(jnp.mean(mid * mid, axis=-1, keepdims=True) + NORM_EPS)
                    h_loc[seq, at, :] = (mid * inv_rms * gain_ref[...]).astype(bf16)
        if step == 3:
            for hop in range(1, 4):
                h_out(hop).start()
            pltpu.make_async_copy(h_loc, h_slot(me_model), h_local).start()
            slice_own().start()
            for hop in range(1, 8):
                slice_copy(hop, False).start()
    for idx in (1, 2):
        for way in range(2):
            send(idx, way, 0).start()
    pltpu.make_async_copy(h_loc, h_slot(me_model), h_local).wait()
    for hop in range(1, 4):
        h_in(hop).wait_recv()
    for way in range(2):
        landed(0, way, 6).wait_recv()
        own(0, way).wait()

    @pl.loop(0, width // TILE)
    def _(tile):
        cols = pl.ds(pl.multiple_of(tile * TILE, TILE), TILE)
        d_act[:, cols] = across(dy_ref[...], w_down[cols, :]).astype(bf16)

    for idx in (1, 2):
        for way in range(2):
            own(idx, way).wait()
    accumulate(0)

    @pl.loop(1, 7)
    def _(step):
        for idx in (1, 2):
            for way in range(2):
                landed(idx, way, step - 1).wait_recv()
                send(idx, way, step).start()
        accumulate(step)

    for idx in (1, 2):
        for way in range(2):
            landed(idx, way, 6).wait_recv()
    accumulate(7)

    @pl.loop(0, width // 256)
    def _(tile):
        cols = pl.ds(pl.multiple_of(tile * 256, 256), 256)
        gate, up_proj = gate_acc[:, cols], up_acc[:, cols]
        d_val = d_act[:, cols].astype(f32)
        sig_gate = jax.nn.sigmoid(gate)
        silu_gate = gate * sig_gate
        act_ref[:, cols] = (silu_gate * up_proj).astype(bf16)
        d_gate_ref[:, cols] = (d_val * up_proj * sig_gate * (1.0 + gate * (1.0 - sig_gate))).astype(bf16)
        d_up_ref[:, cols] = (d_val * silu_gate).astype(bf16)

    @pl.loop(0, width // TILE)
    def _(tile):
        cols = pl.ds(pl.multiple_of(tile * TILE, TILE), TILE)
        dh_part_ref[:, cols] = across(d_gate_ref[...], w_gate[cols, :]) + across(d_up_ref[...], w_up[cols, :])
        y_part_ref[:, cols] = jnp.dot(act_ref[...], w_down[:, cols], preferred_element_type=f32)

    for idx in range(3):
        for way in range(2):
            for step in range(7):
                send(idx, way, step).wait_send()
    slice_own().wait()
    for hop in range(1, 8):
        slice_copy(hop, True).wait_recv()
        slice_copy(hop, False).wait_send()
    for hop in range(1, 4):
        h_out(hop).wait_send()
    for idx in range(2):
        cols_own(idx).wait()
        for hop in range(1, 4):
            cols_copy(idx, hop, True).wait_recv()
            cols_copy(idx, hop, False).wait_send()


def ring_mlp(collective_id, down_sh, gate_sh, up_sh, attn_part, cols_a, cols_b, x_loc, gain, dy_full):
    tokens, d_model = dy_full.shape
    width = gate_sh.shape[1]
    sent = 21 * gate_sh.size * 2
    dma = pltpu.SemaphoreType.DMA
    vmem = pl.BlockSpec(memory_space=pltpu.VMEM)
    hbm = pl.BlockSpec(memory_space=pl.ANY)
    bf16, f32 = jnp.bfloat16, jnp.float32
    hidden = jax.ShapeDtypeStruct((tokens, width), bf16)
    partial_sum = jax.ShapeDtypeStruct((tokens, d_model), f32)
    sliced = jax.ShapeDtypeStruct(cols_a.shape, bf16)
    spread = jax.ShapeDtypeStruct(cols_a.shape[:2] + (4,) + cols_a.shape[2:], bf16)
    return pl.pallas_call(
        mlp_kernel,
        out_shape=[hidden, hidden, hidden, partial_sum, partial_sum, jax.ShapeDtypeStruct(x_loc.shape, bf16),
                   sliced, spread, spread],
        in_specs=[hbm] * 6 + [vmem] * 3,
        out_specs=[vmem] * 6 + [hbm] * 3,
        scratch_shapes=[pltpu.VMEM((width, d_model), bf16), pltpu.VMEM((d_model, width), bf16),
                        pltpu.VMEM((d_model, width), bf16), pltpu.VMEM((tokens, width), f32),
                        pltpu.VMEM((tokens, width), f32), pltpu.VMEM((tokens, width), bf16),
                        pltpu.VMEM(attn_part.shape, bf16), pltpu.VMEM(x_loc.shape, bf16),
                        pltpu.VMEM((4,) + x_loc.shape, f32),
                        dma((3, 2, 7)), dma((3, 2, 7)), dma((3, 2)), dma((4,)), dma((4,)), dma, dma((4,)), dma((4,)), dma,
                        dma((8,)), dma((8,)), dma, dma((2, 4)), dma((2, 4)), dma((2,))],
        compiler_params=pltpu.CompilerParams(collective_id=collective_id, has_side_effects=True,
                                             vmem_limit_bytes=60 * 1024 * 1024),
        cost_estimate=pl.CostEstimate(flops=sent * 3000, bytes_accessed=2 * sent, transcendentals=0),
        name=f'ring_mlp_{collective_id}',
    )(down_sh, gate_sh, up_sh, attn_part, cols_a, cols_b, x_loc, gain, dy_full)


def back_kernel(act, attn, d_gate, d_up, dh_part, y_part, h_cols, w_out_in, w_qkv_in, mid_ref, x_ref, dy_ref, gain_mlp, gain_attn,
                query, key, value, prob, cos_ref, sin_ref,
                act_all, attn_all, gate_all, up_all, qkv_all, gains_all, mix, mid_cols, mid_spread, h_spread, y_ref, dx_ref,
                w_out, w_qkv, d_mid, d_full, d_attn, d_qkv, dh_attn, gains, row_sum, dh_blocks, y_blocks, attn_blocks,
                send_sem, recv_sem, local_sem, block_send, block_recv, block_local, mid_send, mid_recv, mid_local,
                slice_send, slice_recv, slice_local, cols_send, cols_recv, cols_local, mix_send, mix_recv, mix_local, fetch_sem):
    f32, bf16 = jnp.float32, jnp.bfloat16
    me = lax.axis_index('fsdp')
    me_model = lax.axis_index('model')
    place = ring_place(me)
    targets = (ring_device((place + 1) % 8), ring_device((place + 7) % 8))
    barrier = pltpu.get_barrier_semaphore()
    for hop in range(1, 8):
        pl.semaphore_signal(barrier, inc=1, device_id={'fsdp': (me + hop) % 8}, device_id_type=MESH)
    for hop in range(1, 4):
        pl.semaphore_signal(barrier, inc=1, device_id={'model': (me_model + hop) % 4}, device_id_type=MESH)
    pl.semaphore_wait(barrier, 10)
    sources = (act, attn, d_gate, d_up, d_qkv)
    gathered = (act_all, attn_all, gate_all, up_all, qkv_all)
    seqs, block_rows, d_model = x_ref.shape
    seq_len = 4 * block_rows
    slice_width = mid_cols.shape[3]
    head_dim = query.shape[2]
    heads = query.shape[0] // seqs

    def piece(idx, owner, way):
        if idx == 5:
            return gains_all.at[owner, pl.ds(2 * way, 2)]
        rows = sources[idx].shape[0]
        return gathered[idx].at[pl.ds(pl.multiple_of(owner * rows + way * (rows // 2), rows // 2), rows // 2), :]

    def source(idx, way):
        if idx == 5:
            return mix.at[pl.ds(2 * way, 2)]
        half = sources[idx].shape[0] // 2
        return sources[idx].at[pl.ds(way * half, half), :]

    def owner_at(way, step):
        return ring_device((place + (8 - step if way == 0 else step)) % 8)

    def send(idx, way, step):
        dst = piece(idx, owner_at(way, step), way)
        return pltpu.make_async_remote_copy(
            src_ref=source(idx, way) if step == 0 else dst, dst_ref=dst, send_sem=send_sem.at[idx, way, step],
            recv_sem=recv_sem.at[idx, way, step], device_id={'fsdp': targets[way]}, device_id_type=MESH)

    def landed(idx, way, step):
        dst = piece(idx, owner_at(way, step + 1), way)
        return pltpu.make_async_remote_copy(
            src_ref=dst, dst_ref=dst, send_sem=send_sem.at[idx, way, step], recv_sem=recv_sem.at[idx, way, step],
            device_id={'fsdp': targets[way]}, device_id_type=MESH)

    def own(idx, way):
        return pltpu.make_async_copy(source(idx, way), piece(idx, me, way), local_sem.at[idx, way])

    def start_ring(ids):
        for idx in ids:
            for way in range(2):
                send(idx, way, 0).start()

    def forward(ids, step):
        for idx in ids:
            for way in range(2):
                landed(idx, way, step - 1).wait_recv()
                send(idx, way, step).start()

    def to_member(src, dst, send_one, recv_one, hop):
        return pltpu.make_async_remote_copy(
            src_ref=src, dst_ref=dst, send_sem=send_one, recv_sem=recv_one,
            device_id={'model': (me_model + hop) % 4}, device_id_type=MESH)

    block_src, block_dst = (dh_part, y_part, dh_attn), (dh_blocks, y_blocks, attn_blocks)

    def block_of(idx, member):
        return block_src[idx].at[:, pl.ds(pl.multiple_of(member * block_rows, block_rows), block_rows), :]

    def block_copy(idx, hop, incoming):
        slot = block_dst[idx].at[(me_model + 4 - hop) % 4 if incoming else me_model]
        src = slot if incoming else block_of(idx, (me_model + hop) % 4)
        return to_member(src, slot, block_send.at[idx, hop], block_recv.at[idx, hop], hop)

    def block_own(idx):
        return pltpu.make_async_copy(block_of(idx, me_model), block_dst[idx].at[me_model], block_local.at[idx])

    def blocks_start(idx):
        for hop in range(1, 4):
            block_copy(idx, hop, False).start()
        block_own(idx).start()

    def blocks_wait(idx):
        block_own(idx).wait()
        for hop in range(1, 4):
            block_copy(idx, hop, True).wait_recv()
            block_copy(idx, hop, False).wait_send()

    def mid_slot(member):
        return d_full.at[:, pl.ds(pl.multiple_of(member * block_rows, block_rows), block_rows), :]

    def mid_copy(hop, incoming):
        slot = mid_slot((me_model + 4 - hop) % 4 if incoming else me_model)
        return to_member(slot if incoming else d_mid, slot, mid_send.at[hop], mid_recv.at[hop], hop)

    def mid_own():
        return pltpu.make_async_copy(d_mid, mid_slot(me_model), mid_local)

    def columns(peer):
        return d_mid.at[:, :, pl.ds(pl.multiple_of(peer * slice_width, slice_width), slice_width)]

    def slice_copy(hop, incoming):
        peer = (me + hop) % 8
        slot = mid_cols.at[(me + 8 - hop) % 8 if incoming else me]
        return pltpu.make_async_remote_copy(
            src_ref=slot if incoming else columns(peer), dst_ref=slot, send_sem=slice_send.at[hop],
            recv_sem=slice_recv.at[hop], device_id={'fsdp': peer}, device_id_type=MESH)

    def slice_own():
        return pltpu.make_async_copy(columns(me), mid_cols.at[me], slice_local)

    cols_in, cols_all = (h_cols, mid_cols), (h_spread, mid_spread)

    def cols_copy(idx, hop, incoming):
        slot = cols_all[idx].at[:, :, (me_model + 4 - hop) % 4 if incoming else me_model]
        return to_member(slot if incoming else cols_in[idx], slot, cols_send.at[idx, hop], cols_recv.at[idx, hop], hop)

    def cols_own(idx):
        return pltpu.make_async_copy(cols_in[idx], cols_all[idx].at[:, :, me_model], cols_local.at[idx])

    def mix_copy(hop, incoming):
        slot = mix.at[(me_model + 4 - hop) % 4 if incoming else me_model]
        return to_member(slot if incoming else gains, slot, mix_send.at[hop], mix_recv.at[hop], hop)

    def mix_own():
        return pltpu.make_async_copy(gains, mix.at[me_model], mix_local)

    def fetch(idx):
        return pltpu.make_async_copy((w_out_in, w_qkv_in)[idx], (w_out, w_qkv)[idx], fetch_sem.at[idx])

    def across(left, right):
        return lax.dot_general(left, right, (((1,), (1,)), ((), ())), preferred_element_type=f32)

    def along(left, right):
        return lax.dot_general(left, right, (((0,), (0,)), ((), ())), preferred_element_type=f32)

    def add_up(parts, seq, at):
        return ((parts[0, seq, at, :] + parts[1, seq, at, :]) + (parts[2, seq, at, :] + parts[3, seq, at, :])).astype(bf16).astype(f32)

    def norm_back(parts, saved, gain, base, result, first_row):
        row_sum[...] = jnp.zeros_like(row_sum)

        @pl.loop(0, block_rows // 16)
        def _(group):
            at = pl.ds(pl.multiple_of(group * 16, 16), 16)
            for seq in range(seqs):
                d_h = add_up(parts, seq, at)
                val = saved[seq, at, :].astype(f32)
                inv_rms = lax.rsqrt(jnp.mean(val * val, axis=-1, keepdims=True) + NORM_EPS)
                scaled = d_h * gain[...]
                slope = jnp.sum(scaled * val, axis=-1, keepdims=True) * (inv_rms * inv_rms * inv_rms) * (1.0 / d_model)
                result[seq, at, :] = (base[seq, at, :].astype(f32) + (scaled * inv_rms - val * slope)).astype(bf16)
                per_row = d_h * val * inv_rms
                row_sum[...] += per_row[:8] + per_row[8:]
        total = jnp.sum(row_sum[...], axis=0, keepdims=True)
        width = gains.shape[1]
        for row in range(d_model // width):
            gains[first_row + row:first_row + row + 1, :] = total[:, row * width:(row + 1) * width]

    def attention_back():
        d_attn[...] = across(d_full[...].reshape(seqs * seq_len, d_model), w_out[...]).astype(bf16)
        for seq in range(seqs):
            for head in range(heads):
                idx = seq * heads + head
                rows = slice(seq * seq_len, (seq + 1) * seq_len)
                d_out = d_attn[rows, head * head_dim:(head + 1) * head_dim]
                weight = prob[idx]
                d_prob = across(d_out, value[idx])
                row_dot = jnp.sum(d_prob * weight, axis=-1, keepdims=True)
                d_scores = (weight * (d_prob - row_dot) * head_dim ** -0.5).astype(bf16)
                d_query = jnp.dot(d_scores, key[idx], preferred_element_type=f32)
                d_key = along(d_scores, query[idx])
                d_value = along(weight.astype(bf16), d_out)
                for place_in, part in enumerate((d_query, d_key)):
                    turned = part * cos_ref[...] + pltpu.roll(part, head_dim // 2, 1) * sin_ref[...]
                    start = (3 * head + place_in) * head_dim
                    d_qkv[rows, start:start + head_dim] = turned.astype(bf16)
                d_qkv[rows, (3 * head + 2) * head_dim:(3 * head + 3) * head_dim] = d_value.astype(bf16)

        @pl.loop(0, d_model // TILE)
        def _(tile):
            cols = pl.ds(pl.multiple_of(tile * TILE, TILE), TILE)
            dh_attn[:, :, cols] = across(d_qkv[...], w_qkv[cols, :]).reshape(seqs, seq_len, TILE)

    start_ring((0, 1))
    blocks_start(0)
    blocks_start(1)
    for idx in range(4):
        for way in range(2):
            own(idx, way).start()
    for idx in range(2):
        fetch(idx).start()
    for hop in range(1, 4):
        cols_copy(0, hop, False).start()
    cols_own(0).start()
    for step in range(1, 7):
        forward((0, 1), step)
        if step == 2:
            blocks_wait(0)
            norm_back(dh_blocks, mid_ref, gain_mlp, dy_ref, d_mid, 8)
        if step == 3:
            for hop in range(1, 4):
                mid_copy(hop, False).start()
            mid_own().start()
            slice_own().start()
            for hop in range(1, 8):
                slice_copy(hop, False).start()
        if step == 5:
            blocks_wait(1)

            @pl.loop(0, block_rows // 16)
            def _(group):
                at = pl.ds(pl.multiple_of(group * 16, 16), 16)
                for seq in range(seqs):
                    y_ref[seq, at, :] = (mid_ref[seq, at, :].astype(f32) + add_up(y_blocks, seq, at)).astype(bf16)
    start_ring((2, 3))
    for step in range(1, 7):
        forward((2, 3), step)
        if step == 1:
            mid_own().wait()
            for hop in range(1, 4):
                mid_copy(hop, True).wait_recv()
                mid_copy(hop, False).wait_send()
            for idx in range(2):
                fetch(idx).wait()
            attention_back()
        if step == 2:
            blocks_start(2)
            slice_own().wait()
            for hop in range(1, 8):
                slice_copy(hop, True).wait_recv()
                slice_copy(hop, False).wait_send()
            for hop in range(1, 4):
                cols_copy(1, hop, False).start()
            cols_own(1).start()
        if step == 4:
            blocks_wait(2)
            norm_back(attn_blocks, x_ref, gain_attn, d_mid, dx_ref, 0)
        if step == 5:
            mix_own().start()
            for hop in range(1, 4):
                mix_copy(hop, False).start()
    start_ring((4,))
    mix_own().wait()
    for hop in range(1, 4):
        mix_copy(hop, True).wait_recv()
        mix_copy(hop, False).wait_send()
    start_ring((5,))
    for idx in (4, 5):
        for way in range(2):
            own(idx, way).start()
    for step in range(1, 7):
        forward((4, 5), step)
    for idx in range(6):
        for way in range(2):
            landed(idx, way, 6).wait_recv()
            own(idx, way).wait()
            for step in range(7):
                send(idx, way, step).wait_send()
    for idx in range(2):
        cols_own(idx).wait()
        for hop in range(1, 4):
            cols_copy(idx, hop, True).wait_recv()
            cols_copy(idx, hop, False).wait_send()


def ring_back(collective_id, *args):
    act, attn, d_gate, d_up, dh_part, y_part, h_cols, w_out, w_qkv, mid = args[:10]
    tokens = act.shape[0]
    seqs, seq_len, d_model = dh_part.shape
    bf16, f32 = jnp.bfloat16, jnp.float32
    qkv_cols = w_qkv.shape[1]
    sent = 7 * (3 * act.size + attn.size + tokens * qkv_cols) * 2
    dma = pltpu.SemaphoreType.DMA
    vmem = pl.BlockSpec(memory_space=pltpu.VMEM)
    hbm = pl.BlockSpec(memory_space=pl.ANY)
    shape = jax.ShapeDtypeStruct
    gain_shape = (16, d_model // 8)
    spread = shape(h_cols.shape[:2] + (4,) + h_cols.shape[2:], bf16)
    blocks = pltpu.VMEM((4,) + mid.shape, f32)
    return pl.pallas_call(
        back_kernel,
        out_shape=[shape((8 * tokens, array.shape[1]), bf16) for array in (act, attn, d_gate, d_up)]
        + [shape((8 * tokens, qkv_cols), bf16), shape((8, 4) + gain_shape, f32), shape((4,) + gain_shape, f32),
           shape(h_cols.shape, bf16), spread, spread, shape(mid.shape, bf16), shape(mid.shape, bf16)],
        in_specs=[hbm] * 9 + [vmem] * (len(args) - 9),
        out_specs=[hbm] * 10 + [vmem] * 2,
        scratch_shapes=[pltpu.VMEM(w_out.shape, bf16), pltpu.VMEM(w_qkv.shape, bf16), pltpu.VMEM(mid.shape, bf16),
                        pltpu.VMEM(dh_part.shape, bf16), pltpu.VMEM((tokens, w_out.shape[0]), bf16),
                        pltpu.VMEM((tokens, qkv_cols), bf16), pltpu.VMEM(dh_part.shape, f32), pltpu.VMEM(gain_shape, f32),
                        pltpu.VMEM((8, d_model), f32), blocks, blocks, blocks,
                        dma((6, 2, 7)), dma((6, 2, 7)), dma((6, 2)), dma((3, 4)), dma((3, 4)), dma((3,)),
                        dma((4,)), dma((4,)), dma, dma((8,)), dma((8,)), dma, dma((2, 4)), dma((2, 4)), dma((2,)),
                        dma((4,)), dma((4,)), dma, dma((2,))],
        compiler_params=pltpu.CompilerParams(collective_id=collective_id, has_side_effects=True,
                                             vmem_limit_bytes=60 * 1024 * 1024),
        cost_estimate=pl.CostEstimate(flops=sent * 3000, bytes_accessed=2 * sent, transcendentals=0),
        name=f'ring_back_{collective_id}',
    )(*args)


def solution(mesh):
    act_spec = P('fsdp', 'model', None)
    rows_spec = P('fsdp', 'model')
    cols_spec = P('model', 'fsdp')
    f32 = jnp.float32
    bf16 = jnp.bfloat16

    def device_fn(x_loc, dy_loc, gain_attn, gain_mlp, wqkv_sh, wout_sh, wgate_sh, wup_sh, wdown_sh, rope_cos, rope_sin):
        head_dim = 2 * rope_cos.shape[1]
        seq_full = rope_cos.shape[0]
        local_heads = wout_sh.shape[0] // head_dim
        local_kv = (wqkv_sh.shape[1] // head_dim - local_heads) // 2
        group_size = local_heads // local_kv
        rows = x_loc.shape[0]
        tokens = rows * seq_full
        scale = head_dim ** -0.5
        pos_ids = jnp.arange(seq_full)
        causal = pos_ids[:, None] >= pos_ids[None, :]
        cos_q = rope_cos[:, None, None, :]
        sin_q = rope_sin[:, None, None, :]
        cos_k = rope_cos[:, None, :]
        sin_k = rope_sin[:, None, :]

        x_f32 = x_loc.astype(f32)
        h_attn_loc = rms_scale(x_f32, gain_attn).astype(bf16)
        w_qkv, w_out, h_attn_cols, dy_cols, h_attn, dy_full = ring_gather(
            0, [wqkv_sh, wout_sh], [0, 1], [h_attn_loc, dy_loc], [('seq', h_attn_loc), ('seq', dy_loc)])
        qkv = jnp.einsum('bsd,dc->bsc', h_attn, w_qkv, preferred_element_type=f32)
        qkv = qkv.reshape(rows, seq_full, local_kv, group_size + 2, head_dim)
        query = rotate(qkv[:, :, :, :group_size], cos_q, sin_q).astype(bf16)
        key_rot = rotate(qkv[:, :, :, group_size], cos_k, sin_k).astype(bf16)
        value = qkv[:, :, :, group_size + 1].astype(bf16)
        scores = jnp.einsum('bqkgd,btkd->bkgqt', query, key_rot, preferred_element_type=f32) * scale
        attn_prob = jax.nn.softmax(jnp.where(causal, scores, -1e30), axis=-1)
        prob_bf = attn_prob.astype(bf16)
        attn = jnp.einsum('bkgqt,btkd->bqkgd', prob_bf, value, preferred_element_type=f32)
        attn_flat = attn.astype(bf16).reshape(rows, seq_full, local_heads * head_dim)
        attn_part = jnp.einsum('bsh,hd->bsd', attn_flat, w_out, preferred_element_type=f32)
        gated_act, d_gate, d_up, mlp_part, dh_part, mid, h_mlp_cols, h_attn_cols, dy_cols = ring_mlp(
            1, wdown_sh, wgate_sh, wup_sh, attn_part, h_attn_cols, dy_cols, x_loc, gain_mlp.reshape(1, -1),
            dy_full.reshape(tokens, -1))
        def by_head(heads):
            return heads.reshape(rows, seq_full, local_heads, head_dim).transpose(0, 2, 1, 3).reshape(-1, seq_full, head_dim)

        (act_all, attn_all, d_gate_all, d_up_all, d_qkv_all, gains_all, _, _, d_mid_cols, h_mlp_cols, y_loc, dx_loc) = ring_back(
            2, gated_act, attn_flat.reshape(tokens, -1), d_gate, d_up, dh_part.reshape(rows, seq_full, -1),
            mlp_part.reshape(rows, seq_full, -1), h_mlp_cols, w_out, w_qkv, mid, x_loc, dy_loc, gain_mlp.reshape(1, -1),
            gain_attn.reshape(1, -1), by_head(query), by_head(key_rot), by_head(value),
            attn_prob.reshape(-1, seq_full, seq_full), jnp.concatenate([rope_cos, rope_cos], axis=1),
            jnp.concatenate([rope_sin, -rope_sin], axis=1))
        gain_grads = jnp.sum(gains_all, axis=(0, 1)).reshape(2, -1)
        h_attn_cols, dy_cols, h_mlp_cols, d_mid_cols = [
            cols.reshape(8 * tokens, -1) for cols in (h_attn_cols, dy_cols, h_mlp_cols, d_mid_cols)]

        def pair(left, right):
            return lax.dot_general(left, right, (((0,), (0,)), ((), ())), preferred_element_type=f32)

        return (y_loc, dx_loc, gain_grads[0], gain_grads[1],
                pair(h_attn_cols, d_qkv_all), pair(attn_all, d_mid_cols),
                pair(h_mlp_cols, d_gate_all), pair(h_mlp_cols, d_up_all), pair(act_all, dy_cols))

    in_specs = (act_spec, act_spec, P(), P(), rows_spec, cols_spec, rows_spec, rows_spec, cols_spec, P(), P())
    out_specs = (act_spec, act_spec, P(), P(), rows_spec, cols_spec, rows_spec, rows_spec, cols_spec)
    return jax.shard_map(device_fn, mesh=mesh, in_specs=in_specs, out_specs=out_specs, check_vma=False)
```

```python
import functools

import jax
import jax.numpy as jnp
from jax import lax
from jax.experimental import pallas as pl
from jax.experimental.pallas import tpu as pltpu
from jax.sharding import PartitionSpec as P

NORM_EPS = 1e-5
MESH = pl.DeviceIdType.MESH


def ring_place(index):
    z, y = index // 2, index % 2
    return z + y * (7 - 2 * z)


def ring_device(place):
    y = place // 4
    return 2 * (place + y * (7 - 2 * place)) + y


TILE = 512


def front_kernel(qkv_sh, out_sh, down_sh, gate_sh, up_sh, x_ref, dy_in, gain_attn, gain_mlp, cos_ref, sin_ref,
                 w_qkv_all, w_out_all, attn_cols, dy_cols, h_cols, attn_spread, dy_spread,
                 query, key, value, prob, attn_flat, act_ref, d_gate_ref, d_up_ref, y_part_ref, dh_part_ref, mid_ref,
                 w_qkv, w_out, w_down, w_gate, w_up, qkv, attn_part, gate_acc, up_acc, d_act, ha_full, dy_full, h_full,
                 ha_loc, h_loc, blocks,
                 send_sem, recv_sem, local_sem, block_send, block_recv, block_local, seq_send, seq_recv, seq_local,
                 slice_send, slice_recv, slice_local, cols_send, cols_recv, cols_local, fetch_sem):
    f32, bf16 = jnp.float32, jnp.bfloat16
    me = lax.axis_index('fsdp')
    me_model = lax.axis_index('model')
    place = ring_place(me)
    targets = (ring_device((place + 1) % 8), ring_device((place + 7) % 8))
    barrier = pltpu.get_barrier_semaphore()
    for hop in range(1, 8):
        pl.semaphore_signal(barrier, inc=1, device_id={'fsdp': (me + hop) % 8}, device_id_type=MESH)
    for hop in range(1, 4):
        pl.semaphore_signal(barrier, inc=1, device_id={'model': (me_model + hop) % 4}, device_id_type=MESH)
    pl.semaphore_wait(barrier, 10)
    shards, weights = (qkv_sh, out_sh, down_sh, gate_sh, up_sh), (w_qkv_all, w_out_all, w_down, w_gate, w_up)
    accs = {3: gate_acc, 4: up_acc}
    rows, width = gate_sh.shape
    half = rows // 2
    seqs, block_rows, d_model = x_ref.shape
    seq_len = 4 * block_rows
    tokens = seqs * seq_len
    slice_width = h_cols.shape[3]
    head_dim = query.shape[2]
    heads = query.shape[0] // seqs

    def start_of(owner, way):
        return pl.multiple_of(owner * rows + way * half, half)

    def piece(idx, owner, way):
        if idx in (1, 2):
            tall = shards[idx].shape[0] // 2
            return weights[idx].at[pl.ds(way * tall, tall), pl.ds(pl.multiple_of(owner * rows, rows), rows)]
        return weights[idx].at[pl.ds(start_of(owner, way), half), :]

    def source(idx, way):
        size = shards[idx].shape[0] // 2
        return shards[idx].at[pl.ds(way * size, size), :]

    def owner_at(way, step):
        return ring_device((place + (8 - step if way == 0 else step)) % 8)

    def send(idx, way, step):
        dst = piece(idx, owner_at(way, step), way)
        return pltpu.make_async_remote_copy(
            src_ref=source(idx, way) if isinstance(step, int) and step == 0 else dst, dst_ref=dst,
            send_sem=send_sem.at[idx, way, step], recv_sem=recv_sem.at[idx, way, step],
            device_id={'fsdp': targets[way]}, device_id_type=MESH)

    def landed(idx, way, step):
        dst = piece(idx, owner_at(way, step + 1), way)
        return pltpu.make_async_remote_copy(
            src_ref=dst, dst_ref=dst, send_sem=send_sem.at[idx, way, step], recv_sem=recv_sem.at[idx, way, step],
            device_id={'fsdp': targets[way]}, device_id_type=MESH)

    def own(idx, way):
        return pltpu.make_async_copy(source(idx, way), piece(idx, me, way), local_sem.at[idx, way])

    def start_ring(ids):
        for idx in ids:
            for way in range(2):
                send(idx, way, 0).start()

    def forward(ids, step):
        for idx in ids:
            for way in range(2):
                landed(idx, way, step - 1).wait_recv()
                send(idx, way, step).start()

    def finish_ring(ids):
        for idx in ids:
            for way in range(2):
                landed(idx, way, 6).wait_recv()
                own(idx, way).wait()

    def to_member(src, dst, send_one, recv_one, hop):
        return pltpu.make_async_remote_copy(
            src_ref=src, dst_ref=dst, send_sem=send_one, recv_sem=recv_one,
            device_id={'model': (me_model + hop) % 4}, device_id_type=MESH)

    def rows_of(ref, member):
        return ref.at[:, pl.ds(pl.multiple_of(member * block_rows, block_rows), block_rows), :]

    def block_copy(hop, incoming):
        slot = blocks.at[(me_model + 4 - hop) % 4 if incoming else me_model]
        src = slot if incoming else rows_of(attn_part, (me_model + hop) % 4)
        return to_member(src, slot, block_send.at[hop], block_recv.at[hop], hop)

    def block_own():
        return pltpu.make_async_copy(rows_of(attn_part, me_model), blocks.at[me_model], block_local)

    seq_src, seq_dst = (ha_loc, dy_in, h_loc), (ha_full, dy_full, h_full)
    slice_dst, spread_dst = (attn_cols, dy_cols, h_cols), (attn_spread, dy_spread)

    def seq_copy(idx, hop, incoming):
        slot = rows_of(seq_dst[idx], (me_model + 4 - hop) % 4 if incoming else me_model)
        return to_member(slot if incoming else seq_src[idx], slot, seq_send.at[idx, hop], seq_recv.at[idx, hop], hop)

    def seq_own(idx):
        return pltpu.make_async_copy(seq_src[idx], rows_of(seq_dst[idx], me_model), seq_local.at[idx])

    def columns(idx, peer):
        return seq_src[idx].at[:, :, pl.ds(pl.multiple_of(peer * slice_width, slice_width), slice_width)]

    def slice_copy(idx, hop, incoming):
        peer = (me + hop) % 8
        slot = slice_dst[idx].at[(me + 8 - hop) % 8 if incoming else me]
        return pltpu.make_async_remote_copy(
            src_ref=slot if incoming else columns(idx, peer), dst_ref=slot, send_sem=slice_send.at[idx, hop],
            recv_sem=slice_recv.at[idx, hop], device_id={'fsdp': peer}, device_id_type=MESH)

    def slice_own(idx):
        return pltpu.make_async_copy(columns(idx, me), slice_dst[idx].at[me], slice_local.at[idx])

    def hand_out(idx):
        for hop in range(1, 4):
            seq_copy(idx, hop, False).start()
        seq_own(idx).start()
        slice_own(idx).start()
        for hop in range(1, 8):
            slice_copy(idx, hop, False).start()

    def seq_wait(idx):
        seq_own(idx).wait()
        for hop in range(1, 4):
            seq_copy(idx, hop, True).wait_recv()
            seq_copy(idx, hop, False).wait_send()

    def slice_wait(idx):
        slice_own(idx).wait()
        for hop in range(1, 8):
            slice_copy(idx, hop, True).wait_recv()
            slice_copy(idx, hop, False).wait_send()

    def cols_copy(idx, hop, incoming):
        slot = spread_dst[idx].at[:, :, (me_model + 4 - hop) % 4 if incoming else me_model]
        return to_member(slot if incoming else slice_dst[idx], slot, cols_send.at[idx, hop], cols_recv.at[idx, hop], hop)

    def cols_own(idx):
        return pltpu.make_async_copy(slice_dst[idx], spread_dst[idx].at[:, :, me_model], cols_local.at[idx])

    def fetch(idx):
        return pltpu.make_async_copy(weights[idx], (w_qkv, w_out)[idx], fetch_sem.at[idx])

    def normed(val, gain):
        return (val * lax.rsqrt(jnp.mean(val * val, axis=-1, keepdims=True) + NORM_EPS) * gain[...]).astype(bf16)

    def attention():
        @pl.loop(0, qkv.shape[1] // TILE)
        def _(tile):
            cols = pl.ds(pl.multiple_of(tile * TILE, TILE), TILE)
            qkv[:, cols] = jnp.dot(ha_full[...].reshape(tokens, d_model), w_qkv[:, cols], preferred_element_type=f32)
        causal = (lax.broadcasted_iota(jnp.int32, (seq_len, seq_len), 0)
                  >= lax.broadcasted_iota(jnp.int32, (seq_len, seq_len), 1))
        for seq in range(seqs):
            for head in range(heads):
                idx = seq * heads + head
                at = slice(seq * seq_len, (seq + 1) * seq_len)
                start = 3 * head * head_dim
                for place_in, turned_ref in enumerate((query, key)):
                    part = qkv[at, start + place_in * head_dim:start + (place_in + 1) * head_dim]
                    turned = part * cos_ref[...] - pltpu.roll(part, head_dim // 2, 1) * sin_ref[...]
                    turned_ref[idx] = turned.astype(bf16)
                value[idx] = qkv[at, start + 2 * head_dim:start + 3 * head_dim].astype(bf16)
                scores = jnp.where(causal, across(query[idx], key[idx]) * head_dim ** -0.5, -1e30)
                unnormed = jnp.exp(scores - jnp.max(scores, axis=-1, keepdims=True))
                weight = unnormed / jnp.sum(unnormed, axis=-1, keepdims=True)
                prob[idx] = weight
                mixed = jnp.dot(weight.astype(bf16), value[idx], preferred_element_type=f32)
                attn_flat[at, head * head_dim:(head + 1) * head_dim] = mixed.astype(bf16)

        @pl.loop(0, d_model // TILE)
        def _(tile):
            cols = pl.ds(pl.multiple_of(tile * TILE, TILE), TILE)
            attn_part[:, :, cols] = jnp.dot(attn_flat[...], w_out[:, cols],
                                            preferred_element_type=f32).reshape(seqs, seq_len, TILE)

    def accumulate(step):
        for way in range(2):
            start = start_of(owner_at(way, step), way)
            h_block = h_full[:, :, pl.ds(start, half)].reshape(tokens, half)
            for idx in (3, 4):
                @pl.loop(0, width // TILE)
                def _(tile):
                    cols = pl.ds(pl.multiple_of(tile * TILE, TILE), TILE)
                    accs[idx][:, cols] += jnp.dot(h_block, weights[idx][pl.ds(start, half), cols],
                                                  preferred_element_type=f32)

    def across(left, right):
        return lax.dot_general(left, right, (((1,), (1,)), ((), ())), preferred_element_type=f32)

    start_ring((0, 1))
    for idx in range(5):
        for way in range(2):
            own(idx, way).start()
    hand_out(1)

    @pl.loop(0, block_rows // 16)
    def _(group):
        at = pl.ds(pl.multiple_of(group * 16, 16), 16)
        for seq in range(seqs):
            ha_loc[seq, at, :] = normed(x_ref[seq, at, :].astype(f32), gain_attn)
    gate_acc[...] = jnp.zeros_like(gate_acc)
    up_acc[...] = jnp.zeros_like(up_acc)
    for step in range(1, 7):
        forward((0, 1), step)
        if step == 1:
            hand_out(0)
    start_ring((2,))
    finish_ring((0, 1))
    for idx in range(2):
        fetch(idx).start()
    for step in range(1, 7):
        forward((2,), step)
        if step == 1:
            seq_wait(0)
            for idx in range(2):
                fetch(idx).wait()
            attention()
        if step == 2:
            for hop in range(1, 4):
                block_copy(hop, False).start()
            block_own().start()
        if step == 4:
            block_own().wait()
            for hop in range(1, 4):
                block_copy(hop, True).wait_recv()
                block_copy(hop, False).wait_send()

            @pl.loop(0, block_rows // 16)
            def _(group):
                at = pl.ds(pl.multiple_of(group * 16, 16), 16)
                for seq in range(seqs):
                    total = (blocks[0, seq, at, :] + blocks[1, seq, at, :]) + (blocks[2, seq, at, :] + blocks[3, seq, at, :])
                    mid = (x_ref[seq, at, :].astype(f32) + total.astype(bf16).astype(f32)).astype(bf16)
                    mid_ref[seq, at, :] = mid
                    h_loc[seq, at, :] = normed(mid.astype(f32), gain_mlp)
        if step == 5:
            hand_out(2)
    start_ring((3, 4))
    seq_wait(1)
    for idx in range(2):
        slice_wait(idx)
        for hop in range(1, 4):
            cols_copy(idx, hop, False).start()
        cols_own(idx).start()
    finish_ring((2,))

    @pl.loop(0, width // TILE)
    def _(tile):
        cols = pl.ds(pl.multiple_of(tile * TILE, TILE), TILE)
        d_act[:, cols] = across(dy_full[...].reshape(tokens, d_model), w_down[cols, :]).astype(bf16)

    seq_wait(2)
    for idx in (3, 4):
        for way in range(2):
            own(idx, way).wait()
    accumulate(0)

    @pl.loop(1, 7)
    def _(step):
        forward((3, 4), step)
        accumulate(step)

    for idx in (3, 4):
        for way in range(2):
            landed(idx, way, 6).wait_recv()
    accumulate(7)

    @pl.loop(0, width // 256)
    def _(tile):
        cols = pl.ds(pl.multiple_of(tile * 256, 256), 256)
        gate, up_proj = gate_acc[:, cols], up_acc[:, cols]
        d_val = d_act[:, cols].astype(f32)
        sig_gate = jax.nn.sigmoid(gate)
        silu_gate = gate * sig_gate
        act_ref[:, cols] = (silu_gate * up_proj).astype(bf16)
        d_gate_ref[:, cols] = (d_val * up_proj * sig_gate * (1.0 + gate * (1.0 - sig_gate))).astype(bf16)
        d_up_ref[:, cols] = (d_val * silu_gate).astype(bf16)

    @pl.loop(0, width // TILE)
    def _(tile):
        cols = pl.ds(pl.multiple_of(tile * TILE, TILE), TILE)
        dh_part_ref[:, cols] = across(d_gate_ref[...], w_gate[cols, :]) + across(d_up_ref[...], w_up[cols, :])
        y_part_ref[:, cols] = jnp.dot(act_ref[...], w_down[:, cols], preferred_element_type=f32)

    for idx in range(5):
        for way in range(2):
            for step in range(7):
                send(idx, way, step).wait_send()
    slice_wait(2)
    for idx in range(2):
        cols_own(idx).wait()
        for hop in range(1, 4):
            cols_copy(idx, hop, True).wait_recv()
            cols_copy(idx, hop, False).wait_send()


def ring_front(collective_id, *args):
    qkv_sh, out_sh, down_sh, gate_sh, up_sh, x_loc, dy_loc = args[:7]
    seqs, block_rows, d_model = x_loc.shape
    seq_len, head_dim = args[9].shape
    tokens = seqs * seq_len
    width, qkv_cols, attn_cols = gate_sh.shape[1], qkv_sh.shape[1], out_sh.shape[0]
    sent = 7 * (qkv_sh.size + out_sh.size + 3 * gate_sh.size) * 2
    dma = pltpu.SemaphoreType.DMA
    vmem = pl.BlockSpec(memory_space=pltpu.VMEM)
    hbm = pl.BlockSpec(memory_space=pl.ANY)
    bf16, f32 = jnp.bfloat16, jnp.float32
    shape, buf = jax.ShapeDtypeStruct, pltpu.VMEM
    sliced = shape((8, seqs, block_rows, d_model // 8), bf16)
    spread = shape((8, seqs, 4, block_rows, d_model // 8), bf16)
    per_head = shape((seqs * attn_cols // head_dim, seq_len, head_dim), bf16)
    hidden = shape((tokens, width), bf16)
    partial_sum = shape((tokens, d_model), f32)
    whole = (seqs, seq_len, d_model)
    return pl.pallas_call(
        front_kernel,
        out_shape=[shape((d_model, qkv_cols), bf16), shape((attn_cols, d_model), bf16), sliced, sliced, sliced, spread, spread,
                   per_head, per_head, per_head, shape((per_head.shape[0], seq_len, seq_len), f32),
                   shape((tokens, attn_cols), bf16), hidden, hidden, hidden, partial_sum, partial_sum, shape(x_loc.shape, bf16)],
        in_specs=[hbm] * 5 + [vmem] * 6,
        out_specs=[hbm] * 7 + [vmem] * 11,
        scratch_shapes=[buf((d_model, qkv_cols), bf16), buf((attn_cols, d_model), bf16), buf((width, d_model), bf16),
                        buf((d_model, width), bf16), buf((d_model, width), bf16), buf((tokens, qkv_cols), f32), buf(whole, f32),
                        buf((tokens, width), f32), buf((tokens, width), f32), buf((tokens, width), bf16),
                        buf(whole, bf16), buf(whole, bf16), buf(whole, bf16), buf(x_loc.shape, bf16), buf(x_loc.shape, bf16),
                        buf((4,) + x_loc.shape, f32),
                        dma((5, 2, 7)), dma((5, 2, 7)), dma((5, 2)), dma((4,)), dma((4,)), dma, dma((3, 4)), dma((3, 4)), dma((3,)),
                        dma((3, 8)), dma((3, 8)), dma((3,)), dma((2, 4)), dma((2, 4)), dma((2,)), dma((2,))],
        compiler_params=pltpu.CompilerParams(collective_id=collective_id, has_side_effects=True,
                                             vmem_limit_bytes=63 * 1024 * 1024),
        cost_estimate=pl.CostEstimate(flops=sent * 3000, bytes_accessed=2 * sent, transcendentals=0),
        name=f'ring_front_{collective_id}',
    )(*args)


def back_kernel(act, attn, d_gate, d_up, dh_part, y_part, h_cols, w_out_in, w_qkv_in, mid_ref, x_ref, dy_ref, gain_mlp, gain_attn,
                query, key, value, prob, cos_ref, sin_ref,
                act_all, attn_all, gate_all, up_all, qkv_all, gains_all, mix, mid_cols, mid_spread, h_spread, y_ref, dx_ref,
                w_out, w_qkv, d_mid, d_full, d_attn, d_qkv, dh_attn, gains, row_sum, dh_blocks, y_blocks, attn_blocks,
                send_sem, recv_sem, local_sem, block_send, block_recv, block_local, mid_send, mid_recv, mid_local,
                slice_send, slice_recv, slice_local, cols_send, cols_recv, cols_local, mix_send, mix_recv, mix_local, fetch_sem):
    f32, bf16 = jnp.float32, jnp.bfloat16
    me = lax.axis_index('fsdp')
    me_model = lax.axis_index('model')
    place = ring_place(me)
    targets = (ring_device((place + 1) % 8), ring_device((place + 7) % 8))
    barrier = pltpu.get_barrier_semaphore()
    for hop in range(1, 8):
        pl.semaphore_signal(barrier, inc=1, device_id={'fsdp': (me + hop) % 8}, device_id_type=MESH)
    for hop in range(1, 4):
        pl.semaphore_signal(barrier, inc=1, device_id={'model': (me_model + hop) % 4}, device_id_type=MESH)
    pl.semaphore_wait(barrier, 10)
    sources = (act, attn, d_gate, d_up, d_qkv)
    gathered = (act_all, attn_all, gate_all, up_all, qkv_all)
    seqs, block_rows, d_model = x_ref.shape
    seq_len = 4 * block_rows
    slice_width = mid_cols.shape[3]
    head_dim = query.shape[2]
    heads = query.shape[0] // seqs

    def piece(idx, owner, way):
        if idx == 5:
            return gains_all.at[owner, pl.ds(2 * way, 2)]
        rows = sources[idx].shape[0]
        return gathered[idx].at[pl.ds(pl.multiple_of(owner * rows + way * (rows // 2), rows // 2), rows // 2), :]

    def source(idx, way):
        if idx == 5:
            return mix.at[pl.ds(2 * way, 2)]
        half = sources[idx].shape[0] // 2
        return sources[idx].at[pl.ds(way * half, half), :]

    def owner_at(way, step):
        return ring_device((place + (8 - step if way == 0 else step)) % 8)

    def send(idx, way, step):
        dst = piece(idx, owner_at(way, step), way)
        return pltpu.make_async_remote_copy(
            src_ref=source(idx, way) if step == 0 else dst, dst_ref=dst, send_sem=send_sem.at[idx, way, step],
            recv_sem=recv_sem.at[idx, way, step], device_id={'fsdp': targets[way]}, device_id_type=MESH)

    def landed(idx, way, step):
        dst = piece(idx, owner_at(way, step + 1), way)
        return pltpu.make_async_remote_copy(
            src_ref=dst, dst_ref=dst, send_sem=send_sem.at[idx, way, step], recv_sem=recv_sem.at[idx, way, step],
            device_id={'fsdp': targets[way]}, device_id_type=MESH)

    def own(idx, way):
        return pltpu.make_async_copy(source(idx, way), piece(idx, me, way), local_sem.at[idx, way])

    def start_ring(ids):
        for idx in ids:
            for way in range(2):
                send(idx, way, 0).start()

    def forward(ids, step):
        for idx in ids:
            for way in range(2):
                landed(idx, way, step - 1).wait_recv()
                send(idx, way, step).start()

    def to_member(src, dst, send_one, recv_one, hop):
        return pltpu.make_async_remote_copy(
            src_ref=src, dst_ref=dst, send_sem=send_one, recv_sem=recv_one,
            device_id={'model': (me_model + hop) % 4}, device_id_type=MESH)

    block_src, block_dst = (dh_part, y_part, dh_attn), (dh_blocks, y_blocks, attn_blocks)

    def block_of(idx, member):
        return block_src[idx].at[:, pl.ds(pl.multiple_of(member * block_rows, block_rows), block_rows), :]

    def block_copy(idx, hop, incoming):
        slot = block_dst[idx].at[(me_model + 4 - hop) % 4 if incoming else me_model]
        src = slot if incoming else block_of(idx, (me_model + hop) % 4)
        return to_member(src, slot, block_send.at[idx, hop], block_recv.at[idx, hop], hop)

    def block_own(idx):
        return pltpu.make_async_copy(block_of(idx, me_model), block_dst[idx].at[me_model], block_local.at[idx])

    def blocks_start(idx):
        for hop in range(1, 4):
            block_copy(idx, hop, False).start()
        block_own(idx).start()

    def blocks_wait(idx):
        block_own(idx).wait()
        for hop in range(1, 4):
            block_copy(idx, hop, True).wait_recv()
            block_copy(idx, hop, False).wait_send()

    def mid_slot(member):
        return d_full.at[:, pl.ds(pl.multiple_of(member * block_rows, block_rows), block_rows), :]

    def mid_copy(hop, incoming):
        slot = mid_slot((me_model + 4 - hop) % 4 if incoming else me_model)
        return to_member(slot if incoming else d_mid, slot, mid_send.at[hop], mid_recv.at[hop], hop)

    def mid_own():
        return pltpu.make_async_copy(d_mid, mid_slot(me_model), mid_local)

    def columns(peer):
        return d_mid.at[:, :, pl.ds(pl.multiple_of(peer * slice_width, slice_width), slice_width)]

    def slice_copy(hop, incoming):
        peer = (me + hop) % 8
        slot = mid_cols.at[(me + 8 - hop) % 8 if incoming else me]
        return pltpu.make_async_remote_copy(
            src_ref=slot if incoming else columns(peer), dst_ref=slot, send_sem=slice_send.at[hop],
            recv_sem=slice_recv.at[hop], device_id={'fsdp': peer}, device_id_type=MESH)

    def slice_own():
        return pltpu.make_async_copy(columns(me), mid_cols.at[me], slice_local)

    cols_in, cols_all = (h_cols, mid_cols), (h_spread, mid_spread)

    def cols_copy(idx, hop, incoming):
        slot = cols_all[idx].at[:, :, (me_model + 4 - hop) % 4 if incoming else me_model]
        return to_member(slot if incoming else cols_in[idx], slot, cols_send.at[idx, hop], cols_recv.at[idx, hop], hop)

    def cols_own(idx):
        return pltpu.make_async_copy(cols_in[idx], cols_all[idx].at[:, :, me_model], cols_local.at[idx])

    def mix_copy(hop, incoming):
        slot = mix.at[(me_model + 4 - hop) % 4 if incoming else me_model]
        return to_member(slot if incoming else gains, slot, mix_send.at[hop], mix_recv.at[hop], hop)

    def mix_own():
        return pltpu.make_async_copy(gains, mix.at[me_model], mix_local)

    def fetch(idx):
        return pltpu.make_async_copy((w_out_in, w_qkv_in)[idx], (w_out, w_qkv)[idx], fetch_sem.at[idx])

    def across(left, right):
        return lax.dot_general(left, right, (((1,), (1,)), ((), ())), preferred_element_type=f32)

    def along(left, right):
        return lax.dot_general(left, right, (((0,), (0,)), ((), ())), preferred_element_type=f32)

    def add_up(parts, seq, at):
        return ((parts[0, seq, at, :] + parts[1, seq, at, :]) + (parts[2, seq, at, :] + parts[3, seq, at, :])).astype(bf16).astype(f32)

    def norm_back(parts, saved, gain, base, result, first_row):
        row_sum[...] = jnp.zeros_like(row_sum)

        @pl.loop(0, block_rows // 16)
        def _(group):
            at = pl.ds(pl.multiple_of(group * 16, 16), 16)
            for seq in range(seqs):
                d_h = add_up(parts, seq, at)
                val = saved[seq, at, :].astype(f32)
                inv_rms = lax.rsqrt(jnp.mean(val * val, axis=-1, keepdims=True) + NORM_EPS)
                scaled = d_h * gain[...]
                slope = jnp.sum(scaled * val, axis=-1, keepdims=True) * (inv_rms * inv_rms * inv_rms) * (1.0 / d_model)
                result[seq, at, :] = (base[seq, at, :].astype(f32) + (scaled * inv_rms - val * slope)).astype(bf16)
                per_row = d_h * val * inv_rms
                row_sum[...] += per_row[:8] + per_row[8:]
        total = jnp.sum(row_sum[...], axis=0, keepdims=True)
        width = gains.shape[1]
        for row in range(d_model // width):
            gains[first_row + row:first_row + row + 1, :] = total[:, row * width:(row + 1) * width]

    def attention_back():
        d_attn[...] = across(d_full[...].reshape(seqs * seq_len, d_model), w_out[...]).astype(bf16)
        for seq in range(seqs):
            for head in range(heads):
                idx = seq * heads + head
                rows = slice(seq * seq_len, (seq + 1) * seq_len)
                d_out = d_attn[rows, head * head_dim:(head + 1) * head_dim]
                weight = prob[idx]
                d_prob = across(d_out, value[idx])
                row_dot = jnp.sum(d_prob * weight, axis=-1, keepdims=True)
                d_scores = (weight * (d_prob - row_dot) * head_dim ** -0.5).astype(bf16)
                d_query = jnp.dot(d_scores, key[idx], preferred_element_type=f32)
                d_key = along(d_scores, query[idx])
                d_value = along(weight.astype(bf16), d_out)
                for place_in, part in enumerate((d_query, d_key)):
                    turned = part * cos_ref[...] + pltpu.roll(part, head_dim // 2, 1) * sin_ref[...]
                    start = (3 * head + place_in) * head_dim
                    d_qkv[rows, start:start + head_dim] = turned.astype(bf16)
                d_qkv[rows, (3 * head + 2) * head_dim:(3 * head + 3) * head_dim] = d_value.astype(bf16)

        @pl.loop(0, d_model // TILE)
        def _(tile):
            cols = pl.ds(pl.multiple_of(tile * TILE, TILE), TILE)
            dh_attn[:, :, cols] = across(d_qkv[...], w_qkv[cols, :]).reshape(seqs, seq_len, TILE)

    start_ring((0, 1))
    blocks_start(0)
    blocks_start(1)
    for idx in range(4):
        for way in range(2):
            own(idx, way).start()
    for idx in range(2):
        fetch(idx).start()
    for hop in range(1, 4):
        cols_copy(0, hop, False).start()
    cols_own(0).start()
    for step in range(1, 7):
        forward((0, 1), step)
        if step == 2:
            blocks_wait(0)
            norm_back(dh_blocks, mid_ref, gain_mlp, dy_ref, d_mid, 8)
        if step == 3:
            for hop in range(1, 4):
                mid_copy(hop, False).start()
            mid_own().start()
            slice_own().start()
            for hop in range(1, 8):
                slice_copy(hop, False).start()
        if step == 5:
            blocks_wait(1)

            @pl.loop(0, block_rows // 16)
            def _(group):
                at = pl.ds(pl.multiple_of(group * 16, 16), 16)
                for seq in range(seqs):
                    y_ref[seq, at, :] = (mid_ref[seq, at, :].astype(f32) + add_up(y_blocks, seq, at)).astype(bf16)
    start_ring((2, 3))
    for step in range(1, 7):
        forward((2, 3), step)
        if step == 1:
            mid_own().wait()
            for hop in range(1, 4):
                mid_copy(hop, True).wait_recv()
                mid_copy(hop, False).wait_send()
            for idx in range(2):
                fetch(idx).wait()
            attention_back()
        if step == 2:
            blocks_start(2)
            slice_own().wait()
            for hop in range(1, 8):
                slice_copy(hop, True).wait_recv()
                slice_copy(hop, False).wait_send()
            for hop in range(1, 4):
                cols_copy(1, hop, False).start()
            cols_own(1).start()
        if step == 4:
            blocks_wait(2)
            norm_back(attn_blocks, x_ref, gain_attn, d_mid, dx_ref, 0)
        if step == 5:
            mix_own().start()
            for hop in range(1, 4):
                mix_copy(hop, False).start()
    start_ring((4,))
    mix_own().wait()
    for hop in range(1, 4):
        mix_copy(hop, True).wait_recv()
        mix_copy(hop, False).wait_send()
    start_ring((5,))
    for idx in (4, 5):
        for way in range(2):
            own(idx, way).start()
    for step in range(1, 7):
        forward((4, 5), step)
    for idx in range(6):
        for way in range(2):
            landed(idx, way, 6).wait_recv()
            own(idx, way).wait()
            for step in range(7):
                send(idx, way, step).wait_send()
    for idx in range(2):
        cols_own(idx).wait()
        for hop in range(1, 4):
            cols_copy(idx, hop, True).wait_recv()
            cols_copy(idx, hop, False).wait_send()


def ring_back(collective_id, *args):
    act, attn, d_gate, d_up, dh_part, y_part, h_cols, w_out, w_qkv, mid = args[:10]
    tokens = act.shape[0]
    seqs, seq_len, d_model = dh_part.shape
    bf16, f32 = jnp.bfloat16, jnp.float32
    qkv_cols = w_qkv.shape[1]
    sent = 7 * (3 * act.size + attn.size + tokens * qkv_cols) * 2
    dma = pltpu.SemaphoreType.DMA
    vmem = pl.BlockSpec(memory_space=pltpu.VMEM)
    hbm = pl.BlockSpec(memory_space=pl.ANY)
    shape = jax.ShapeDtypeStruct
    gain_shape = (16, d_model // 8)
    spread = shape(h_cols.shape[:2] + (4,) + h_cols.shape[2:], bf16)
    blocks = pltpu.VMEM((4,) + mid.shape, f32)
    return pl.pallas_call(
        back_kernel,
        out_shape=[shape((8 * tokens, array.shape[1]), bf16) for array in (act, attn, d_gate, d_up)]
        + [shape((8 * tokens, qkv_cols), bf16), shape((8, 4) + gain_shape, f32), shape((4,) + gain_shape, f32),
           shape(h_cols.shape, bf16), spread, spread, shape(mid.shape, bf16), shape(mid.shape, bf16)],
        in_specs=[hbm] * 9 + [vmem] * (len(args) - 9),
        out_specs=[hbm] * 10 + [vmem] * 2,
        scratch_shapes=[pltpu.VMEM(w_out.shape, bf16), pltpu.VMEM(w_qkv.shape, bf16), pltpu.VMEM(mid.shape, bf16),
                        pltpu.VMEM(dh_part.shape, bf16), pltpu.VMEM((tokens, w_out.shape[0]), bf16),
                        pltpu.VMEM((tokens, qkv_cols), bf16), pltpu.VMEM(dh_part.shape, f32), pltpu.VMEM(gain_shape, f32),
                        pltpu.VMEM((8, d_model), f32), blocks, blocks, blocks,
                        dma((6, 2, 7)), dma((6, 2, 7)), dma((6, 2)), dma((3, 4)), dma((3, 4)), dma((3,)),
                        dma((4,)), dma((4,)), dma, dma((8,)), dma((8,)), dma, dma((2, 4)), dma((2, 4)), dma((2,)),
                        dma((4,)), dma((4,)), dma, dma((2,))],
        compiler_params=pltpu.CompilerParams(collective_id=collective_id, has_side_effects=True,
                                             vmem_limit_bytes=60 * 1024 * 1024),
        cost_estimate=pl.CostEstimate(flops=sent * 3000, bytes_accessed=2 * sent, transcendentals=0),
        name=f'ring_back_{collective_id}',
    )(*args)


def solution(mesh):
    act_spec = P('fsdp', 'model', None)
    rows_spec = P('fsdp', 'model')
    cols_spec = P('model', 'fsdp')
    f32 = jnp.float32

    def device_fn(x_loc, dy_loc, gain_attn, gain_mlp, wqkv_sh, wout_sh, wgate_sh, wup_sh, wdown_sh, rope_cos, rope_sin):
        tokens = x_loc.shape[0] * rope_cos.shape[0]
        cos_two = jnp.concatenate([rope_cos, rope_cos], axis=1)
        sin_two = jnp.concatenate([rope_sin, -rope_sin], axis=1)
        gain_a, gain_m = gain_attn.reshape(1, -1), gain_mlp.reshape(1, -1)
        (w_qkv, w_out, _, _, h_mlp_cols, h_attn_cols, dy_cols, query, key_rot, value, prob, attn_flat, gated_act, d_gate, d_up,
         mlp_part, dh_part, mid) = ring_front(
            1, wqkv_sh, wout_sh, wdown_sh, wgate_sh, wup_sh, x_loc, dy_loc, gain_a, gain_m, cos_two, sin_two)
        whole = (x_loc.shape[0], rope_cos.shape[0], x_loc.shape[2])
        (act_all, attn_all, d_gate_all, d_up_all, d_qkv_all, gains_all, _, _, d_mid_cols, h_mlp_cols, y_loc, dx_loc) = ring_back(
            2, gated_act, attn_flat, d_gate, d_up, dh_part.reshape(whole), mlp_part.reshape(whole), h_mlp_cols, w_out, w_qkv,
            mid, x_loc, dy_loc, gain_m, gain_a, query, key_rot, value, prob, cos_two, sin_two)
        gain_grads = jnp.sum(gains_all, axis=(0, 1)).reshape(2, -1)
        h_attn_cols, dy_cols, h_mlp_cols, d_mid_cols = [
            cols.reshape(8 * tokens, -1) for cols in (h_attn_cols, dy_cols, h_mlp_cols, d_mid_cols)]

        def pair(left, right):
            return lax.dot_general(left, right, (((0,), (0,)), ((), ())), preferred_element_type=f32)

        return (y_loc, dx_loc, gain_grads[0], gain_grads[1],
                pair(h_attn_cols, d_qkv_all), pair(attn_all, d_mid_cols),
                pair(h_mlp_cols, d_gate_all), pair(h_mlp_cols, d_up_all), pair(act_all, dy_cols))

    in_specs = (act_spec, act_spec, P(), P(), rows_spec, cols_spec, rows_spec, rows_spec, cols_spec, P(), P())
    out_specs = (act_spec, act_spec, P(), P(), rows_spec, cols_spec, rows_spec, rows_spec, cols_spec)
    return jax.shard_map(device_fn, mesh=mesh, in_specs=in_specs, out_specs=out_specs, check_vma=False)
```

```python
import functools

import jax
import jax.numpy as jnp
from jax import lax
from jax.experimental import pallas as pl
from jax.experimental.pallas import tpu as pltpu
from jax.sharding import PartitionSpec as P

NORM_EPS = 1e-5
MESH = pl.DeviceIdType.MESH
WAYS, STEPS, LATER = range(2), range(7), range(1, 7)
MATES, OTHERS = range(1, 4), range(1, 8)
DMA = pltpu.SemaphoreType.DMA
MATE_SEMS, OTHER_SEMS, PAIR, TRIO = DMA((4,)), DMA((8,)), DMA((2,)), DMA((3,))
PAIR_MATES, TRIO_MATES, TRIO_OTHERS = DMA((2, 4)), DMA((3, 4)), DMA((3, 8))


def ring_place(index):
    z, y = index // 2, index % 2
    return z + y * (7 - 2 * z)


def ring_device(place):
    y = place // 4
    return 2 * (place + y * (7 - 2 * place)) + y


def neighbours(place):
    return ring_device((place + 1) % 8), ring_device((place + 7) % 8)


def owner_of(place, way, step):
    return ring_device((place + (8 - step if way == 0 else step)) % 8)


def enter(me, me_model):
    barrier = pltpu.get_barrier_semaphore()
    for hop in OTHERS:
        pl.semaphore_signal(barrier, inc=1, device_id={'fsdp': (me + hop) % 8}, device_id_type=MESH)
    for hop in MATES:
        pl.semaphore_signal(barrier, inc=1, device_id={'model': (me_model + hop) % 4}, device_id_type=MESH)
    pl.semaphore_wait(barrier, 10)


def member(me_model, hop, incoming):
    return (me_model + 4 - hop) % 4 if incoming else me_model


def across(left, right):
    return lax.dot_general(left, right, (((1,), (1,)), ((), ())), preferred_element_type=jnp.float32)


def along(left, right):
    return lax.dot_general(left, right, (((0,), (0,)), ((), ())), preferred_element_type=jnp.float32)


def tiles(width, tile_width, body):
    @pl.loop(0, width // tile_width)
    def _(tile):
        body(pl.ds(pl.multiple_of(tile * tile_width, tile_width), tile_width))


def wide_tables(cos_ref, sin_ref):
    cos_t, sin_t = cos_ref[...], sin_ref[...]
    return jnp.concatenate([cos_t, cos_t], axis=1), jnp.concatenate([sin_t, -sin_t], axis=1)


def sum_blocks(parts, seq, at):
    total = (parts[0, seq, at, :] + parts[1, seq, at, :]) + (parts[2, seq, at, :] + parts[3, seq, at, :])
    return total.astype(jnp.bfloat16).astype(jnp.float32)


TILE, GROUP = 512, 16


def front_kernel(qkv_sh, out_sh, down_sh, gate_sh, up_sh, x_ref, dy_in, gain_attn, gain_mlp, cos_ref, sin_ref,
                 w_qkv_all, w_out_all, attn_cols, dy_cols, h_cols, attn_spread, dy_spread,
                 query, key, value, prob, attn_flat, act_ref, d_gate_ref, d_up_ref, y_part_ref, dh_part_ref, mid_ref,
                 w_qkv, w_out, w_down, w_gate, w_up, qkv, attn_part, gate_acc, up_acc, d_act, ha_full, dy_full, h_full,
                 ha_loc, h_loc, blocks,
                 send_sem, recv_sem, local_sem, block_send, block_recv, block_local, seq_send, seq_recv, seq_local,
                 slice_send, slice_recv, slice_local, cols_send, cols_recv, cols_local, fetch_sem):
    f32, bf16 = jnp.float32, jnp.bfloat16
    me = lax.axis_index('fsdp')
    me_model = lax.axis_index('model')
    place = ring_place(me)
    targets = neighbours(place)
    enter(me, me_model)
    shards, weights = (qkv_sh, out_sh, down_sh, gate_sh, up_sh), (w_qkv_all, w_out_all, w_down, w_gate, w_up)
    accs = {3: gate_acc, 4: up_acc}
    rows, width = gate_sh.shape
    half = rows // 2
    seqs, block_rows, d_model = x_ref.shape
    seq_len = 4 * block_rows
    tokens = seqs * seq_len
    slice_width = h_cols.shape[3]
    head_dim = query.shape[2]
    heads = query.shape[0] // seqs

    def start_of(owner, way):
        return pl.multiple_of(owner * rows + way * half, half)

    def piece(idx, owner, way):
        if idx in (1, 2):
            tall = shards[idx].shape[0] // 2
            return weights[idx].at[pl.ds(way * tall, tall), pl.ds(pl.multiple_of(owner * rows, rows), rows)]
        return weights[idx].at[pl.ds(start_of(owner, way), half), :]

    def source(idx, way):
        size = shards[idx].shape[0] // 2
        return shards[idx].at[pl.ds(way * size, size), :]

    def owner_at(way, step):
        return owner_of(place, way, step)

    def send(idx, way, step):
        dst = piece(idx, owner_at(way, step), way)
        return pltpu.make_async_remote_copy(
            src_ref=source(idx, way) if isinstance(step, int) and step == 0 else dst, dst_ref=dst,
            send_sem=send_sem.at[idx, way, step], recv_sem=recv_sem.at[idx, way, step],
            device_id={'fsdp': targets[way]}, device_id_type=MESH)

    def landed(idx, way, step):
        dst = piece(idx, owner_at(way, step + 1), way)
        return pltpu.make_async_remote_copy(
            src_ref=dst, dst_ref=dst, send_sem=send_sem.at[idx, way, step], recv_sem=recv_sem.at[idx, way, step],
            device_id={'fsdp': targets[way]}, device_id_type=MESH)

    def own(idx, way):
        return pltpu.make_async_copy(source(idx, way), piece(idx, me, way), local_sem.at[idx, way])

    def start_ring(ids):
        for idx in ids:
            for way in WAYS:
                send(idx, way, 0).start()

    def forward(ids, step):
        for idx in ids:
            for way in WAYS:
                landed(idx, way, step - 1).wait_recv()
                send(idx, way, step).start()

    def finish_ring(ids):
        for idx in ids:
            for way in WAYS:
                landed(idx, way, 6).wait_recv()
                own(idx, way).wait()

    def to_member(src, dst, send_one, recv_one, hop):
        return pltpu.make_async_remote_copy(
            src_ref=src, dst_ref=dst, send_sem=send_one, recv_sem=recv_one,
            device_id={'model': (me_model + hop) % 4}, device_id_type=MESH)

    def rows_of(ref, who):
        return ref.at[:, pl.ds(pl.multiple_of(who * block_rows, block_rows), block_rows), :]

    def block_copy(hop, incoming):
        slot = blocks.at[member(me_model, hop, incoming)]
        src = slot if incoming else rows_of(attn_part, (me_model + hop) % 4)
        return to_member(src, slot, block_send.at[hop], block_recv.at[hop], hop)

    def block_own():
        return pltpu.make_async_copy(rows_of(attn_part, me_model), blocks.at[me_model], block_local)

    seq_src, seq_dst = (ha_loc, dy_in, h_loc), (ha_full, dy_full, h_full)
    slice_dst, spread_dst = (attn_cols, dy_cols, h_cols), (attn_spread, dy_spread)

    def seq_copy(idx, hop, incoming):
        slot = rows_of(seq_dst[idx], member(me_model, hop, incoming))
        return to_member(slot if incoming else seq_src[idx], slot, seq_send.at[idx, hop], seq_recv.at[idx, hop], hop)

    def seq_own(idx):
        return pltpu.make_async_copy(seq_src[idx], rows_of(seq_dst[idx], me_model), seq_local.at[idx])

    def columns(idx, peer):
        return seq_src[idx].at[:, :, pl.ds(pl.multiple_of(peer * slice_width, slice_width), slice_width)]

    def slice_copy(idx, hop, incoming):
        peer = (me + hop) % 8
        slot = slice_dst[idx].at[(me + 8 - hop) % 8 if incoming else me]
        return pltpu.make_async_remote_copy(
            src_ref=slot if incoming else columns(idx, peer), dst_ref=slot, send_sem=slice_send.at[idx, hop],
            recv_sem=slice_recv.at[idx, hop], device_id={'fsdp': peer}, device_id_type=MESH)

    def slice_own(idx):
        return pltpu.make_async_copy(columns(idx, me), slice_dst[idx].at[me], slice_local.at[idx])

    def hand_out(idx):
        for hop in MATES:
            seq_copy(idx, hop, False).start()
        seq_own(idx).start()
        slice_own(idx).start()
        for hop in OTHERS:
            slice_copy(idx, hop, False).start()

    def seq_wait(idx):
        seq_own(idx).wait()
        for hop in MATES:
            seq_copy(idx, hop, True).wait_recv()
            seq_copy(idx, hop, False).wait_send()

    def slice_wait(idx):
        slice_own(idx).wait()
        for hop in OTHERS:
            slice_copy(idx, hop, True).wait_recv()
            slice_copy(idx, hop, False).wait_send()

    def cols_copy(idx, hop, incoming):
        slot = spread_dst[idx].at[:, :, member(me_model, hop, incoming)]
        return to_member(slot if incoming else slice_dst[idx], slot, cols_send.at[idx, hop], cols_recv.at[idx, hop], hop)

    def cols_own(idx):
        return pltpu.make_async_copy(slice_dst[idx], spread_dst[idx].at[:, :, me_model], cols_local.at[idx])

    def fetch(idx):
        return pltpu.make_async_copy(weights[idx], (w_qkv, w_out)[idx], fetch_sem.at[idx])

    def normed(val, gain):
        return (val * lax.rsqrt(jnp.mean(val * val, axis=-1, keepdims=True) + NORM_EPS) * gain[...]).astype(bf16)

    def attention():
        cos_two, sin_two = wide_tables(cos_ref, sin_ref)
        @functools.partial(tiles, qkv.shape[1], TILE)
        def _(cols):
            qkv[:, cols] = jnp.dot(ha_full[...].reshape(tokens, d_model), w_qkv[:, cols], preferred_element_type=f32)
        causal = (lax.broadcasted_iota(jnp.int32, (seq_len, seq_len), 0)
                  >= lax.broadcasted_iota(jnp.int32, (seq_len, seq_len), 1))
        for seq in range(seqs):
            for head in range(heads):
                idx = seq * heads + head
                at = slice(seq * seq_len, (seq + 1) * seq_len)
                start = 3 * head * head_dim
                for place_in, turned_ref in enumerate((query, key)):
                    part = qkv[at, start + place_in * head_dim:start + (place_in + 1) * head_dim]
                    turned = part * cos_two - pltpu.roll(part, head_dim // 2, 1) * sin_two
                    turned_ref[idx] = turned.astype(bf16)
                value[idx] = qkv[at, start + 2 * head_dim:start + 3 * head_dim].astype(bf16)
                scores = jnp.where(causal, across(query[idx], key[idx]) * head_dim ** -0.5, -1e30)
                unnormed = jnp.exp(scores - jnp.max(scores, axis=-1, keepdims=True))
                weight = unnormed / jnp.sum(unnormed, axis=-1, keepdims=True)
                prob[idx] = weight
                mixed = jnp.dot(weight.astype(bf16), value[idx], preferred_element_type=f32)
                attn_flat[at, head * head_dim:(head + 1) * head_dim] = mixed.astype(bf16)

        @functools.partial(tiles, d_model, TILE)
        def _(cols):
            attn_part[:, :, cols] = jnp.dot(attn_flat[...], w_out[:, cols],
                                            preferred_element_type=f32).reshape(seqs, seq_len, TILE)

    def accumulate(step):
        for way in WAYS:
            start = start_of(owner_at(way, step), way)
            h_block = h_full[:, :, pl.ds(start, half)].reshape(tokens, half)
            for idx in (3, 4):
                @functools.partial(tiles, width, TILE)
                def _(cols):
                    accs[idx][:, cols] += jnp.dot(h_block, weights[idx][pl.ds(start, half), cols],
                                                  preferred_element_type=f32)

    start_ring((0, 1))
    for idx in range(5):
        for way in WAYS:
            own(idx, way).start()
    hand_out(1)

    @functools.partial(tiles, block_rows, GROUP)
    def _(at):
        for seq in range(seqs):
            ha_loc[seq, at, :] = normed(x_ref[seq, at, :].astype(f32), gain_attn)
    gate_acc[...] = jnp.zeros_like(gate_acc)
    up_acc[...] = jnp.zeros_like(up_acc)
    for step in LATER:
        forward((0, 1), step)
        if step == 1:
            hand_out(0)
    start_ring((2,))
    finish_ring((0, 1))
    for idx in WAYS:
        fetch(idx).start()
    for step in LATER:
        forward((2,), step)
        if step == 1:
            seq_wait(0)
            for idx in WAYS:
                fetch(idx).wait()
            attention()
        if step == 2:
            for hop in MATES:
                block_copy(hop, False).start()
            block_own().start()
        if step == 4:
            block_own().wait()
            for hop in MATES:
                block_copy(hop, True).wait_recv()
                block_copy(hop, False).wait_send()

            @functools.partial(tiles, block_rows, GROUP)
            def _(at):
                for seq in range(seqs):
                    mid = (x_ref[seq, at, :].astype(f32) + sum_blocks(blocks, seq, at)).astype(bf16)
                    mid_ref[seq, at, :] = mid
                    h_loc[seq, at, :] = normed(mid.astype(f32), gain_mlp)
        if step == 5:
            hand_out(2)
    start_ring((3, 4))
    seq_wait(1)
    for idx in WAYS:
        slice_wait(idx)
        for hop in MATES:
            cols_copy(idx, hop, False).start()
        cols_own(idx).start()
    finish_ring((2,))

    @functools.partial(tiles, width, TILE)
    def _(cols):
        d_act[:, cols] = across(dy_full[...].reshape(tokens, d_model), w_down[cols, :]).astype(bf16)

    seq_wait(2)
    for idx in (3, 4):
        for way in WAYS:
            own(idx, way).wait()
    accumulate(0)

    @pl.loop(1, 7)
    def _(step):
        forward((3, 4), step)
        accumulate(step)

    for idx in (3, 4):
        for way in WAYS:
            landed(idx, way, 6).wait_recv()
    accumulate(7)

    @functools.partial(tiles, width, 256)
    def _(cols):
        gate, up_proj = gate_acc[:, cols], up_acc[:, cols]
        d_val = d_act[:, cols].astype(f32)
        sig_gate = jax.nn.sigmoid(gate)
        silu_gate = gate * sig_gate
        act_ref[:, cols] = (silu_gate * up_proj).astype(bf16)
        d_gate_ref[:, cols] = (d_val * up_proj * sig_gate * (1.0 + gate * (1.0 - sig_gate))).astype(bf16)
        d_up_ref[:, cols] = (d_val * silu_gate).astype(bf16)

    @functools.partial(tiles, width, TILE)
    def _(cols):
        dh_part_ref[:, cols] = across(d_gate_ref[...], w_gate[cols, :]) + across(d_up_ref[...], w_up[cols, :])
        y_part_ref[:, cols] = jnp.dot(act_ref[...], w_down[:, cols], preferred_element_type=f32)

    for idx in range(5):
        for way in WAYS:
            for step in STEPS:
                send(idx, way, step).wait_send()
    slice_wait(2)
    for idx in WAYS:
        cols_own(idx).wait()
        for hop in MATES:
            cols_copy(idx, hop, True).wait_recv()
            cols_copy(idx, hop, False).wait_send()


def ring_front(collective_id, *args):
    qkv_sh, out_sh, down_sh, gate_sh, up_sh, x_loc, dy_loc = args[:7]
    seqs, block_rows, d_model = x_loc.shape
    seq_len, head_dim = args[9].shape[0], 2 * args[9].shape[1]
    tokens = seqs * seq_len
    width, qkv_cols, attn_cols = gate_sh.shape[1], qkv_sh.shape[1], out_sh.shape[0]
    sent = 7 * (qkv_sh.size + out_sh.size + 3 * gate_sh.size) * 2
    vmem = pl.BlockSpec(memory_space=pltpu.VMEM)
    hbm = pl.BlockSpec(memory_space=pl.ANY)
    bf16, f32 = jnp.bfloat16, jnp.float32
    shape, buf = jax.ShapeDtypeStruct, pltpu.VMEM
    sliced = shape((8, seqs, block_rows, d_model // 8), bf16)
    spread = shape((8, seqs, 4, block_rows, d_model // 8), bf16)
    per_head = shape((seqs * attn_cols // head_dim, seq_len, head_dim), bf16)
    hidden = shape((tokens, width), bf16)
    partial_sum = shape((tokens, d_model), f32)
    whole = (seqs, seq_len, d_model)
    return pl.pallas_call(
        front_kernel,
        out_shape=[shape((d_model, qkv_cols), bf16), shape((attn_cols, d_model), bf16), sliced, sliced, sliced, spread, spread,
                   per_head, per_head, per_head, shape((per_head.shape[0], seq_len, seq_len), f32),
                   shape((tokens, attn_cols), bf16), hidden, hidden, hidden, partial_sum, partial_sum, shape(x_loc.shape, bf16)],
        in_specs=[hbm] * 5 + [vmem] * 6,
        out_specs=[hbm] * 7 + [vmem] * 11,
        scratch_shapes=[buf((d_model, qkv_cols), bf16), buf((attn_cols, d_model), bf16), buf((width, d_model), bf16),
                        buf((d_model, width), bf16), buf((d_model, width), bf16), buf((tokens, qkv_cols), f32), buf(whole, f32),
                        buf((tokens, width), f32), buf((tokens, width), f32), buf((tokens, width), bf16),
                        buf(whole, bf16), buf(whole, bf16), buf(whole, bf16), buf(x_loc.shape, bf16), buf(x_loc.shape, bf16),
                        buf((4,) + x_loc.shape, f32),
                        DMA((5, 2, 7)), DMA((5, 2, 7)), DMA((5, 2)), MATE_SEMS, MATE_SEMS, DMA, TRIO_MATES, TRIO_MATES, TRIO,
                        TRIO_OTHERS, TRIO_OTHERS, TRIO, PAIR_MATES, PAIR_MATES, PAIR, PAIR],
        compiler_params=pltpu.CompilerParams(collective_id=collective_id, has_side_effects=True,
                                             vmem_limit_bytes=63 * 1024 * 1024),
        cost_estimate=pl.CostEstimate(flops=sent * 3000, bytes_accessed=2 * sent, transcendentals=0),
        name=f'ring_front_{collective_id}',
    )(*args)


def back_kernel(act, attn, d_gate, d_up, dh_part, y_part, h_cols, w_out_in, w_qkv_in, mid_ref, x_ref, dy_ref, gain_mlp, gain_attn,
                query, key, value, prob, cos_ref, sin_ref,
                act_all, attn_all, gate_all, up_all, qkv_all, gains_all, mix, mid_cols, mid_spread, h_spread, y_ref, dx_ref,
                w_out, w_qkv, d_mid, d_full, d_attn, d_qkv, dh_attn, gains, row_sum, dh_blocks, y_blocks, attn_blocks,
                send_sem, recv_sem, local_sem, block_send, block_recv, block_local, mid_send, mid_recv, mid_local,
                slice_send, slice_recv, slice_local, cols_send, cols_recv, cols_local, mix_send, mix_recv, mix_local, fetch_sem):
    f32, bf16 = jnp.float32, jnp.bfloat16
    me = lax.axis_index('fsdp')
    me_model = lax.axis_index('model')
    place = ring_place(me)
    targets = neighbours(place)
    enter(me, me_model)
    sources = (act, attn, d_gate, d_up, d_qkv)
    gathered = (act_all, attn_all, gate_all, up_all, qkv_all)
    seqs, block_rows, d_model = x_ref.shape
    seq_len = 4 * block_rows
    slice_width = mid_cols.shape[3]
    head_dim = query.shape[2]
    heads = query.shape[0] // seqs

    def piece(idx, owner, way):
        if idx == 5:
            return gains_all.at[owner, pl.ds(2 * way, 2)]
        rows = sources[idx].shape[0]
        return gathered[idx].at[pl.ds(pl.multiple_of(owner * rows + way * (rows // 2), rows // 2), rows // 2), :]

    def source(idx, way):
        if idx == 5:
            return mix.at[pl.ds(2 * way, 2)]
        half = sources[idx].shape[0] // 2
        return sources[idx].at[pl.ds(way * half, half), :]

    def owner_at(way, step):
        return owner_of(place, way, step)

    def send(idx, way, step):
        dst = piece(idx, owner_at(way, step), way)
        return pltpu.make_async_remote_copy(
            src_ref=source(idx, way) if step == 0 else dst, dst_ref=dst, send_sem=send_sem.at[idx, way, step],
            recv_sem=recv_sem.at[idx, way, step], device_id={'fsdp': targets[way]}, device_id_type=MESH)

    def landed(idx, way, step):
        dst = piece(idx, owner_at(way, step + 1), way)
        return pltpu.make_async_remote_copy(
            src_ref=dst, dst_ref=dst, send_sem=send_sem.at[idx, way, step], recv_sem=recv_sem.at[idx, way, step],
            device_id={'fsdp': targets[way]}, device_id_type=MESH)

    def own(idx, way):
        return pltpu.make_async_copy(source(idx, way), piece(idx, me, way), local_sem.at[idx, way])

    def start_ring(ids):
        for idx in ids:
            for way in WAYS:
                send(idx, way, 0).start()

    def forward(ids, step):
        for idx in ids:
            for way in WAYS:
                landed(idx, way, step - 1).wait_recv()
                send(idx, way, step).start()

    def to_member(src, dst, send_one, recv_one, hop):
        return pltpu.make_async_remote_copy(
            src_ref=src, dst_ref=dst, send_sem=send_one, recv_sem=recv_one,
            device_id={'model': (me_model + hop) % 4}, device_id_type=MESH)

    block_src, block_dst = (dh_part, y_part, dh_attn), (dh_blocks, y_blocks, attn_blocks)

    def block_of(idx, who):
        return block_src[idx].at[:, pl.ds(pl.multiple_of(who * block_rows, block_rows), block_rows), :]

    def block_copy(idx, hop, incoming):
        slot = block_dst[idx].at[member(me_model, hop, incoming)]
        src = slot if incoming else block_of(idx, (me_model + hop) % 4)
        return to_member(src, slot, block_send.at[idx, hop], block_recv.at[idx, hop], hop)

    def block_own(idx):
        return pltpu.make_async_copy(block_of(idx, me_model), block_dst[idx].at[me_model], block_local.at[idx])

    def blocks_start(idx):
        for hop in MATES:
            block_copy(idx, hop, False).start()
        block_own(idx).start()

    def blocks_wait(idx):
        block_own(idx).wait()
        for hop in MATES:
            block_copy(idx, hop, True).wait_recv()
            block_copy(idx, hop, False).wait_send()

    def mid_slot(who):
        return d_full.at[:, pl.ds(pl.multiple_of(who * block_rows, block_rows), block_rows), :]

    def mid_copy(hop, incoming):
        slot = mid_slot(member(me_model, hop, incoming))
        return to_member(slot if incoming else d_mid, slot, mid_send.at[hop], mid_recv.at[hop], hop)

    def mid_own():
        return pltpu.make_async_copy(d_mid, mid_slot(me_model), mid_local)

    def columns(peer):
        return d_mid.at[:, :, pl.ds(pl.multiple_of(peer * slice_width, slice_width), slice_width)]

    def slice_copy(hop, incoming):
        peer = (me + hop) % 8
        slot = mid_cols.at[(me + 8 - hop) % 8 if incoming else me]
        return pltpu.make_async_remote_copy(
            src_ref=slot if incoming else columns(peer), dst_ref=slot, send_sem=slice_send.at[hop],
            recv_sem=slice_recv.at[hop], device_id={'fsdp': peer}, device_id_type=MESH)

    def slice_own():
        return pltpu.make_async_copy(columns(me), mid_cols.at[me], slice_local)

    cols_in, cols_all = (h_cols, mid_cols), (h_spread, mid_spread)

    def cols_copy(idx, hop, incoming):
        slot = cols_all[idx].at[:, :, member(me_model, hop, incoming)]
        return to_member(slot if incoming else cols_in[idx], slot, cols_send.at[idx, hop], cols_recv.at[idx, hop], hop)

    def cols_own(idx):
        return pltpu.make_async_copy(cols_in[idx], cols_all[idx].at[:, :, me_model], cols_local.at[idx])

    def mix_copy(hop, incoming):
        slot = mix.at[member(me_model, hop, incoming)]
        return to_member(slot if incoming else gains, slot, mix_send.at[hop], mix_recv.at[hop], hop)

    def mix_own():
        return pltpu.make_async_copy(gains, mix.at[me_model], mix_local)

    def fetch(idx):
        return pltpu.make_async_copy((w_out_in, w_qkv_in)[idx], (w_out, w_qkv)[idx], fetch_sem.at[idx])

    def norm_back(parts, saved, gain, base, result, first_row):
        row_sum[...] = jnp.zeros_like(row_sum)

        @functools.partial(tiles, block_rows, GROUP)
        def _(at):
            for seq in range(seqs):
                d_h = sum_blocks(parts, seq, at)
                val = saved[seq, at, :].astype(f32)
                inv_rms = lax.rsqrt(jnp.mean(val * val, axis=-1, keepdims=True) + NORM_EPS)
                scaled = d_h * gain[...]
                slope = jnp.sum(scaled * val, axis=-1, keepdims=True) * (inv_rms * inv_rms * inv_rms) * (1.0 / d_model)
                result[seq, at, :] = (base[seq, at, :].astype(f32) + (scaled * inv_rms - val * slope)).astype(bf16)
                per_row = d_h * val * inv_rms
                row_sum[...] += per_row[:8] + per_row[8:]
        total = jnp.sum(row_sum[...], axis=0, keepdims=True)
        width = gains.shape[1]
        for row in range(d_model // width):
            gains[first_row + row:first_row + row + 1, :] = total[:, row * width:(row + 1) * width]

    def attention_back():
        cos_two, sin_two = wide_tables(cos_ref, sin_ref)
        d_attn[...] = across(d_full[...].reshape(seqs * seq_len, d_model), w_out[...]).astype(bf16)
        for seq in range(seqs):
            for head in range(heads):
                idx = seq * heads + head
                rows = slice(seq * seq_len, (seq + 1) * seq_len)
                d_out = d_attn[rows, head * head_dim:(head + 1) * head_dim]
                weight = prob[idx]
                d_prob = across(d_out, value[idx])
                row_dot = jnp.sum(d_prob * weight, axis=-1, keepdims=True)
                d_scores = (weight * (d_prob - row_dot) * head_dim ** -0.5).astype(bf16)
                d_query = jnp.dot(d_scores, key[idx], preferred_element_type=f32)
                d_key = along(d_scores, query[idx])
                d_value = along(weight.astype(bf16), d_out)
                for place_in, part in enumerate((d_query, d_key)):
                    turned = part * cos_two + pltpu.roll(part, head_dim // 2, 1) * sin_two
                    start = (3 * head + place_in) * head_dim
                    d_qkv[rows, start:start + head_dim] = turned.astype(bf16)
                d_qkv[rows, (3 * head + 2) * head_dim:(3 * head + 3) * head_dim] = d_value.astype(bf16)

        @functools.partial(tiles, d_model, TILE)
        def _(cols):
            dh_attn[:, :, cols] = across(d_qkv[...], w_qkv[cols, :]).reshape(seqs, seq_len, TILE)

    start_ring((0, 1))
    blocks_start(0)
    blocks_start(1)
    for idx in range(4):
        for way in WAYS:
            own(idx, way).start()
    for idx in WAYS:
        fetch(idx).start()
    for hop in MATES:
        cols_copy(0, hop, False).start()
    cols_own(0).start()
    for step in LATER:
        forward((0, 1), step)
        if step == 2:
            blocks_wait(0)
            norm_back(dh_blocks, mid_ref, gain_mlp, dy_ref, d_mid, 8)
        if step == 3:
            for hop in MATES:
                mid_copy(hop, False).start()
            mid_own().start()
            slice_own().start()
            for hop in OTHERS:
                slice_copy(hop, False).start()
        if step == 5:
            blocks_wait(1)

            @functools.partial(tiles, block_rows, GROUP)
            def _(at):
                for seq in range(seqs):
                    y_ref[seq, at, :] = (mid_ref[seq, at, :].astype(f32) + sum_blocks(y_blocks, seq, at)).astype(bf16)
    start_ring((2, 3))
    for step in LATER:
        forward((2, 3), step)
        if step == 1:
            mid_own().wait()
            for hop in MATES:
                mid_copy(hop, True).wait_recv()
                mid_copy(hop, False).wait_send()
            for idx in WAYS:
                fetch(idx).wait()
            attention_back()
        if step == 2:
            blocks_start(2)
            slice_own().wait()
            for hop in OTHERS:
                slice_copy(hop, True).wait_recv()
                slice_copy(hop, False).wait_send()
            for hop in MATES:
                cols_copy(1, hop, False).start()
            cols_own(1).start()
        if step == 4:
            blocks_wait(2)
            norm_back(attn_blocks, x_ref, gain_attn, d_mid, dx_ref, 0)
        if step == 5:
            mix_own().start()
            for hop in MATES:
                mix_copy(hop, False).start()
    start_ring((4,))
    mix_own().wait()
    for hop in MATES:
        mix_copy(hop, True).wait_recv()
        mix_copy(hop, False).wait_send()
    start_ring((5,))
    for idx in (4, 5):
        for way in WAYS:
            own(idx, way).start()
    for step in LATER:
        forward((4, 5), step)
    for idx in range(6):
        for way in WAYS:
            landed(idx, way, 6).wait_recv()
            own(idx, way).wait()
            for step in STEPS:
                send(idx, way, step).wait_send()
    for idx in WAYS:
        cols_own(idx).wait()
        for hop in MATES:
            cols_copy(idx, hop, True).wait_recv()
            cols_copy(idx, hop, False).wait_send()


def ring_back(collective_id, *args):
    act, attn, d_gate, d_up, dh_part, y_part, h_cols, w_out, w_qkv, mid = args[:10]
    tokens = act.shape[0]
    seqs, seq_len, d_model = dh_part.shape
    bf16, f32 = jnp.bfloat16, jnp.float32
    qkv_cols = w_qkv.shape[1]
    sent = 7 * (3 * act.size + attn.size + tokens * qkv_cols) * 2
    vmem = pl.BlockSpec(memory_space=pltpu.VMEM)
    hbm = pl.BlockSpec(memory_space=pl.ANY)
    shape = jax.ShapeDtypeStruct
    gain_shape = (16, d_model // 8)
    spread = shape(h_cols.shape[:2] + (4,) + h_cols.shape[2:], bf16)
    blocks = pltpu.VMEM((4,) + mid.shape, f32)
    return pl.pallas_call(
        back_kernel,
        out_shape=[shape((8 * tokens, array.shape[1]), bf16) for array in (act, attn, d_gate, d_up)]
        + [shape((8 * tokens, qkv_cols), bf16), shape((8, 4) + gain_shape, f32), shape((4,) + gain_shape, f32),
           shape(h_cols.shape, bf16), spread, spread, shape(mid.shape, bf16), shape(mid.shape, bf16)],
        in_specs=[hbm] * 9 + [vmem] * (len(args) - 9),
        out_specs=[hbm] * 10 + [vmem] * 2,
        scratch_shapes=[pltpu.VMEM(w_out.shape, bf16), pltpu.VMEM(w_qkv.shape, bf16), pltpu.VMEM(mid.shape, bf16),
                        pltpu.VMEM(dh_part.shape, bf16), pltpu.VMEM((tokens, w_out.shape[0]), bf16),
                        pltpu.VMEM((tokens, qkv_cols), bf16), pltpu.VMEM(dh_part.shape, f32), pltpu.VMEM(gain_shape, f32),
                        pltpu.VMEM((8, d_model), f32), blocks, blocks, blocks,
                        DMA((6, 2, 7)), DMA((6, 2, 7)), DMA((6, 2)), TRIO_MATES, TRIO_MATES, TRIO,
                        MATE_SEMS, MATE_SEMS, DMA, OTHER_SEMS, OTHER_SEMS, DMA, PAIR_MATES, PAIR_MATES, PAIR,
                        MATE_SEMS, MATE_SEMS, DMA, PAIR],
        compiler_params=pltpu.CompilerParams(collective_id=collective_id, has_side_effects=True,
                                             vmem_limit_bytes=60 * 1024 * 1024),
        cost_estimate=pl.CostEstimate(flops=sent * 3000, bytes_accessed=2 * sent, transcendentals=0),
        name=f'ring_back_{collective_id}',
    )(*args)


def solution(mesh):
    act_spec = P('fsdp', 'model', None)
    rows_spec = P('fsdp', 'model')
    cols_spec = P('model', 'fsdp')
    f32 = jnp.float32

    def device_fn(x_loc, dy_loc, gain_attn, gain_mlp, wqkv_sh, wout_sh, wgate_sh, wup_sh, wdown_sh, rope_cos, rope_sin):
        tokens = x_loc.shape[0] * rope_cos.shape[0]
        gain_a, gain_m = gain_attn.reshape(1, -1), gain_mlp.reshape(1, -1)
        (w_qkv, w_out, _, _, h_mlp_cols, h_attn_cols, dy_cols, query, key_rot, value, prob, attn_flat, gated_act, d_gate, d_up,
         mlp_part, dh_part, mid) = ring_front(
            1, wqkv_sh, wout_sh, wdown_sh, wgate_sh, wup_sh, x_loc, dy_loc, gain_a, gain_m, rope_cos, rope_sin)
        whole = (x_loc.shape[0], rope_cos.shape[0], x_loc.shape[2])
        (act_all, attn_all, d_gate_all, d_up_all, d_qkv_all, gains_all, _, _, d_mid_cols, h_mlp_cols, y_loc, dx_loc) = ring_back(
            2, gated_act, attn_flat, d_gate, d_up, dh_part.reshape(whole), mlp_part.reshape(whole), h_mlp_cols, w_out, w_qkv,
            mid, x_loc, dy_loc, gain_m, gain_a, query, key_rot, value, prob, rope_cos, rope_sin)
        gain_grads = jnp.sum(gains_all, axis=(0, 1)).reshape(2, -1)
        h_attn_cols, dy_cols, h_mlp_cols, d_mid_cols = [
            cols.reshape(8 * tokens, -1) for cols in (h_attn_cols, dy_cols, h_mlp_cols, d_mid_cols)]

        def pair(left, right):
            return lax.dot_general(left, right, (((0,), (0,)), ((), ())), preferred_element_type=f32)

        return (y_loc, dx_loc, gain_grads[0], gain_grads[1],
                pair(h_attn_cols, d_qkv_all), pair(attn_all, d_mid_cols),
                pair(h_mlp_cols, d_gate_all), pair(h_mlp_cols, d_up_all), pair(act_all, dy_cols))

    in_specs = (act_spec, act_spec, P(), P(), rows_spec, cols_spec, rows_spec, rows_spec, cols_spec, P(), P())
    out_specs = (act_spec, act_spec, P(), P(), rows_spec, cols_spec, rows_spec, rows_spec, cols_spec)
    return jax.shard_map(device_fn, mesh=mesh, in_specs=in_specs, out_specs=out_specs, check_vma=False)
```

```python
import functools

import jax
import jax.numpy as jnp
from jax import lax
from jax.experimental import pallas as pl
from jax.experimental.pallas import tpu as pltpu
from jax.sharding import PartitionSpec as P

NORM_EPS = 1e-5
MESH = pl.DeviceIdType.MESH
WAYS, STEPS, LATER = range(2), range(7), range(1, 7)
MATES, OTHERS = range(1, 4), range(1, 8)
DMA = pltpu.SemaphoreType.DMA
MATE_SEMS, OTHER_SEMS, PAIR, TRIO = DMA((4,)), DMA((8,)), DMA((2,)), DMA((3,))
PAIR_MATES, TRIO_MATES, TRIO_OTHERS = DMA((2, 4)), DMA((3, 4)), DMA((3, 8))


def ring_place(index):
    z, y = index // 2, index % 2
    return z + y * (7 - 2 * z)


def ring_device(place):
    y = place // 4
    return 2 * (place + y * (7 - 2 * place)) + y


def neighbours(place):
    return ring_device((place + 1) % 8), ring_device((place + 7) % 8)


def owner_of(place, way, step):
    return ring_device((place + (8 - step if way == 0 else step)) % 8)


def enter(me, me_model):
    barrier = pltpu.get_barrier_semaphore()
    for hop in OTHERS:
        pl.semaphore_signal(barrier, inc=1, device_id={'fsdp': (me + hop) % 8}, device_id_type=MESH)
    for hop in MATES:
        pl.semaphore_signal(barrier, inc=1, device_id={'model': (me_model + hop) % 4}, device_id_type=MESH)
    pl.semaphore_wait(barrier, 10)


def member(me_model, hop, incoming):
    return (me_model + 4 - hop) % 4 if incoming else me_model


def across(left, right):
    return lax.dot_general(left, right, (((1,), (1,)), ((), ())), preferred_element_type=jnp.float32)


def along(left, right):
    return lax.dot_general(left, right, (((0,), (0,)), ((), ())), preferred_element_type=jnp.float32)


def tiles(width, tile_width, body):
    @pl.loop(0, width // tile_width)
    def _(tile):
        body(pl.ds(pl.multiple_of(tile * tile_width, tile_width), tile_width))


def wide_tables(cos_ref, sin_ref):
    cos_t, sin_t = cos_ref[...], sin_ref[...]
    return jnp.concatenate([cos_t, cos_t], axis=1), jnp.concatenate([sin_t, -sin_t], axis=1)


def sum_blocks(parts, seq, at):
    total = (parts[0, seq, at, :] + parts[1, seq, at, :]) + (parts[2, seq, at, :] + parts[3, seq, at, :])
    return total.astype(jnp.bfloat16).astype(jnp.float32)


TILE, GROUP = 512, 16


def front_kernel(qkv_sh, out_sh, down_sh, gate_sh, up_sh, x_ref, dy_in, gain_attn, gain_mlp, cos_ref, sin_ref,
                 w_qkv_all, w_out_all, attn_cols, dy_cols, h_cols, attn_spread, dy_spread,
                 query, key, value, prob, attn_flat, act_ref, d_gate_ref, d_up_ref, y_part_ref, dh_part_ref, mid_ref,
                 w_qkv, w_out, w_down, w_gate, w_up, qkv, attn_part, gate_acc, up_acc, d_act, ha_full, dy_full, h_full,
                 ha_loc, h_loc, blocks,
                 send_sem, recv_sem, local_sem, block_send, block_recv, block_local, seq_send, seq_recv, seq_local,
                 slice_send, slice_recv, slice_local, cols_send, cols_recv, cols_local, fetch_sem):
    f32, bf16 = jnp.float32, jnp.bfloat16
    me = lax.axis_index('fsdp')
    me_model = lax.axis_index('model')
    place = ring_place(me)
    targets = neighbours(place)
    enter(me, me_model)
    shards, weights = (qkv_sh, out_sh, down_sh, gate_sh, up_sh), (w_qkv_all, w_out_all, w_down, w_gate, w_up)
    accs = {3: gate_acc, 4: up_acc}
    rows, width = gate_sh.shape
    half = rows // 2
    seqs, block_rows, d_model = x_ref.shape
    seq_len = 4 * block_rows
    tokens = seqs * seq_len
    slice_width = h_cols.shape[3]
    head_dim = query.shape[2]
    heads = query.shape[0] // seqs

    def start_of(owner, way):
        return pl.multiple_of(owner * rows + way * half, half)

    def piece(idx, owner, way):
        if idx in (1, 2):
            tall = shards[idx].shape[0] // 2
            return weights[idx].at[pl.ds(way * tall, tall), pl.ds(pl.multiple_of(owner * rows, rows), rows)]
        return weights[idx].at[pl.ds(start_of(owner, way), half), :]

    def source(idx, way):
        size = shards[idx].shape[0] // 2
        return shards[idx].at[pl.ds(way * size, size), :]

    def owner_at(way, step):
        return owner_of(place, way, step)

    def send(idx, way, step):
        dst = piece(idx, owner_at(way, step), way)
        return pltpu.make_async_remote_copy(
            src_ref=source(idx, way) if isinstance(step, int) and step == 0 else dst, dst_ref=dst,
            send_sem=send_sem.at[idx, way, step], recv_sem=recv_sem.at[idx, way, step],
            device_id={'fsdp': targets[way]}, device_id_type=MESH)

    def landed(idx, way, step):
        dst = piece(idx, owner_at(way, step + 1), way)
        return pltpu.make_async_remote_copy(
            src_ref=dst, dst_ref=dst, send_sem=send_sem.at[idx, way, step], recv_sem=recv_sem.at[idx, way, step],
            device_id={'fsdp': targets[way]}, device_id_type=MESH)

    def own(idx, way):
        return pltpu.make_async_copy(source(idx, way), piece(idx, me, way), local_sem.at[idx, way])

    def start_ring(ids):
        for idx in ids:
            for way in WAYS:
                send(idx, way, 0).start()

    def forward(ids, step):
        for idx in ids:
            for way in WAYS:
                landed(idx, way, step - 1).wait_recv()
                send(idx, way, step).start()

    def finish_ring(ids):
        for idx in ids:
            for way in WAYS:
                landed(idx, way, 6).wait_recv()
                own(idx, way).wait()

    def to_member(src, dst, send_one, recv_one, hop):
        return pltpu.make_async_remote_copy(
            src_ref=src, dst_ref=dst, send_sem=send_one, recv_sem=recv_one,
            device_id={'model': (me_model + hop) % 4}, device_id_type=MESH)

    def rows_of(ref, who):
        return ref.at[:, pl.ds(pl.multiple_of(who * block_rows, block_rows), block_rows), :]

    def block_copy(hop, incoming):
        slot = blocks.at[member(me_model, hop, incoming)]
        src = slot if incoming else rows_of(attn_part, (me_model + hop) % 4)
        return to_member(src, slot, block_send.at[hop], block_recv.at[hop], hop)

    def block_own():
        return pltpu.make_async_copy(rows_of(attn_part, me_model), blocks.at[me_model], block_local)

    seq_src, seq_dst = (ha_loc, dy_in, h_loc), (ha_full, dy_full, h_full)
    slice_dst, spread_dst = (attn_cols, dy_cols, h_cols), (attn_spread, dy_spread)

    def seq_copy(idx, hop, incoming):
        slot = rows_of(seq_dst[idx], member(me_model, hop, incoming))
        return to_member(slot if incoming else seq_src[idx], slot, seq_send.at[idx, hop], seq_recv.at[idx, hop], hop)

    def seq_own(idx):
        return pltpu.make_async_copy(seq_src[idx], rows_of(seq_dst[idx], me_model), seq_local.at[idx])

    def columns(idx, peer):
        return seq_src[idx].at[:, :, pl.ds(pl.multiple_of(peer * slice_width, slice_width), slice_width)]

    def slice_copy(idx, hop, incoming):
        peer = (me + hop) % 8
        slot = slice_dst[idx].at[(me + 8 - hop) % 8 if incoming else me]
        return pltpu.make_async_remote_copy(
            src_ref=slot if incoming else columns(idx, peer), dst_ref=slot, send_sem=slice_send.at[idx, hop],
            recv_sem=slice_recv.at[idx, hop], device_id={'fsdp': peer}, device_id_type=MESH)

    def slice_own(idx):
        return pltpu.make_async_copy(columns(idx, me), slice_dst[idx].at[me], slice_local.at[idx])

    def hand_out(idx):
        for hop in MATES:
            seq_copy(idx, hop, False).start()
        seq_own(idx).start()
        slice_own(idx).start()
        for hop in OTHERS:
            slice_copy(idx, hop, False).start()

    def seq_wait(idx):
        seq_own(idx).wait()
        for hop in MATES:
            seq_copy(idx, hop, True).wait_recv()
            seq_copy(idx, hop, False).wait_send()

    def slice_wait(idx):
        slice_own(idx).wait()
        for hop in OTHERS:
            slice_copy(idx, hop, True).wait_recv()
            slice_copy(idx, hop, False).wait_send()

    def cols_copy(idx, hop, incoming):
        slot = spread_dst[idx].at[:, :, member(me_model, hop, incoming)]
        return to_member(slot if incoming else slice_dst[idx], slot, cols_send.at[idx, hop], cols_recv.at[idx, hop], hop)

    def cols_own(idx):
        return pltpu.make_async_copy(slice_dst[idx], spread_dst[idx].at[:, :, me_model], cols_local.at[idx])

    def fetch(idx):
        return pltpu.make_async_copy(weights[idx], (w_qkv, w_out)[idx], fetch_sem.at[idx])

    def normed(val, gain):
        return (val * lax.rsqrt(jnp.mean(val * val, axis=-1, keepdims=True) + NORM_EPS) * gain[...]).astype(bf16)

    def attention():
        cos_two, sin_two = wide_tables(cos_ref, sin_ref)
        @functools.partial(tiles, qkv.shape[1], TILE)
        def _(cols):
            qkv[:, cols] = jnp.dot(ha_full[...].reshape(tokens, d_model), w_qkv[:, cols], preferred_element_type=f32)
        causal = (lax.broadcasted_iota(jnp.int32, (seq_len, seq_len), 0)
                  >= lax.broadcasted_iota(jnp.int32, (seq_len, seq_len), 1))
        for seq in range(seqs):
            for head in range(heads):
                idx = seq * heads + head
                at = slice(seq * seq_len, (seq + 1) * seq_len)
                start = 3 * head * head_dim
                for place_in, turned_ref in enumerate((query, key)):
                    part = qkv[at, start + place_in * head_dim:start + (place_in + 1) * head_dim]
                    turned = part * cos_two - pltpu.roll(part, head_dim // 2, 1) * sin_two
                    turned_ref[idx] = turned.astype(bf16)
                value[idx] = qkv[at, start + 2 * head_dim:start + 3 * head_dim].astype(bf16)
                scores = jnp.where(causal, across(query[idx], key[idx]) * head_dim ** -0.5, -1e30)
                unnormed = jnp.exp(scores - jnp.max(scores, axis=-1, keepdims=True))
                weight = unnormed / jnp.sum(unnormed, axis=-1, keepdims=True)
                prob[idx] = weight
                mixed = jnp.dot(weight.astype(bf16), value[idx], preferred_element_type=f32)
                attn_flat[at, head * head_dim:(head + 1) * head_dim] = mixed.astype(bf16)

        @functools.partial(tiles, d_model, TILE)
        def _(cols):
            attn_part[:, :, cols] = jnp.dot(attn_flat[...], w_out[:, cols],
                                            preferred_element_type=f32).reshape(seqs, seq_len, TILE)

    def accumulate(step):
        for way in WAYS:
            start = start_of(owner_at(way, step), way)
            h_block = h_full[:, :, pl.ds(start, half)].reshape(tokens, half)
            for idx in (3, 4):
                @functools.partial(tiles, width, TILE)
                def _(cols):
                    accs[idx][:, cols] += jnp.dot(h_block, weights[idx][pl.ds(start, half), cols],
                                                  preferred_element_type=f32)

    start_ring((0, 1))
    for idx in range(5):
        for way in WAYS:
            own(idx, way).start()
    hand_out(1)

    @functools.partial(tiles, block_rows, GROUP)
    def _(at):
        for seq in range(seqs):
            ha_loc[seq, at, :] = normed(x_ref[seq, at, :].astype(f32), gain_attn)
    gate_acc[...] = jnp.zeros_like(gate_acc)
    up_acc[...] = jnp.zeros_like(up_acc)
    for step in LATER:
        forward((0, 1), step)
        if step == 1:
            hand_out(0)
    start_ring((2,))
    finish_ring((0, 1))
    for idx in WAYS:
        fetch(idx).start()
    for step in LATER:
        forward((2,), step)
        if step == 1:
            seq_wait(0)
            for idx in WAYS:
                fetch(idx).wait()
            attention()
        if step == 2:
            for hop in MATES:
                block_copy(hop, False).start()
            block_own().start()
        if step == 4:
            block_own().wait()
            for hop in MATES:
                block_copy(hop, True).wait_recv()
                block_copy(hop, False).wait_send()

            @functools.partial(tiles, block_rows, GROUP)
            def _(at):
                for seq in range(seqs):
                    mid = (x_ref[seq, at, :].astype(f32) + sum_blocks(blocks, seq, at)).astype(bf16)
                    mid_ref[seq, at, :] = mid
                    h_loc[seq, at, :] = normed(mid.astype(f32), gain_mlp)
        if step == 5:
            hand_out(2)
    start_ring((3, 4))
    seq_wait(1)
    for idx in WAYS:
        slice_wait(idx)
        for hop in MATES:
            cols_copy(idx, hop, False).start()
        cols_own(idx).start()
    finish_ring((2,))

    @functools.partial(tiles, width, TILE)
    def _(cols):
        d_act[:, cols] = across(dy_full[...].reshape(tokens, d_model), w_down[cols, :]).astype(bf16)

    seq_wait(2)
    for idx in (3, 4):
        for way in WAYS:
            own(idx, way).wait()
    accumulate(0)

    @pl.loop(1, 7)
    def _(step):
        forward((3, 4), step)
        accumulate(step)

    for idx in (3, 4):
        for way in WAYS:
            landed(idx, way, 6).wait_recv()
    accumulate(7)

    @functools.partial(tiles, width, 256)
    def _(cols):
        gate, up_proj = gate_acc[:, cols], up_acc[:, cols]
        d_val = d_act[:, cols].astype(f32)
        sig_gate = jax.nn.sigmoid(gate)
        silu_gate = gate * sig_gate
        act_ref[:, cols] = (silu_gate * up_proj).astype(bf16)
        d_gate_ref[:, cols] = (d_val * up_proj * sig_gate * (1.0 + gate * (1.0 - sig_gate))).astype(bf16)
        d_up_ref[:, cols] = (d_val * silu_gate).astype(bf16)

    @functools.partial(tiles, width, TILE)
    def _(cols):
        dh_part_ref[:, cols] = across(d_gate_ref[...], w_gate[cols, :]) + across(d_up_ref[...], w_up[cols, :])
        y_part_ref[:, cols] = jnp.dot(act_ref[...], w_down[:, cols], preferred_element_type=f32)

    for idx in range(5):
        for way in WAYS:
            for step in STEPS:
                send(idx, way, step).wait_send()
    slice_wait(2)
    for idx in WAYS:
        cols_own(idx).wait()
        for hop in MATES:
            cols_copy(idx, hop, True).wait_recv()
            cols_copy(idx, hop, False).wait_send()


def ring_front(collective_id, *args):
    qkv_sh, out_sh, down_sh, gate_sh, up_sh, x_loc, dy_loc = args[:7]
    seqs, block_rows, d_model = x_loc.shape
    seq_len, head_dim = args[9].shape[0], 2 * args[9].shape[1]
    tokens = seqs * seq_len
    width, qkv_cols, attn_cols = gate_sh.shape[1], qkv_sh.shape[1], out_sh.shape[0]
    sent = 7 * (qkv_sh.size + out_sh.size + 3 * gate_sh.size) * 2
    vmem = pl.BlockSpec(memory_space=pltpu.VMEM)
    hbm = pl.BlockSpec(memory_space=pl.ANY)
    bf16, f32 = jnp.bfloat16, jnp.float32
    shape, buf = jax.ShapeDtypeStruct, pltpu.VMEM
    sliced = shape((8, seqs, block_rows, d_model // 8), bf16)
    spread = shape((8, seqs, 4, block_rows, d_model // 8), bf16)
    per_head = shape((seqs * attn_cols // head_dim, seq_len, head_dim), bf16)
    hidden = shape((tokens, width), bf16)
    partial_sum = shape((tokens, d_model), f32)
    whole = (seqs, seq_len, d_model)
    return pl.pallas_call(
        front_kernel,
        out_shape=[shape((d_model, qkv_cols), bf16), shape((attn_cols, d_model), bf16), sliced, sliced, sliced, spread, spread,
                   per_head, per_head, per_head, shape((per_head.shape[0], seq_len, seq_len), f32),
                   shape((tokens, attn_cols), bf16), hidden, hidden, hidden, partial_sum, partial_sum, shape(x_loc.shape, bf16)],
        in_specs=[hbm] * 5 + [vmem] * 6,
        out_specs=[hbm] * 7 + [vmem] * 11,
        scratch_shapes=[buf((d_model, qkv_cols), bf16), buf((attn_cols, d_model), bf16), buf((width, d_model), bf16),
                        buf((d_model, width), bf16), buf((d_model, width), bf16), buf((tokens, qkv_cols), f32), buf(whole, f32),
                        buf((tokens, width), f32), buf((tokens, width), f32), buf((tokens, width), bf16),
                        buf(whole, bf16), buf(whole, bf16), buf(whole, bf16), buf(x_loc.shape, bf16), buf(x_loc.shape, bf16),
                        buf((4,) + x_loc.shape, f32),
                        DMA((5, 2, 7)), DMA((5, 2, 7)), DMA((5, 2)), MATE_SEMS, MATE_SEMS, DMA, TRIO_MATES, TRIO_MATES, TRIO,
                        TRIO_OTHERS, TRIO_OTHERS, TRIO, PAIR_MATES, PAIR_MATES, PAIR, PAIR],
        compiler_params=pltpu.CompilerParams(collective_id=collective_id, has_side_effects=True,
                                             vmem_limit_bytes=63 * 1024 * 1024),
        cost_estimate=pl.CostEstimate(flops=sent * 3000, bytes_accessed=2 * sent, transcendentals=0),
        name=f'ring_front_{collective_id}',
    )(*args)


def back_kernel(act, attn, d_gate, d_up, dh_part, y_part, h_cols, w_out_in, w_qkv_in, mid_ref, x_ref, dy_ref, gain_mlp, gain_attn,
                query, key, value, prob, cos_ref, sin_ref, dy_spread,
                dw_down, dw_out, dw_gate, dw_up, act_all, attn_all, gate_all, up_all, qkv_all, gains_all, mix, mid_cols, mid_spread, h_spread, y_ref, dx_ref,
                w_out, w_qkv, d_mid, d_full, d_attn, d_qkv, dh_attn, gains, row_sum, dh_blocks, y_blocks, attn_blocks,
                send_sem, recv_sem, local_sem, block_send, block_recv, block_local, mid_send, mid_recv, mid_local,
                slice_send, slice_recv, slice_local, cols_send, cols_recv, cols_local, mix_send, mix_recv, mix_local, fetch_sem,
                small, big, tall, flat, small_sem, big_sem, product_sem):
    f32, bf16 = jnp.float32, jnp.bfloat16
    me = lax.axis_index('fsdp')
    me_model = lax.axis_index('model')
    place = ring_place(me)
    targets = neighbours(place)
    enter(me, me_model)
    sources = (act, attn, d_gate, d_up, d_qkv)
    gathered = (act_all, attn_all, gate_all, up_all, qkv_all)
    seqs, block_rows, d_model = x_ref.shape
    seq_len = 4 * block_rows
    slice_width = mid_cols.shape[3]
    head_dim = query.shape[2]
    heads = query.shape[0] // seqs

    def piece(idx, owner, way):
        if idx == 5:
            return gains_all.at[owner, pl.ds(2 * way, 2)]
        rows = sources[idx].shape[0]
        return gathered[idx].at[pl.ds(pl.multiple_of(owner * rows + way * (rows // 2), rows // 2), rows // 2), :]

    def source(idx, way):
        if idx == 5:
            return mix.at[pl.ds(2 * way, 2)]
        half = sources[idx].shape[0] // 2
        return sources[idx].at[pl.ds(way * half, half), :]

    def owner_at(way, step):
        return owner_of(place, way, step)

    def send(idx, way, step):
        dst = piece(idx, owner_at(way, step), way)
        return pltpu.make_async_remote_copy(
            src_ref=source(idx, way) if step == 0 else dst, dst_ref=dst, send_sem=send_sem.at[idx, way, step],
            recv_sem=recv_sem.at[idx, way, step], device_id={'fsdp': targets[way]}, device_id_type=MESH)

    def landed(idx, way, step):
        dst = piece(idx, owner_at(way, step + 1), way)
        return pltpu.make_async_remote_copy(
            src_ref=dst, dst_ref=dst, send_sem=send_sem.at[idx, way, step], recv_sem=recv_sem.at[idx, way, step],
            device_id={'fsdp': targets[way]}, device_id_type=MESH)

    def own(idx, way):
        return pltpu.make_async_copy(source(idx, way), piece(idx, me, way), local_sem.at[idx, way])

    def start_ring(ids):
        for idx in ids:
            for way in WAYS:
                send(idx, way, 0).start()

    def forward(ids, step):
        for idx in ids:
            for way in WAYS:
                landed(idx, way, step - 1).wait_recv()
                send(idx, way, step).start()

    def to_member(src, dst, send_one, recv_one, hop):
        return pltpu.make_async_remote_copy(
            src_ref=src, dst_ref=dst, send_sem=send_one, recv_sem=recv_one,
            device_id={'model': (me_model + hop) % 4}, device_id_type=MESH)

    block_src, block_dst = (dh_part, y_part, dh_attn), (dh_blocks, y_blocks, attn_blocks)

    def block_of(idx, who):
        return block_src[idx].at[:, pl.ds(pl.multiple_of(who * block_rows, block_rows), block_rows), :]

    def block_copy(idx, hop, incoming):
        slot = block_dst[idx].at[member(me_model, hop, incoming)]
        src = slot if incoming else block_of(idx, (me_model + hop) % 4)
        return to_member(src, slot, block_send.at[idx, hop], block_recv.at[idx, hop], hop)

    def block_own(idx):
        return pltpu.make_async_copy(block_of(idx, me_model), block_dst[idx].at[me_model], block_local.at[idx])

    def blocks_start(idx):
        for hop in MATES:
            block_copy(idx, hop, False).start()
        block_own(idx).start()

    def blocks_wait(idx):
        block_own(idx).wait()
        for hop in MATES:
            block_copy(idx, hop, True).wait_recv()
            block_copy(idx, hop, False).wait_send()

    def mid_slot(who):
        return d_full.at[:, pl.ds(pl.multiple_of(who * block_rows, block_rows), block_rows), :]

    def mid_copy(hop, incoming):
        slot = mid_slot(member(me_model, hop, incoming))
        return to_member(slot if incoming else d_mid, slot, mid_send.at[hop], mid_recv.at[hop], hop)

    def mid_own():
        return pltpu.make_async_copy(d_mid, mid_slot(me_model), mid_local)

    def columns(peer):
        return d_mid.at[:, :, pl.ds(pl.multiple_of(peer * slice_width, slice_width), slice_width)]

    def slice_copy(hop, incoming):
        peer = (me + hop) % 8
        slot = mid_cols.at[(me + 8 - hop) % 8 if incoming else me]
        return pltpu.make_async_remote_copy(
            src_ref=slot if incoming else columns(peer), dst_ref=slot, send_sem=slice_send.at[hop],
            recv_sem=slice_recv.at[hop], device_id={'fsdp': peer}, device_id_type=MESH)

    def slice_own():
        return pltpu.make_async_copy(columns(me), mid_cols.at[me], slice_local)

    cols_in, cols_all = (h_cols, mid_cols), (h_spread, mid_spread)

    def cols_copy(idx, hop, incoming):
        slot = cols_all[idx].at[:, :, member(me_model, hop, incoming)]
        return to_member(slot if incoming else cols_in[idx], slot, cols_send.at[idx, hop], cols_recv.at[idx, hop], hop)

    def cols_own(idx):
        return pltpu.make_async_copy(cols_in[idx], cols_all[idx].at[:, :, me_model], cols_local.at[idx])

    def finish_ring(ids):
        for idx in ids:
            for way in WAYS:
                landed(idx, way, 6).wait_recv()
                own(idx, way).wait()

    def cols_wait(idx):
        cols_own(idx).wait()
        for hop in MATES:
            cols_copy(idx, hop, True).wait_recv()
            cols_copy(idx, hop, False).wait_send()

    def mix_copy(hop, incoming):
        slot = mix.at[member(me_model, hop, incoming)]
        return to_member(slot if incoming else gains, slot, mix_send.at[hop], mix_recv.at[hop], hop)

    def mix_own():
        return pltpu.make_async_copy(gains, mix.at[me_model], mix_local)

    def fetch(idx):
        return pltpu.make_async_copy((w_out_in, w_qkv_in)[idx], (w_out, w_qkv)[idx], fetch_sem.at[idx])

    def norm_back(parts, saved, gain, base, result, first_row):
        row_sum[...] = jnp.zeros_like(row_sum)

        @functools.partial(tiles, block_rows, GROUP)
        def _(at):
            for seq in range(seqs):
                d_h = sum_blocks(parts, seq, at)
                val = saved[seq, at, :].astype(f32)
                inv_rms = lax.rsqrt(jnp.mean(val * val, axis=-1, keepdims=True) + NORM_EPS)
                scaled = d_h * gain[...]
                slope = jnp.sum(scaled * val, axis=-1, keepdims=True) * (inv_rms * inv_rms * inv_rms) * (1.0 / d_model)
                result[seq, at, :] = (base[seq, at, :].astype(f32) + (scaled * inv_rms - val * slope)).astype(bf16)
                per_row = d_h * val * inv_rms
                row_sum[...] += per_row[:8] + per_row[8:]
        total = jnp.sum(row_sum[...], axis=0, keepdims=True)
        width = gains.shape[1]
        for row in range(d_model // width):
            gains[first_row + row:first_row + row + 1, :] = total[:, row * width:(row + 1) * width]

    def attention_back():
        cos_two, sin_two = wide_tables(cos_ref, sin_ref)
        d_attn[...] = across(d_full[...].reshape(seqs * seq_len, d_model), w_out[...]).astype(bf16)
        for seq in range(seqs):
            for head in range(heads):
                idx = seq * heads + head
                rows = slice(seq * seq_len, (seq + 1) * seq_len)
                d_out = d_attn[rows, head * head_dim:(head + 1) * head_dim]
                weight = prob[idx]
                d_prob = across(d_out, value[idx])
                row_dot = jnp.sum(d_prob * weight, axis=-1, keepdims=True)
                d_scores = (weight * (d_prob - row_dot) * head_dim ** -0.5).astype(bf16)
                d_query = jnp.dot(d_scores, key[idx], preferred_element_type=f32)
                d_key = along(d_scores, query[idx])
                d_value = along(weight.astype(bf16), d_out)
                for place_in, part in enumerate((d_query, d_key)):
                    turned = part * cos_two + pltpu.roll(part, head_dim // 2, 1) * sin_two
                    start = (3 * head + place_in) * head_dim
                    d_qkv[rows, start:start + head_dim] = turned.astype(bf16)
                d_qkv[rows, (3 * head + 2) * head_dim:(3 * head + 3) * head_dim] = d_value.astype(bf16)

        @functools.partial(tiles, d_model, TILE)
        def _(cols):
            dh_attn[:, :, cols] = across(d_qkv[...], w_qkv[cols, :]).reshape(seqs, seq_len, TILE)

    bigs, smalls, products = (act_all, attn_all, gate_all, up_all), (dy_spread, mid_spread, h_spread), (dw_down, dw_out, dw_gate, dw_up)

    def span(tile):
        return pl.ds(tile * TILE, TILE)

    def small_copy(which):
        return pltpu.make_async_copy(smalls[which], small.at[which], small_sem.at[which])

    def big_copy(kind, tile, slot):
        return pltpu.make_async_copy(bigs[kind].at[:, span(tile)], big.at[slot], big_sem.at[slot])

    def product_copy(kind, tile, slot):
        if kind < 2:
            return pltpu.make_async_copy(tall.at[slot], products[kind].at[span(tile), :], product_sem.at[slot])
        return pltpu.make_async_copy(flat.at[slot], products[kind].at[:, span(tile)], product_sem.at[slot])

    def begin(jobs, done=()):
        for slot, job in enumerate(done):
            product_copy(*job, slot).wait()
        for slot, job in enumerate(jobs):
            big_copy(*job, slot).start()

    def multiply(jobs):
        for slot, (kind, tile) in enumerate(jobs):
            big_copy(kind, tile, slot).wait()
            side = small[min(kind, 2)].reshape(big.shape[1], slice_width)
            if kind < 2:
                tall[slot] = along(big[slot], side)
            else:
                flat[slot] = along(side, big[slot])
            product_copy(kind, tile, slot).start()

    early = {3: ((0, 0), (0, 1)), 5: ((0, 2), (0, 3)), 6: ((1, 0),)}
    late = {2: ((2, 0), (2, 1)), 3: ((2, 2), (2, 3)), 4: ((3, 0), (3, 1)), 5: ((3, 2), (3, 3))}
    small_copy(0).start()
    start_ring((0, 1))
    blocks_start(0)
    blocks_start(1)
    for idx in range(4):
        for way in WAYS:
            own(idx, way).start()
    for idx in WAYS:
        fetch(idx).start()
    for hop in MATES:
        cols_copy(0, hop, False).start()
    cols_own(0).start()
    for step in LATER:
        forward((0, 1), step)
        if step == 2:
            blocks_wait(0)
            norm_back(dh_blocks, mid_ref, gain_mlp, dy_ref, d_mid, 8)
        if step == 3:
            for hop in MATES:
                mid_copy(hop, False).start()
            mid_own().start()
            slice_own().start()
            for hop in OTHERS:
                slice_copy(hop, False).start()
        if step == 5:
            blocks_wait(1)

            @functools.partial(tiles, block_rows, GROUP)
            def _(at):
                for seq in range(seqs):
                    y_ref[seq, at, :] = (mid_ref[seq, at, :].astype(f32) + sum_blocks(y_blocks, seq, at)).astype(bf16)
    start_ring((2, 3))
    past = ()
    for step in LATER:
        if step == 3:
            small_copy(0).wait()
            finish_ring((0, 1))
        if step == 5:
            cols_wait(0)
            small_copy(2).start()
        if step == 6:
            cols_wait(1)
            small_copy(1).start()
        if step in early:
            begin(early[step], past)
            past = early[step]
        forward((2, 3), step)
        if step == 6:
            small_copy(1).wait()
        if step in early:
            multiply(early[step])
        if step == 1:
            mid_own().wait()
            for hop in MATES:
                mid_copy(hop, True).wait_recv()
                mid_copy(hop, False).wait_send()
            for idx in WAYS:
                fetch(idx).wait()
            attention_back()
        if step == 2:
            blocks_start(2)
            slice_own().wait()
            for hop in OTHERS:
                slice_copy(hop, True).wait_recv()
                slice_copy(hop, False).wait_send()
            for hop in MATES:
                cols_copy(1, hop, False).start()
            cols_own(1).start()
        if step == 4:
            blocks_wait(2)
            norm_back(attn_blocks, x_ref, gain_attn, d_mid, dx_ref, 0)
        if step == 5:
            mix_own().start()
            for hop in MATES:
                mix_copy(hop, False).start()
    start_ring((4,))
    mix_own().wait()
    for hop in MATES:
        mix_copy(hop, True).wait_recv()
        mix_copy(hop, False).wait_send()
    start_ring((5,))
    for idx in (4, 5):
        for way in WAYS:
            own(idx, way).start()
    for step in LATER:
        if step == 2:
            small_copy(2).wait()
            finish_ring((2, 3))
        if step in late:
            begin(late[step], past)
            past = late[step]
        forward((4, 5), step)
        if step in late:
            multiply(late[step])
    begin((), past)
    finish_ring((4, 5))
    for idx in range(6):
        for way in WAYS:
            for step in STEPS:
                send(idx, way, step).wait_send()


def ring_back(collective_id, *args):
    act, attn, d_gate, d_up, dh_part, y_part, h_cols, w_out, w_qkv, mid = args[:10]
    tokens = act.shape[0]
    seqs, seq_len, d_model = dh_part.shape
    bf16, f32 = jnp.bfloat16, jnp.float32
    qkv_cols = w_qkv.shape[1]
    sent = 7 * (3 * act.size + attn.size + tokens * qkv_cols) * 2
    vmem = pl.BlockSpec(memory_space=pltpu.VMEM)
    hbm = pl.BlockSpec(memory_space=pl.ANY)
    shape = jax.ShapeDtypeStruct
    gain_shape = (16, d_model // 8)
    side = d_model // 8
    spread = shape(h_cols.shape[:2] + (4,) + h_cols.shape[2:], bf16)
    blocks = pltpu.VMEM((4,) + mid.shape, f32)
    return pl.pallas_call(
        back_kernel,
        out_shape=[shape((act.shape[1], side), f32), shape((attn.shape[1], side), f32), shape((side, act.shape[1]), f32),
                   shape((side, act.shape[1]), f32)]
        + [shape((8 * tokens, array.shape[1]), bf16) for array in (act, attn, d_gate, d_up)]
        + [shape((8 * tokens, qkv_cols), bf16), shape((8, 4) + gain_shape, f32), shape((4,) + gain_shape, f32),
           shape(h_cols.shape, bf16), spread, spread, shape(mid.shape, bf16), shape(mid.shape, bf16)],
        in_specs=[hbm] * 9 + [vmem] * (len(args) - 10) + [hbm],
        out_specs=[hbm] * 14 + [vmem] * 2,
        scratch_shapes=[pltpu.VMEM(w_out.shape, bf16), pltpu.VMEM(w_qkv.shape, bf16), pltpu.VMEM(mid.shape, bf16),
                        pltpu.VMEM(dh_part.shape, bf16), pltpu.VMEM((tokens, w_out.shape[0]), bf16),
                        pltpu.VMEM((tokens, qkv_cols), bf16), pltpu.VMEM(dh_part.shape, f32), pltpu.VMEM(gain_shape, f32),
                        pltpu.VMEM((8, d_model), f32), blocks, blocks, blocks,
                        DMA((6, 2, 7)), DMA((6, 2, 7)), DMA((6, 2)), TRIO_MATES, TRIO_MATES, TRIO,
                        MATE_SEMS, MATE_SEMS, DMA, OTHER_SEMS, OTHER_SEMS, DMA, PAIR_MATES, PAIR_MATES, PAIR,
                        MATE_SEMS, MATE_SEMS, DMA, PAIR,
                        pltpu.VMEM((3,) + spread.shape, bf16), pltpu.VMEM((2, 8 * tokens, TILE), bf16),
                        pltpu.VMEM((2, TILE, side), f32), pltpu.VMEM((2, side, TILE), f32), TRIO, PAIR, PAIR],
        compiler_params=pltpu.CompilerParams(collective_id=collective_id, has_side_effects=True,
                                             vmem_limit_bytes=60 * 1024 * 1024),
        cost_estimate=pl.CostEstimate(flops=sent * 3000, bytes_accessed=2 * sent, transcendentals=0),
        name=f'ring_back_{collective_id}',
    )(*args)


def solution(mesh):
    act_spec = P('fsdp', 'model', None)
    rows_spec = P('fsdp', 'model')
    cols_spec = P('model', 'fsdp')
    f32 = jnp.float32

    def device_fn(x_loc, dy_loc, gain_attn, gain_mlp, wqkv_sh, wout_sh, wgate_sh, wup_sh, wdown_sh, rope_cos, rope_sin):
        tokens = x_loc.shape[0] * rope_cos.shape[0]
        gain_a, gain_m = gain_attn.reshape(1, -1), gain_mlp.reshape(1, -1)
        (w_qkv, w_out, _, _, h_mlp_cols, h_attn_cols, dy_cols, query, key_rot, value, prob, attn_flat, gated_act, d_gate, d_up,
         mlp_part, dh_part, mid) = ring_front(
            1, wqkv_sh, wout_sh, wdown_sh, wgate_sh, wup_sh, x_loc, dy_loc, gain_a, gain_m, rope_cos, rope_sin)
        whole = (x_loc.shape[0], rope_cos.shape[0], x_loc.shape[2])
        (dw_down, dw_out, dw_gate, dw_up, _, _, _, _, d_qkv_all, gains_all, _, _, _, _, y_loc, dx_loc) = ring_back(
            2, gated_act, attn_flat, d_gate, d_up, dh_part.reshape(whole), mlp_part.reshape(whole), h_mlp_cols, w_out, w_qkv,
            mid, x_loc, dy_loc, gain_m, gain_a, query, key_rot, value, prob, rope_cos, rope_sin, dy_cols)
        gain_grads = jnp.sum(gains_all, axis=(0, 1)).reshape(2, -1)
        dw_qkv = along(h_attn_cols.reshape(8 * tokens, -1), d_qkv_all)
        return (y_loc, dx_loc, gain_grads[0], gain_grads[1], dw_qkv, dw_out, dw_gate, dw_up, dw_down)

    in_specs = (act_spec, act_spec, P(), P(), rows_spec, cols_spec, rows_spec, rows_spec, cols_spec, P(), P())
    out_specs = (act_spec, act_spec, P(), P(), rows_spec, cols_spec, rows_spec, rows_spec, cols_spec)
    return jax.shard_map(device_fn, mesh=mesh, in_specs=in_specs, out_specs=out_specs, check_vma=False)
```

```python
import functools

import jax
import jax.numpy as jnp
from jax import lax
from jax.experimental import pallas as pl
from jax.experimental.pallas import tpu as pltpu
from jax.sharding import PartitionSpec as P

NORM_EPS = 1e-5
MESH = pl.DeviceIdType.MESH
WAYS, STEPS, LATER = range(2), range(7), range(1, 7)
MATES, OTHERS = range(1, 4), range(1, 8)
DMA = pltpu.SemaphoreType.DMA
MATE_SEMS, OTHER_SEMS, PAIR, TRIO = DMA((4,)), DMA((8,)), DMA((2,)), DMA((3,))
PAIR_MATES, TRIO_MATES, TRIO_OTHERS = DMA((2, 4)), DMA((3, 4)), DMA((3, 8))


def ring_place(index):
    z, y = index // 2, index % 2
    return z + y * (7 - 2 * z)


def ring_device(place):
    y = place // 4
    return 2 * (place + y * (7 - 2 * place)) + y


def neighbours(place):
    return ring_device((place + 1) % 8), ring_device((place + 7) % 8)


def owner_of(place, way, step):
    return ring_device((place + (8 - step if way == 0 else step)) % 8)


def enter(me, me_model):
    barrier = pltpu.get_barrier_semaphore()
    for hop in OTHERS:
        pl.semaphore_signal(barrier, inc=1, device_id={'fsdp': (me + hop) % 8}, device_id_type=MESH)
    for hop in MATES:
        pl.semaphore_signal(barrier, inc=1, device_id={'model': (me_model + hop) % 4}, device_id_type=MESH)
    pl.semaphore_wait(barrier, 10)


def member(me_model, hop, incoming):
    return (me_model + 4 - hop) % 4 if incoming else me_model


def across(left, right):
    return lax.dot_general(left, right, (((1,), (1,)), ((), ())), preferred_element_type=jnp.float32)


def along(left, right):
    return lax.dot_general(left, right, (((0,), (0,)), ((), ())), preferred_element_type=jnp.float32)


def tiles(width, tile_width, body):
    @pl.loop(0, width // tile_width)
    def _(tile):
        body(pl.ds(pl.multiple_of(tile * tile_width, tile_width), tile_width))


def wide_tables(cos_ref, sin_ref):
    cos_t, sin_t = cos_ref[...], sin_ref[...]
    return jnp.concatenate([cos_t, cos_t], axis=0).T, jnp.concatenate([sin_t, -sin_t], axis=0).T


def sum_blocks(parts, seq, at):
    total = (parts[0, seq, at, :] + parts[1, seq, at, :]) + (parts[2, seq, at, :] + parts[3, seq, at, :])
    return total.astype(jnp.bfloat16).astype(jnp.float32)


TILE, GROUP = 512, 16


def front_kernel(qkv_sh, out_sh, down_sh, gate_sh, up_sh, x_ref, dy_in, gain_attn, gain_mlp, cos_ref, sin_ref,
                 w_qkv_all, w_out_all, attn_cols, dy_cols, h_cols, attn_spread, dy_spread,
                 query, key, value, prob, attn_flat, act_ref, d_gate_ref, d_up_ref, y_part_ref, dh_part_ref, mid_ref,
                 w_qkv, w_out, w_down, w_gate, w_up, qkv, attn_part, gate_acc, up_acc, d_act, ha_full, dy_full, h_full,
                 ha_loc, h_loc, blocks,
                 send_sem, recv_sem, local_sem, block_send, block_recv, block_local, seq_send, seq_recv, seq_local,
                 slice_send, slice_recv, slice_local, cols_send, cols_recv, cols_local, fetch_sem):
    f32, bf16 = jnp.float32, jnp.bfloat16
    me = lax.axis_index('fsdp')
    me_model = lax.axis_index('model')
    place = ring_place(me)
    targets = neighbours(place)
    enter(me, me_model)
    shards, weights = (qkv_sh, out_sh, down_sh, gate_sh, up_sh), (w_qkv_all, w_out_all, w_down, w_gate, w_up)
    accs = {3: gate_acc, 4: up_acc}
    rows, width = gate_sh.shape
    half = rows // 2
    seqs, block_rows, d_model = x_ref.shape
    seq_len = 4 * block_rows
    tokens = seqs * seq_len
    slice_width = h_cols.shape[3]
    head_dim = query.shape[2]
    heads = query.shape[0] // seqs

    def start_of(owner, way):
        return pl.multiple_of(owner * rows + way * half, half)

    def piece(idx, owner, way):
        if idx in (1, 2):
            tall = shards[idx].shape[0] // 2
            return weights[idx].at[pl.ds(way * tall, tall), pl.ds(pl.multiple_of(owner * rows, rows), rows)]
        return weights[idx].at[pl.ds(start_of(owner, way), half), :]

    def source(idx, way):
        size = shards[idx].shape[0] // 2
        return shards[idx].at[pl.ds(way * size, size), :]

    def owner_at(way, step):
        return owner_of(place, way, step)

    def send(idx, way, step):
        dst = piece(idx, owner_at(way, step), way)
        return pltpu.make_async_remote_copy(
            src_ref=source(idx, way) if isinstance(step, int) and step == 0 else dst, dst_ref=dst,
            send_sem=send_sem.at[idx, way, step], recv_sem=recv_sem.at[idx, way, step],
            device_id={'fsdp': targets[way]}, device_id_type=MESH)

    def landed(idx, way, step):
        dst = piece(idx, owner_at(way, step + 1), way)
        return pltpu.make_async_remote_copy(
            src_ref=dst, dst_ref=dst, send_sem=send_sem.at[idx, way, step], recv_sem=recv_sem.at[idx, way, step],
            device_id={'fsdp': targets[way]}, device_id_type=MESH)

    def own(idx, way):
        return pltpu.make_async_copy(source(idx, way), piece(idx, me, way), local_sem.at[idx, way])

    def start_ring(ids):
        for idx in ids:
            for way in WAYS:
                send(idx, way, 0).start()

    def forward(ids, step):
        for idx in ids:
            for way in WAYS:
                landed(idx, way, step - 1).wait_recv()
                send(idx, way, step).start()

    def finish_ring(ids):
        for idx in ids:
            for way in WAYS:
                landed(idx, way, 6).wait_recv()
                own(idx, way).wait()

    def to_member(src, dst, send_one, recv_one, hop):
        return pltpu.make_async_remote_copy(
            src_ref=src, dst_ref=dst, send_sem=send_one, recv_sem=recv_one,
            device_id={'model': (me_model + hop) % 4}, device_id_type=MESH)

    def rows_of(ref, who):
        return ref.at[:, pl.ds(pl.multiple_of(who * block_rows, block_rows), block_rows), :]

    def block_copy(hop, incoming):
        slot = blocks.at[member(me_model, hop, incoming)]
        src = slot if incoming else rows_of(attn_part, (me_model + hop) % 4)
        return to_member(src, slot, block_send.at[hop], block_recv.at[hop], hop)

    def block_own():
        return pltpu.make_async_copy(rows_of(attn_part, me_model), blocks.at[me_model], block_local)

    seq_src, seq_dst = (ha_loc, dy_in, h_loc), (ha_full, dy_full, h_full)
    slice_dst, spread_dst = (attn_cols, dy_cols, h_cols), (attn_spread, dy_spread)

    def seq_copy(idx, hop, incoming):
        slot = rows_of(seq_dst[idx], member(me_model, hop, incoming))
        return to_member(slot if incoming else seq_src[idx], slot, seq_send.at[idx, hop], seq_recv.at[idx, hop], hop)

    def seq_own(idx):
        return pltpu.make_async_copy(seq_src[idx], rows_of(seq_dst[idx], me_model), seq_local.at[idx])

    def columns(idx, peer):
        return seq_src[idx].at[:, :, pl.ds(pl.multiple_of(peer * slice_width, slice_width), slice_width)]

    def slice_copy(idx, hop, incoming):
        peer = (me + hop) % 8
        slot = slice_dst[idx].at[(me + 8 - hop) % 8 if incoming else me]
        return pltpu.make_async_remote_copy(
            src_ref=slot if incoming else columns(idx, peer), dst_ref=slot, send_sem=slice_send.at[idx, hop],
            recv_sem=slice_recv.at[idx, hop], device_id={'fsdp': peer}, device_id_type=MESH)

    def slice_own(idx):
        return pltpu.make_async_copy(columns(idx, me), slice_dst[idx].at[me], slice_local.at[idx])

    def hand_out(idx):
        for hop in MATES:
            seq_copy(idx, hop, False).start()
        seq_own(idx).start()
        slice_own(idx).start()
        for hop in OTHERS:
            slice_copy(idx, hop, False).start()

    def seq_wait(idx):
        seq_own(idx).wait()
        for hop in MATES:
            seq_copy(idx, hop, True).wait_recv()
            seq_copy(idx, hop, False).wait_send()

    def slice_wait(idx):
        slice_own(idx).wait()
        for hop in OTHERS:
            slice_copy(idx, hop, True).wait_recv()
            slice_copy(idx, hop, False).wait_send()

    def cols_copy(idx, hop, incoming):
        slot = spread_dst[idx].at[:, :, member(me_model, hop, incoming)]
        return to_member(slot if incoming else slice_dst[idx], slot, cols_send.at[idx, hop], cols_recv.at[idx, hop], hop)

    def cols_own(idx):
        return pltpu.make_async_copy(slice_dst[idx], spread_dst[idx].at[:, :, me_model], cols_local.at[idx])

    def fetch(idx):
        return pltpu.make_async_copy(weights[idx], (w_qkv, w_out)[idx], fetch_sem.at[idx])

    def normed(val, gain):
        return (val * lax.rsqrt(jnp.mean(val * val, axis=-1, keepdims=True) + NORM_EPS) * gain[...]).astype(bf16)

    def attention():
        cos_two, sin_two = wide_tables(cos_ref, sin_ref)
        @functools.partial(tiles, qkv.shape[1], TILE)
        def _(cols):
            qkv[:, cols] = jnp.dot(ha_full[...].reshape(tokens, d_model), w_qkv[:, cols], preferred_element_type=f32)
        causal = (lax.broadcasted_iota(jnp.int32, (seq_len, seq_len), 0)
                  >= lax.broadcasted_iota(jnp.int32, (seq_len, seq_len), 1))
        for seq in range(seqs):
            for head in range(heads):
                idx = seq * heads + head
                at = slice(seq * seq_len, (seq + 1) * seq_len)
                start = 3 * head * head_dim
                for place_in, turned_ref in enumerate((query, key)):
                    part = qkv[at, start + place_in * head_dim:start + (place_in + 1) * head_dim]
                    turned = part * cos_two - pltpu.roll(part, head_dim // 2, 1) * sin_two
                    turned_ref[idx] = turned.astype(bf16)
                value[idx] = qkv[at, start + 2 * head_dim:start + 3 * head_dim].astype(bf16)
                scores = jnp.where(causal, across(query[idx], key[idx]) * head_dim ** -0.5, -1e30)
                unnormed = jnp.exp(scores - jnp.max(scores, axis=-1, keepdims=True))
                weight = unnormed / jnp.sum(unnormed, axis=-1, keepdims=True)
                prob[idx] = weight
                mixed = jnp.dot(weight.astype(bf16), value[idx], preferred_element_type=f32)
                attn_flat[at, head * head_dim:(head + 1) * head_dim] = mixed.astype(bf16)

        @functools.partial(tiles, d_model, TILE)
        def _(cols):
            attn_part[:, :, cols] = jnp.dot(attn_flat[...], w_out[:, cols],
                                            preferred_element_type=f32).reshape(seqs, seq_len, TILE)

    def accumulate(step):
        for way in WAYS:
            start = start_of(owner_at(way, step), way)
            h_block = h_full[:, :, pl.ds(start, half)].reshape(tokens, half)
            for idx in (3, 4):
                @functools.partial(tiles, width, TILE)
                def _(cols):
                    accs[idx][:, cols] += jnp.dot(h_block, weights[idx][pl.ds(start, half), cols],
                                                  preferred_element_type=f32)

    start_ring((0, 1))
    for idx in range(5):
        for way in WAYS:
            own(idx, way).start()
    hand_out(1)

    @functools.partial(tiles, block_rows, GROUP)
    def _(at):
        for seq in range(seqs):
            ha_loc[seq, at, :] = normed(x_ref[seq, at, :].astype(f32), gain_attn)
    gate_acc[...] = jnp.zeros_like(gate_acc)
    up_acc[...] = jnp.zeros_like(up_acc)
    for step in LATER:
        forward((0, 1), step)
        if step == 1:
            hand_out(0)
    start_ring((2,))
    finish_ring((0, 1))
    for idx in WAYS:
        fetch(idx).start()
    for step in LATER:
        forward((2,), step)
        if step == 1:
            seq_wait(0)
            for idx in WAYS:
                fetch(idx).wait()
            attention()
        if step == 2:
            for hop in MATES:
                block_copy(hop, False).start()
            block_own().start()
        if step == 4:
            block_own().wait()
            for hop in MATES:
                block_copy(hop, True).wait_recv()
                block_copy(hop, False).wait_send()

            @functools.partial(tiles, block_rows, GROUP)
            def _(at):
                for seq in range(seqs):
                    mid = (x_ref[seq, at, :].astype(f32) + sum_blocks(blocks, seq, at)).astype(bf16)
                    mid_ref[seq, at, :] = mid
                    h_loc[seq, at, :] = normed(mid.astype(f32), gain_mlp)
        if step == 5:
            hand_out(2)
    start_ring((3, 4))
    seq_wait(1)
    for idx in WAYS:
        slice_wait(idx)
        for hop in MATES:
            cols_copy(idx, hop, False).start()
        cols_own(idx).start()
    finish_ring((2,))

    @functools.partial(tiles, width, TILE)
    def _(cols):
        d_act[:, cols] = across(dy_full[...].reshape(tokens, d_model), w_down[cols, :]).astype(bf16)

    seq_wait(2)
    for idx in (3, 4):
        for way in WAYS:
            own(idx, way).wait()
    accumulate(0)

    @pl.loop(1, 7)
    def _(step):
        forward((3, 4), step)
        accumulate(step)

    for idx in (3, 4):
        for way in WAYS:
            landed(idx, way, 6).wait_recv()
    accumulate(7)

    @functools.partial(tiles, width, 256)
    def _(cols):
        gate, up_proj = gate_acc[:, cols], up_acc[:, cols]
        d_val = d_act[:, cols].astype(f32)
        sig_gate = jax.nn.sigmoid(gate)
        silu_gate = gate * sig_gate
        act_ref[:, cols] = (silu_gate * up_proj).astype(bf16)
        d_gate_ref[:, cols] = (d_val * up_proj * sig_gate * (1.0 + gate * (1.0 - sig_gate))).astype(bf16)
        d_up_ref[:, cols] = (d_val * silu_gate).astype(bf16)

    @functools.partial(tiles, width, TILE)
    def _(cols):
        dh_part_ref[:, cols] = across(d_gate_ref[...], w_gate[cols, :]) + across(d_up_ref[...], w_up[cols, :])
        y_part_ref[:, cols] = jnp.dot(act_ref[...], w_down[:, cols], preferred_element_type=f32)

    for idx in range(5):
        for way in WAYS:
            for step in STEPS:
                send(idx, way, step).wait_send()
    slice_wait(2)
    for idx in WAYS:
        cols_own(idx).wait()
        for hop in MATES:
            cols_copy(idx, hop, True).wait_recv()
            cols_copy(idx, hop, False).wait_send()


def ring_front(collective_id, *args):
    qkv_sh, out_sh, down_sh, gate_sh, up_sh, x_loc, dy_loc = args[:7]
    seqs, block_rows, d_model = x_loc.shape
    seq_len, head_dim = args[9].shape[1], 2 * args[9].shape[0]
    tokens = seqs * seq_len
    width, qkv_cols, attn_cols = gate_sh.shape[1], qkv_sh.shape[1], out_sh.shape[0]
    sent = 7 * (qkv_sh.size + out_sh.size + 3 * gate_sh.size) * 2
    vmem = pl.BlockSpec(memory_space=pltpu.VMEM)
    hbm = pl.BlockSpec(memory_space=pl.ANY)
    bf16, f32 = jnp.bfloat16, jnp.float32
    shape, buf = jax.ShapeDtypeStruct, pltpu.VMEM
    sliced = shape((8, seqs, block_rows, d_model // 8), bf16)
    spread = shape((8, seqs, 4, block_rows, d_model // 8), bf16)
    per_head = shape((seqs * attn_cols // head_dim, seq_len, head_dim), bf16)
    hidden = shape((tokens, width), bf16)
    partial_sum = shape((tokens, d_model), f32)
    whole = (seqs, seq_len, d_model)
    return pl.pallas_call(
        front_kernel,
        out_shape=[shape((d_model, qkv_cols), bf16), shape((attn_cols, d_model), bf16), sliced, sliced, sliced, spread, spread,
                   per_head, per_head, per_head, shape((per_head.shape[0], seq_len, seq_len), f32),
                   shape((tokens, attn_cols), bf16), hidden, hidden, hidden, partial_sum, partial_sum, shape(x_loc.shape, bf16)],
        in_specs=[hbm] * 5 + [vmem] * 6,
        out_specs=[hbm] * 7 + [vmem] * 11,
        scratch_shapes=[buf((d_model, qkv_cols), bf16), buf((attn_cols, d_model), bf16), buf((width, d_model), bf16),
                        buf((d_model, width), bf16), buf((d_model, width), bf16), buf((tokens, qkv_cols), f32), buf(whole, f32),
                        buf((tokens, width), f32), buf((tokens, width), f32), buf((tokens, width), bf16),
                        buf(whole, bf16), buf(whole, bf16), buf(whole, bf16), buf(x_loc.shape, bf16), buf(x_loc.shape, bf16),
                        buf((4,) + x_loc.shape, f32),
                        DMA((5, 2, 7)), DMA((5, 2, 7)), DMA((5, 2)), MATE_SEMS, MATE_SEMS, DMA, TRIO_MATES, TRIO_MATES, TRIO,
                        TRIO_OTHERS, TRIO_OTHERS, TRIO, PAIR_MATES, PAIR_MATES, PAIR, PAIR],
        compiler_params=pltpu.CompilerParams(collective_id=collective_id, has_side_effects=True,
                                             vmem_limit_bytes=63 * 1024 * 1024),
        cost_estimate=pl.CostEstimate(flops=sent * 3000, bytes_accessed=2 * sent, transcendentals=0),
        name=f'ring_front_{collective_id}',
    )(*args)


def back_kernel(act, attn, d_gate, d_up, dh_part, y_part, h_cols, w_out_in, w_qkv_in, mid_ref, x_ref, dy_ref, gain_mlp, gain_attn,
                query, key, value, prob, cos_ref, sin_ref, dy_spread, attn_spread,
                dw_qkv, dw_down, dw_out, dw_gate, dw_up, act_all, attn_all, gate_all, up_all, gains_all, mix, mid_cols, mid_spread, h_spread, y_ref, dx_ref,
                w_out, w_qkv, d_mid, d_full, d_attn, d_qkv, dh_attn, gains, row_sum, dh_blocks, y_blocks, attn_blocks,
                send_sem, recv_sem, local_sem, block_send, block_recv, block_local, mid_send, mid_recv, mid_local,
                slice_send, slice_recv, slice_local, cols_send, cols_recv, cols_local, mix_send, mix_recv, mix_local, fetch_sem,
                small, big, tall, flat, qkv_all, qkv_acc, small_sem, big_sem, product_sem):
    f32, bf16 = jnp.float32, jnp.bfloat16
    me = lax.axis_index('fsdp')
    me_model = lax.axis_index('model')
    place = ring_place(me)
    targets = neighbours(place)
    enter(me, me_model)
    sources = (act, attn, d_gate, d_up, d_qkv)
    gathered = (act_all, attn_all, gate_all, up_all, qkv_all)
    seqs, block_rows, d_model = x_ref.shape
    seq_len = 4 * block_rows
    slice_width = mid_cols.shape[3]
    head_dim = query.shape[2]
    heads = query.shape[0] // seqs

    def piece(idx, owner, way):
        if idx == 5:
            return gains_all.at[owner, pl.ds(2 * way, 2)]
        rows = sources[idx].shape[0]
        return gathered[idx].at[pl.ds(pl.multiple_of(owner * rows + way * (rows // 2), rows // 2), rows // 2), :]

    def source(idx, way):
        if idx == 5:
            return mix.at[pl.ds(2 * way, 2)]
        half = sources[idx].shape[0] // 2
        return sources[idx].at[pl.ds(way * half, half), :]

    def owner_at(way, step):
        return owner_of(place, way, step)

    def send(idx, way, step):
        dst = piece(idx, owner_at(way, step), way)
        return pltpu.make_async_remote_copy(
            src_ref=source(idx, way) if step == 0 else dst, dst_ref=dst, send_sem=send_sem.at[idx, way, step],
            recv_sem=recv_sem.at[idx, way, step], device_id={'fsdp': targets[way]}, device_id_type=MESH)

    def landed(idx, way, step):
        dst = piece(idx, owner_at(way, step + 1), way)
        return pltpu.make_async_remote_copy(
            src_ref=dst, dst_ref=dst, send_sem=send_sem.at[idx, way, step], recv_sem=recv_sem.at[idx, way, step],
            device_id={'fsdp': targets[way]}, device_id_type=MESH)

    def own(idx, way):
        return pltpu.make_async_copy(source(idx, way), piece(idx, me, way), local_sem.at[idx, way])

    def start_ring(ids):
        for idx in ids:
            for way in WAYS:
                send(idx, way, 0).start()

    def forward(ids, step):
        for idx in ids:
            for way in WAYS:
                landed(idx, way, step - 1).wait_recv()
                send(idx, way, step).start()

    def to_member(src, dst, send_one, recv_one, hop):
        return pltpu.make_async_remote_copy(
            src_ref=src, dst_ref=dst, send_sem=send_one, recv_sem=recv_one,
            device_id={'model': (me_model + hop) % 4}, device_id_type=MESH)

    block_src, block_dst = (dh_part, y_part, dh_attn), (dh_blocks, y_blocks, attn_blocks)

    def block_of(idx, who):
        return block_src[idx].at[:, pl.ds(pl.multiple_of(who * block_rows, block_rows), block_rows), :]

    def block_copy(idx, hop, incoming):
        slot = block_dst[idx].at[member(me_model, hop, incoming)]
        src = slot if incoming else block_of(idx, (me_model + hop) % 4)
        return to_member(src, slot, block_send.at[idx, hop], block_recv.at[idx, hop], hop)

    def block_own(idx):
        return pltpu.make_async_copy(block_of(idx, me_model), block_dst[idx].at[me_model], block_local.at[idx])

    def blocks_start(idx):
        for hop in MATES:
            block_copy(idx, hop, False).start()
        block_own(idx).start()

    def blocks_wait(idx):
        block_own(idx).wait()
        for hop in MATES:
            block_copy(idx, hop, True).wait_recv()
            block_copy(idx, hop, False).wait_send()

    def mid_slot(who):
        return d_full.at[:, pl.ds(pl.multiple_of(who * block_rows, block_rows), block_rows), :]

    def mid_copy(hop, incoming):
        slot = mid_slot(member(me_model, hop, incoming))
        return to_member(slot if incoming else d_mid, slot, mid_send.at[hop], mid_recv.at[hop], hop)

    def mid_own():
        return pltpu.make_async_copy(d_mid, mid_slot(me_model), mid_local)

    def columns(peer):
        return d_mid.at[:, :, pl.ds(pl.multiple_of(peer * slice_width, slice_width), slice_width)]

    def slice_copy(hop, incoming):
        peer = (me + hop) % 8
        slot = mid_cols.at[(me + 8 - hop) % 8 if incoming else me]
        return pltpu.make_async_remote_copy(
            src_ref=slot if incoming else columns(peer), dst_ref=slot, send_sem=slice_send.at[hop],
            recv_sem=slice_recv.at[hop], device_id={'fsdp': peer}, device_id_type=MESH)

    def slice_own():
        return pltpu.make_async_copy(columns(me), mid_cols.at[me], slice_local)

    cols_in, cols_all = (h_cols, mid_cols), (h_spread, mid_spread)

    def cols_copy(idx, hop, incoming):
        slot = cols_all[idx].at[:, :, member(me_model, hop, incoming)]
        return to_member(slot if incoming else cols_in[idx], slot, cols_send.at[idx, hop], cols_recv.at[idx, hop], hop)

    def cols_own(idx):
        return pltpu.make_async_copy(cols_in[idx], cols_all[idx].at[:, :, me_model], cols_local.at[idx])

    def finish_ring(ids):
        for idx in ids:
            for way in WAYS:
                landed(idx, way, 6).wait_recv()
                own(idx, way).wait()

    def cols_wait(idx):
        cols_own(idx).wait()
        for hop in MATES:
            cols_copy(idx, hop, True).wait_recv()
            cols_copy(idx, hop, False).wait_send()

    def mix_copy(hop, incoming):
        slot = mix.at[member(me_model, hop, incoming)]
        return to_member(slot if incoming else gains, slot, mix_send.at[hop], mix_recv.at[hop], hop)

    def mix_own():
        return pltpu.make_async_copy(gains, mix.at[me_model], mix_local)

    def fetch(idx):
        return pltpu.make_async_copy((w_out_in, w_qkv_in)[idx], (w_out, w_qkv)[idx], fetch_sem.at[idx])

    def norm_back(parts, saved, gain, base, result, first_row):
        row_sum[...] = jnp.zeros_like(row_sum)

        @functools.partial(tiles, block_rows, GROUP)
        def _(at):
            for seq in range(seqs):
                d_h = sum_blocks(parts, seq, at)
                val = saved[seq, at, :].astype(f32)
                inv_rms = lax.rsqrt(jnp.mean(val * val, axis=-1, keepdims=True) + NORM_EPS)
                scaled = d_h * gain[...]
                slope = jnp.sum(scaled * val, axis=-1, keepdims=True) * (inv_rms * inv_rms * inv_rms) * (1.0 / d_model)
                result[seq, at, :] = (base[seq, at, :].astype(f32) + (scaled * inv_rms - val * slope)).astype(bf16)
                per_row = d_h * val * inv_rms
                row_sum[...] += per_row[:8] + per_row[8:]
        total = jnp.sum(row_sum[...], axis=0, keepdims=True)
        width = gains.shape[1]
        for row in range(d_model // width):
            gains[first_row + row:first_row + row + 1, :] = total[:, row * width:(row + 1) * width]

    def attention_back():
        cos_two, sin_two = wide_tables(cos_ref, sin_ref)
        d_attn[...] = across(d_full[...].reshape(seqs * seq_len, d_model), w_out[...]).astype(bf16)
        for seq in range(seqs):
            for head in range(heads):
                idx = seq * heads + head
                rows = slice(seq * seq_len, (seq + 1) * seq_len)
                d_out = d_attn[rows, head * head_dim:(head + 1) * head_dim]
                weight = prob[idx]
                d_prob = across(d_out, value[idx])
                row_dot = jnp.sum(d_prob * weight, axis=-1, keepdims=True)
                d_scores = (weight * (d_prob - row_dot) * head_dim ** -0.5).astype(bf16)
                d_query = jnp.dot(d_scores, key[idx], preferred_element_type=f32)
                d_key = along(d_scores, query[idx])
                d_value = along(weight.astype(bf16), d_out)
                for place_in, part in enumerate((d_query, d_key)):
                    turned = part * cos_two + pltpu.roll(part, head_dim // 2, 1) * sin_two
                    start = (3 * head + place_in) * head_dim
                    d_qkv[rows, start:start + head_dim] = turned.astype(bf16)
                d_qkv[rows, (3 * head + 2) * head_dim:(3 * head + 3) * head_dim] = d_value.astype(bf16)

        @functools.partial(tiles, d_model, TILE)
        def _(cols):
            dh_attn[:, :, cols] = across(d_qkv[...], w_qkv[cols, :]).reshape(seqs, seq_len, TILE)

    bigs, smalls, products = (act_all, attn_all, gate_all, up_all), (dy_spread, mid_spread, h_spread, attn_spread), (dw_down, dw_out, dw_gate, dw_up)

    def span(tile):
        return pl.ds(tile * TILE, TILE)

    def small_copy(which):
        return pltpu.make_async_copy(smalls[which], small.at[which], small_sem.at[which])

    def big_copy(kind, tile, slot):
        return pltpu.make_async_copy(bigs[kind].at[:, span(tile)], big.at[slot], big_sem.at[slot])

    def product_copy(kind, tile, slot):
        if kind < 2:
            return pltpu.make_async_copy(tall.at[slot], products[kind].at[span(tile), :], product_sem.at[slot])
        return pltpu.make_async_copy(flat.at[slot], products[kind].at[:, span(tile)], product_sem.at[slot])

    def begin(jobs, done=()):
        for slot, job in enumerate(done):
            product_copy(*job, slot).wait()
        for slot, job in enumerate(jobs):
            big_copy(*job, slot).start()

    def multiply(jobs):
        for slot, (kind, tile) in enumerate(jobs):
            big_copy(kind, tile, slot).wait()
            side = small[min(kind, 2)].reshape(big.shape[1], slice_width)
            if kind < 2:
                tall[slot] = along(big[slot], side)
            else:
                flat[slot] = along(side, big[slot])
            product_copy(kind, tile, slot).start()

    def accumulate(step):
        for way in WAYS:
            owner = owner_at(way, step)
            side = small[3, owner, way].reshape(seq_len, slice_width)

            @functools.partial(tiles, qkv_acc.shape[1], TILE)
            def _(cols):
                if step == 0:
                    block = d_qkv[way * seq_len:(way + 1) * seq_len, cols]
                else:
                    block = qkv_all[pl.ds(pl.multiple_of((2 * owner + way) * seq_len, seq_len), seq_len), cols]
                qkv_acc[:, cols] += along(side, block)

    early = {3: ((0, 0), (0, 1)), 5: ((0, 2), (0, 3)), 6: ((1, 0),)}
    late = {2: ((2, 0), (2, 1)), 3: ((2, 2), (2, 3)), 4: ((3, 0), (3, 1)), 5: ((3, 2), (3, 3))}
    small_copy(0).start()
    small_copy(3).start()
    qkv_acc[...] = jnp.zeros_like(qkv_acc)
    start_ring((0, 1))
    blocks_start(0)
    blocks_start(1)
    for idx in range(4):
        for way in WAYS:
            own(idx, way).start()
    for idx in WAYS:
        fetch(idx).start()
    for hop in MATES:
        cols_copy(0, hop, False).start()
    cols_own(0).start()
    for step in LATER:
        forward((0, 1), step)
        if step == 2:
            blocks_wait(0)
            norm_back(dh_blocks, mid_ref, gain_mlp, dy_ref, d_mid, 8)
        if step == 3:
            for hop in MATES:
                mid_copy(hop, False).start()
            mid_own().start()
            slice_own().start()
            for hop in OTHERS:
                slice_copy(hop, False).start()
        if step == 5:
            blocks_wait(1)

            @functools.partial(tiles, block_rows, GROUP)
            def _(at):
                for seq in range(seqs):
                    y_ref[seq, at, :] = (mid_ref[seq, at, :].astype(f32) + sum_blocks(y_blocks, seq, at)).astype(bf16)
    start_ring((2, 3))
    past = ()
    for step in LATER:
        if step == 3:
            small_copy(0).wait()
            finish_ring((0, 1))
        if step == 5:
            cols_wait(0)
            small_copy(2).start()
        if step == 6:
            cols_wait(1)
            small_copy(1).start()
        if step in early:
            begin(early[step], past)
            past = early[step]
        forward((2, 3), step)
        if step == 6:
            small_copy(1).wait()
        if step in early:
            multiply(early[step])
        if step == 1:
            mid_own().wait()
            for hop in MATES:
                mid_copy(hop, True).wait_recv()
                mid_copy(hop, False).wait_send()
            for idx in WAYS:
                fetch(idx).wait()
            attention_back()
        if step == 2:
            blocks_start(2)
            slice_own().wait()
            for hop in OTHERS:
                slice_copy(hop, True).wait_recv()
                slice_copy(hop, False).wait_send()
            for hop in MATES:
                cols_copy(1, hop, False).start()
            cols_own(1).start()
        if step == 4:
            blocks_wait(2)
            norm_back(attn_blocks, x_ref, gain_attn, d_mid, dx_ref, 0)
        if step == 5:
            mix_own().start()
            for hop in MATES:
                mix_copy(hop, False).start()
    start_ring((4,))
    mix_own().wait()
    for hop in MATES:
        mix_copy(hop, True).wait_recv()
        mix_copy(hop, False).wait_send()
    start_ring((5,))
    for idx in (4, 5):
        for way in WAYS:
            own(idx, way).start()
    small_copy(3).wait()
    accumulate(0)
    for step in LATER:
        if step == 2:
            small_copy(2).wait()
            finish_ring((2, 3))
        if step in late:
            begin(late[step], past)
            past = late[step]
        forward((4, 5), step)
        if step in late:
            multiply(late[step])
        accumulate(step)
    begin((), past)
    finish_ring((4, 5))
    accumulate(7)
    result = pltpu.make_async_copy(qkv_acc, dw_qkv, fetch_sem.at[0])
    result.start()
    for idx in range(6):
        for way in WAYS:
            for step in STEPS:
                send(idx, way, step).wait_send()
    result.wait()


def ring_back(collective_id, *args):
    act, attn, d_gate, d_up, dh_part, y_part, h_cols, w_out, w_qkv, mid = args[:10]
    tokens = act.shape[0]
    seqs, seq_len, d_model = dh_part.shape
    bf16, f32 = jnp.bfloat16, jnp.float32
    qkv_cols = w_qkv.shape[1]
    sent = 7 * (3 * act.size + attn.size + tokens * qkv_cols) * 2
    vmem = pl.BlockSpec(memory_space=pltpu.VMEM)
    hbm = pl.BlockSpec(memory_space=pl.ANY)
    shape = jax.ShapeDtypeStruct
    gain_shape = (16, d_model // 8)
    side = d_model // 8
    spread = shape(h_cols.shape[:2] + (4,) + h_cols.shape[2:], bf16)
    blocks = pltpu.VMEM((4,) + mid.shape, f32)
    return pl.pallas_call(
        back_kernel,
        out_shape=[shape((side, qkv_cols), f32), shape((act.shape[1], side), f32), shape((attn.shape[1], side), f32), shape((side, act.shape[1]), f32),
                   shape((side, act.shape[1]), f32)]
        + [shape((8 * tokens, array.shape[1]), bf16) for array in (act, attn, d_gate, d_up)]
        + [shape((8, 4) + gain_shape, f32), shape((4,) + gain_shape, f32),
           shape(h_cols.shape, bf16), spread, spread, shape(mid.shape, bf16), shape(mid.shape, bf16)],
        in_specs=[hbm] * 9 + [vmem] * (len(args) - 11) + [hbm] * 2,
        out_specs=[hbm] * 14 + [vmem] * 2,
        scratch_shapes=[pltpu.VMEM(w_out.shape, bf16), pltpu.VMEM(w_qkv.shape, bf16), pltpu.VMEM(mid.shape, bf16),
                        pltpu.VMEM(dh_part.shape, bf16), pltpu.VMEM((tokens, w_out.shape[0]), bf16),
                        pltpu.VMEM((tokens, qkv_cols), bf16), pltpu.VMEM(dh_part.shape, f32), pltpu.VMEM(gain_shape, f32),
                        pltpu.VMEM((8, d_model), f32), blocks, blocks, blocks,
                        DMA((6, 2, 7)), DMA((6, 2, 7)), DMA((6, 2)), TRIO_MATES, TRIO_MATES, TRIO,
                        MATE_SEMS, MATE_SEMS, DMA, OTHER_SEMS, OTHER_SEMS, DMA, PAIR_MATES, PAIR_MATES, PAIR,
                        MATE_SEMS, MATE_SEMS, DMA, PAIR,
                        pltpu.VMEM((4,) + spread.shape, bf16), pltpu.VMEM((2, 8 * tokens, TILE), bf16),
                        pltpu.VMEM((2, TILE, side), f32), pltpu.VMEM((2, side, TILE), f32), pltpu.VMEM((8 * tokens, qkv_cols), bf16),
                        pltpu.VMEM((side, qkv_cols), f32), MATE_SEMS, PAIR, PAIR],
        compiler_params=pltpu.CompilerParams(collective_id=collective_id, has_side_effects=True,
                                             vmem_limit_bytes=60 * 1024 * 1024),
        cost_estimate=pl.CostEstimate(flops=sent * 3000, bytes_accessed=2 * sent, transcendentals=0),
        name=f'ring_back_{collective_id}',
    )(*args)


def solution(mesh):
    act_spec = P('fsdp', 'model', None)
    rows_spec = P('fsdp', 'model')
    cols_spec = P('model', 'fsdp')
    f32 = jnp.float32

    def device_fn(x_loc, dy_loc, gain_attn, gain_mlp, wqkv_sh, wout_sh, wgate_sh, wup_sh, wdown_sh, rope_cos, rope_sin):
        gain_a, gain_m = gain_attn.reshape(1, -1), gain_mlp.reshape(1, -1)
        rope_cos_t, rope_sin_t = rope_cos.T, rope_sin.T
        (w_qkv, w_out, _, _, h_mlp_cols, h_attn_cols, dy_cols, query, key_rot, value, prob, attn_flat, gated_act, d_gate, d_up,
         mlp_part, dh_part, mid) = ring_front(
            1, wqkv_sh, wout_sh, wdown_sh, wgate_sh, wup_sh, x_loc, dy_loc, gain_a, gain_m, rope_cos_t, rope_sin_t)
        whole = (x_loc.shape[0], rope_cos.shape[0], x_loc.shape[2])
        (dw_qkv, dw_down, dw_out, dw_gate, dw_up, _, _, _, _, gains_all, _, _, _, _, y_loc, dx_loc) = ring_back(
            2, gated_act, attn_flat, d_gate, d_up, dh_part.reshape(whole), mlp_part.reshape(whole), h_mlp_cols, w_out, w_qkv,
            mid, x_loc, dy_loc, gain_m, gain_a, query, key_rot, value, prob, rope_cos_t, rope_sin_t, dy_cols, h_attn_cols)
        gain_grads = jnp.sum(gains_all, axis=(0, 1)).reshape(2, -1)
        return (y_loc, dx_loc, gain_grads[0], gain_grads[1], dw_qkv, dw_out, dw_gate, dw_up, dw_down)

    in_specs = (act_spec, act_spec, P(), P(), rows_spec, cols_spec, rows_spec, rows_spec, cols_spec, P(), P())
    out_specs = (act_spec, act_spec, P(), P(), rows_spec, cols_spec, rows_spec, rows_spec, cols_spec)
    return jax.shard_map(device_fn, mesh=mesh, in_specs=in_specs, out_specs=out_specs, check_vma=False)
```

```python
import functools

import jax
import jax.numpy as jnp
from jax import lax
from jax.experimental import pallas as pl
from jax.experimental.pallas import tpu as pltpu
from jax.sharding import PartitionSpec as P

NORM_EPS = 1e-5
MESH = pl.DeviceIdType.MESH
WAYS, STEPS, LATER = range(2), range(7), range(1, 7)
MATES, OTHERS = range(1, 4), range(1, 8)
DMA = pltpu.SemaphoreType.DMA
MATE_SEMS, OTHER_SEMS, PAIR, TRIO = DMA((4,)), DMA((8,)), DMA((2,)), DMA((3,))
PAIR_MATES, TRIO_MATES, TRIO_OTHERS = DMA((2, 4)), DMA((3, 4)), DMA((3, 8))


def ring_place(index):
    z, y = index // 2, index % 2
    return z + y * (7 - 2 * z)


def ring_device(place):
    y = place // 4
    return 2 * (place + y * (7 - 2 * place)) + y


def neighbours(place):
    return ring_device((place + 1) % 8), ring_device((place + 7) % 8)


def owner_of(place, way, step):
    return ring_device((place + (8 - step if way == 0 else step)) % 8)


def enter(me, me_model):
    barrier = pltpu.get_barrier_semaphore()
    for hop in OTHERS:
        pl.semaphore_signal(barrier, inc=1, device_id={'fsdp': (me + hop) % 8}, device_id_type=MESH)
    for hop in MATES:
        pl.semaphore_signal(barrier, inc=1, device_id={'model': (me_model + hop) % 4}, device_id_type=MESH)
    pl.semaphore_wait(barrier, 10)


def member(me_model, hop, incoming):
    return (me_model + 4 - hop) % 4 if incoming else me_model


def across(left, right):
    return lax.dot_general(left, right, (((1,), (1,)), ((), ())), preferred_element_type=jnp.float32)


def along(left, right):
    return lax.dot_general(left, right, (((0,), (0,)), ((), ())), preferred_element_type=jnp.float32)


def tiles(width, tile_width, body):
    @pl.loop(0, width // tile_width)
    def _(tile):
        body(pl.ds(pl.multiple_of(tile * tile_width, tile_width), tile_width))


def wide_tables(cos_ref, sin_ref):
    cos_t, sin_t = cos_ref[...], sin_ref[...]
    return jnp.concatenate([cos_t, cos_t], axis=0).T, jnp.concatenate([sin_t, -sin_t], axis=0).T


def sum_blocks(parts, seq, at):
    total = (parts[0, seq, at, :] + parts[1, seq, at, :]) + (parts[2, seq, at, :] + parts[3, seq, at, :])
    return total.astype(jnp.bfloat16).astype(jnp.float32)


TILE, GROUP = 512, 16


def front_kernel(qkv_sh, out_sh, down_sh, gate_sh, up_sh, x_ref, dy_in, gain_attn, gain_mlp, cos_ref, sin_ref,
                 w_qkv_all, w_out_all, attn_cols, dy_cols, h_cols, attn_spread, dy_spread,
                 query, key, value, prob, attn_flat, act_ref, d_gate_ref, d_up_ref, y_part_ref, dh_part_ref, mid_ref,
                 w_qkv, w_out, w_down, w_gate, w_up, qkv, attn_part, gate_acc, up_acc, d_act, ha_full, dy_full, h_full,
                 ha_loc, h_loc, blocks,
                 send_sem, recv_sem, local_sem, block_send, block_recv, block_local, seq_send, seq_recv, seq_local,
                 slice_send, slice_recv, slice_local, cols_send, cols_recv, cols_local, fetch_sem):
    f32, bf16 = jnp.float32, jnp.bfloat16
    me = lax.axis_index('fsdp')
    me_model = lax.axis_index('model')
    place = ring_place(me)
    targets = neighbours(place)
    enter(me, me_model)
    shards, weights = (qkv_sh, out_sh, down_sh, gate_sh, up_sh), (w_qkv_all, w_out_all, w_down, w_gate, w_up)
    accs = {3: gate_acc, 4: up_acc}
    rows, width = gate_sh.shape
    half = rows // 2
    seqs, block_rows, d_model = x_ref.shape
    seq_len = 4 * block_rows
    tokens = seqs * seq_len
    slice_width = h_cols.shape[3]
    head_dim = query.shape[2]
    heads = query.shape[0] // seqs

    def start_of(owner, way):
        return pl.multiple_of(owner * rows + way * half, half)

    def piece(idx, owner, way):
        if idx in (1, 2):
            tall = shards[idx].shape[0] // 2
            return weights[idx].at[pl.ds(way * tall, tall), pl.ds(pl.multiple_of(owner * rows, rows), rows)]
        return weights[idx].at[pl.ds(start_of(owner, way), half), :]

    def source(idx, way):
        size = shards[idx].shape[0] // 2
        return shards[idx].at[pl.ds(way * size, size), :]

    def owner_at(way, step):
        return owner_of(place, way, step)

    def send(idx, way, step):
        dst = piece(idx, owner_at(way, step), way)
        return pltpu.make_async_remote_copy(
            src_ref=source(idx, way) if isinstance(step, int) and step == 0 else dst, dst_ref=dst,
            send_sem=send_sem.at[idx, way, step], recv_sem=recv_sem.at[idx, way, step],
            device_id={'fsdp': targets[way]}, device_id_type=MESH)

    def landed(idx, way, step):
        dst = piece(idx, owner_at(way, step + 1), way)
        return pltpu.make_async_remote_copy(
            src_ref=dst, dst_ref=dst, send_sem=send_sem.at[idx, way, step], recv_sem=recv_sem.at[idx, way, step],
            device_id={'fsdp': targets[way]}, device_id_type=MESH)

    def own(idx, way):
        return pltpu.make_async_copy(source(idx, way), piece(idx, me, way), local_sem.at[idx, way])

    def start_ring(ids):
        for idx in ids:
            for way in WAYS:
                send(idx, way, 0).start()

    def forward(ids, step):
        for idx in ids:
            for way in WAYS:
                landed(idx, way, step - 1).wait_recv()
                send(idx, way, step).start()

    def finish_ring(ids):
        for idx in ids:
            for way in WAYS:
                landed(idx, way, 6).wait_recv()
                own(idx, way).wait()

    def to_member(src, dst, send_one, recv_one, hop):
        return pltpu.make_async_remote_copy(
            src_ref=src, dst_ref=dst, send_sem=send_one, recv_sem=recv_one,
            device_id={'model': (me_model + hop) % 4}, device_id_type=MESH)

    def rows_of(ref, who):
        return ref.at[:, pl.ds(pl.multiple_of(who * block_rows, block_rows), block_rows), :]

    def block_copy(hop, incoming):
        slot = blocks.at[member(me_model, hop, incoming)]
        src = slot if incoming else rows_of(attn_part, (me_model + hop) % 4)
        return to_member(src, slot, block_send.at[hop], block_recv.at[hop], hop)

    def block_own():
        return pltpu.make_async_copy(rows_of(attn_part, me_model), blocks.at[me_model], block_local)

    seq_src, seq_dst = (ha_loc, dy_in, h_loc), (ha_full, dy_full, h_full)
    slice_dst, spread_dst = (attn_cols, dy_cols, h_cols), (attn_spread, dy_spread)

    def seq_copy(idx, hop, incoming):
        slot = rows_of(seq_dst[idx], member(me_model, hop, incoming))
        return to_member(slot if incoming else seq_src[idx], slot, seq_send.at[idx, hop], seq_recv.at[idx, hop], hop)

    def seq_own(idx):
        return pltpu.make_async_copy(seq_src[idx], rows_of(seq_dst[idx], me_model), seq_local.at[idx])

    def columns(idx, peer):
        return seq_src[idx].at[:, :, pl.ds(pl.multiple_of(peer * slice_width, slice_width), slice_width)]

    def slice_copy(idx, hop, incoming):
        peer = (me + hop) % 8
        slot = slice_dst[idx].at[(me + 8 - hop) % 8 if incoming else me]
        return pltpu.make_async_remote_copy(
            src_ref=slot if incoming else columns(idx, peer), dst_ref=slot, send_sem=slice_send.at[idx, hop],
            recv_sem=slice_recv.at[idx, hop], device_id={'fsdp': peer}, device_id_type=MESH)

    def slice_own(idx):
        return pltpu.make_async_copy(columns(idx, me), slice_dst[idx].at[me], slice_local.at[idx])

    def hand_out(idx):
        for hop in MATES:
            seq_copy(idx, hop, False).start()
        seq_own(idx).start()
        slice_own(idx).start()
        for hop in OTHERS:
            slice_copy(idx, hop, False).start()

    def seq_wait(idx):
        seq_own(idx).wait()
        for hop in MATES:
            seq_copy(idx, hop, True).wait_recv()
            seq_copy(idx, hop, False).wait_send()

    def slice_wait(idx):
        slice_own(idx).wait()
        for hop in OTHERS:
            slice_copy(idx, hop, True).wait_recv()
            slice_copy(idx, hop, False).wait_send()

    def cols_copy(idx, hop, incoming):
        slot = spread_dst[idx].at[:, :, member(me_model, hop, incoming)]
        return to_member(slot if incoming else slice_dst[idx], slot, cols_send.at[idx, hop], cols_recv.at[idx, hop], hop)

    def cols_own(idx):
        return pltpu.make_async_copy(slice_dst[idx], spread_dst[idx].at[:, :, me_model], cols_local.at[idx])

    def fetch(idx):
        return pltpu.make_async_copy(weights[idx], (w_qkv, w_out)[idx], fetch_sem.at[idx])

    def normed(val, gain):
        return (val * lax.rsqrt(jnp.mean(val * val, axis=-1, keepdims=True) + NORM_EPS) * gain[...]).astype(bf16)

    def attention():
        cos_two, sin_two = wide_tables(cos_ref, sin_ref)
        @functools.partial(tiles, qkv.shape[1], TILE)
        def _(cols):
            qkv[:, cols] = jnp.dot(ha_full[...].reshape(tokens, d_model), w_qkv[:, cols], preferred_element_type=f32)
        causal = (lax.broadcasted_iota(jnp.int32, (seq_len, seq_len), 0)
                  >= lax.broadcasted_iota(jnp.int32, (seq_len, seq_len), 1))
        for seq in range(seqs):
            for head in range(heads):
                idx = seq * heads + head
                at = slice(seq * seq_len, (seq + 1) * seq_len)
                start = 3 * head * head_dim
                for place_in, turned_ref in enumerate((query, key)):
                    part = qkv[at, start + place_in * head_dim:start + (place_in + 1) * head_dim]
                    turned = part * cos_two - pltpu.roll(part, head_dim // 2, 1) * sin_two
                    turned_ref[idx] = turned.astype(bf16)
                value[idx] = qkv[at, start + 2 * head_dim:start + 3 * head_dim].astype(bf16)
                scores = jnp.where(causal, across(query[idx], key[idx]) * head_dim ** -0.5, -1e30)
                unnormed = jnp.exp(scores - jnp.max(scores, axis=-1, keepdims=True))
                weight = unnormed / jnp.sum(unnormed, axis=-1, keepdims=True)
                prob[idx] = weight
                mixed = jnp.dot(weight.astype(bf16), value[idx], preferred_element_type=f32)
                attn_flat[at, head * head_dim:(head + 1) * head_dim] = mixed.astype(bf16)

        @functools.partial(tiles, d_model, TILE)
        def _(cols):
            attn_part[:, :, cols] = jnp.dot(attn_flat[...], w_out[:, cols],
                                            preferred_element_type=f32).reshape(seqs, seq_len, TILE)

    def accumulate(step):
        for way in WAYS:
            start = start_of(owner_at(way, step), way)
            h_block = h_full[:, :, pl.ds(start, half)].reshape(tokens, half)
            for idx in (3, 4):
                @functools.partial(tiles, width, TILE)
                def _(cols):
                    accs[idx][:, cols] += jnp.dot(h_block, weights[idx][pl.ds(start, half), cols],
                                                  preferred_element_type=f32)

    start_ring((0, 1))
    for idx in range(5):
        for way in WAYS:
            own(idx, way).start()
    hand_out(1)

    @functools.partial(tiles, block_rows, GROUP)
    def _(at):
        for seq in range(seqs):
            ha_loc[seq, at, :] = normed(x_ref[seq, at, :].astype(f32), gain_attn)
    gate_acc[...] = jnp.zeros_like(gate_acc)
    up_acc[...] = jnp.zeros_like(up_acc)
    for step in LATER:
        forward((0, 1), step)
        if step == 1:
            hand_out(0)
    start_ring((2,))
    finish_ring((0, 1))
    for idx in WAYS:
        fetch(idx).start()
    for step in LATER:
        forward((2,), step)
        if step == 1:
            seq_wait(0)
            for idx in WAYS:
                fetch(idx).wait()
            attention()
        if step == 2:
            for hop in MATES:
                block_copy(hop, False).start()
            block_own().start()
        if step == 4:
            block_own().wait()
            for hop in MATES:
                block_copy(hop, True).wait_recv()
                block_copy(hop, False).wait_send()

            @functools.partial(tiles, block_rows, GROUP)
            def _(at):
                for seq in range(seqs):
                    mid = (x_ref[seq, at, :].astype(f32) + sum_blocks(blocks, seq, at)).astype(bf16)
                    mid_ref[seq, at, :] = mid
                    h_loc[seq, at, :] = normed(mid.astype(f32), gain_mlp)
        if step == 5:
            hand_out(2)
    start_ring((3, 4))
    seq_wait(1)
    for idx in WAYS:
        slice_wait(idx)
        for hop in MATES:
            cols_copy(idx, hop, False).start()
        cols_own(idx).start()
    finish_ring((2,))

    @functools.partial(tiles, width, TILE)
    def _(cols):
        d_act[:, cols] = across(dy_full[...].reshape(tokens, d_model), w_down[cols, :]).astype(bf16)

    seq_wait(2)
    for idx in (3, 4):
        for way in WAYS:
            own(idx, way).wait()
    accumulate(0)

    @pl.loop(1, 7)
    def _(step):
        forward((3, 4), step)
        accumulate(step)

    for idx in (3, 4):
        for way in WAYS:
            landed(idx, way, 6).wait_recv()
    accumulate(7)

    @functools.partial(tiles, width, 256)
    def _(cols):
        gate, up_proj = gate_acc[:, cols], up_acc[:, cols]
        d_val = d_act[:, cols].astype(f32)
        sig_gate = jax.nn.sigmoid(gate)
        silu_gate = gate * sig_gate
        act_ref[:, cols] = (silu_gate * up_proj).astype(bf16)
        d_gate_ref[:, cols] = (d_val * up_proj * sig_gate * (1.0 + gate * (1.0 - sig_gate))).astype(bf16)
        d_up_ref[:, cols] = (d_val * silu_gate).astype(bf16)

    @functools.partial(tiles, width, TILE)
    def _(cols):
        dh_part_ref[:, cols] = across(d_gate_ref[...], w_gate[cols, :]) + across(d_up_ref[...], w_up[cols, :])
        y_part_ref[:, cols] = jnp.dot(act_ref[...], w_down[:, cols], preferred_element_type=f32)

    for idx in range(5):
        for way in WAYS:
            for step in STEPS:
                send(idx, way, step).wait_send()
    slice_wait(2)
    for idx in WAYS:
        cols_own(idx).wait()
        for hop in MATES:
            cols_copy(idx, hop, True).wait_recv()
            cols_copy(idx, hop, False).wait_send()


def ring_front(collective_id, *args):
    qkv_sh, out_sh, down_sh, gate_sh, up_sh, x_loc, dy_loc = args[:7]
    seqs, block_rows, d_model = x_loc.shape
    seq_len, head_dim = args[9].shape[1], 2 * args[9].shape[0]
    tokens = seqs * seq_len
    width, qkv_cols, attn_cols = gate_sh.shape[1], qkv_sh.shape[1], out_sh.shape[0]
    sent = 7 * (qkv_sh.size + out_sh.size + 3 * gate_sh.size) * 2
    vmem = pl.BlockSpec(memory_space=pltpu.VMEM)
    hbm = pl.BlockSpec(memory_space=pl.ANY)
    bf16, f32 = jnp.bfloat16, jnp.float32
    shape, buf = jax.ShapeDtypeStruct, pltpu.VMEM
    sliced = shape((8, seqs, block_rows, d_model // 8), bf16)
    spread = shape((8, seqs, 4, block_rows, d_model // 8), bf16)
    per_head = shape((seqs * attn_cols // head_dim, seq_len, head_dim), bf16)
    hidden = shape((tokens, width), bf16)
    partial_sum = shape((tokens, d_model), f32)
    whole = (seqs, seq_len, d_model)
    return pl.pallas_call(
        front_kernel,
        out_shape=[shape((d_model, qkv_cols), bf16), shape((attn_cols, d_model), bf16), sliced, sliced, sliced, spread, spread,
                   per_head, per_head, per_head, shape((per_head.shape[0], seq_len, seq_len), f32),
                   shape((tokens, attn_cols), bf16), hidden, hidden, hidden, partial_sum, partial_sum, shape(x_loc.shape, bf16)],
        in_specs=[hbm] * 5 + [vmem] * 6,
        out_specs=[hbm] * 7 + [vmem] * 11,
        scratch_shapes=[buf((d_model, qkv_cols), bf16), buf((attn_cols, d_model), bf16), buf((width, d_model), bf16),
                        buf((d_model, width), bf16), buf((d_model, width), bf16), buf((tokens, qkv_cols), f32), buf(whole, f32),
                        buf((tokens, width), f32), buf((tokens, width), f32), buf((tokens, width), bf16),
                        buf(whole, bf16), buf(whole, bf16), buf(whole, bf16), buf(x_loc.shape, bf16), buf(x_loc.shape, bf16),
                        buf((4,) + x_loc.shape, f32),
                        DMA((5, 2, 7)), DMA((5, 2, 7)), DMA((5, 2)), MATE_SEMS, MATE_SEMS, DMA, TRIO_MATES, TRIO_MATES, TRIO,
                        TRIO_OTHERS, TRIO_OTHERS, TRIO, PAIR_MATES, PAIR_MATES, PAIR, PAIR],
        compiler_params=pltpu.CompilerParams(collective_id=collective_id, has_side_effects=True,
                                             vmem_limit_bytes=63 * 1024 * 1024),
        cost_estimate=pl.CostEstimate(flops=sent * 3000, bytes_accessed=2 * sent, transcendentals=0),
        name=f'ring_front_{collective_id}',
    )(*args)


def back_kernel(act, attn, d_gate, d_up, dh_part, y_part, h_cols, w_out_in, w_qkv_in, mid_ref, x_ref, dy_ref, gain_mlp, gain_attn,
                query, key, value, prob, cos_ref, sin_ref, dy_spread, attn_spread,
                dw_qkv, dw_down, dw_out, dw_gate, dw_up, act_all, attn_all, gate_all, up_all, gains_all, mix, mid_cols, mid_spread, h_spread, y_ref, dx_ref,
                w_out, w_qkv, d_mid, d_full, d_attn, d_qkv, dh_attn, gains, row_sum, dh_blocks, y_blocks, attn_blocks,
                send_sem, recv_sem, local_sem, block_send, block_recv, block_local, mid_send, mid_recv, mid_local,
                slice_send, slice_recv, slice_local, cols_send, cols_recv, cols_local, mix_send, mix_recv, mix_local, fetch_sem,
                small, big, tall, flat, qkv_all, qkv_acc, small_sem, big_sem, product_sem):
    f32, bf16 = jnp.float32, jnp.bfloat16
    me = lax.axis_index('fsdp')
    me_model = lax.axis_index('model')
    place = ring_place(me)
    targets = neighbours(place)
    enter(me, me_model)
    sources = (act, attn, d_gate, d_up, d_qkv)
    gathered = (act_all, attn_all, gate_all, up_all, qkv_all)
    seqs, block_rows, d_model = x_ref.shape
    seq_len = 4 * block_rows
    slice_width = mid_cols.shape[3]
    head_dim = query.shape[2]
    heads = query.shape[0] // seqs

    def piece(idx, owner, way):
        if idx == 5:
            return gains_all.at[owner, pl.ds(2 * way, 2)]
        rows = sources[idx].shape[0]
        return gathered[idx].at[pl.ds(pl.multiple_of(owner * rows + way * (rows // 2), rows // 2), rows // 2), :]

    def source(idx, way):
        if idx == 5:
            return mix.at[pl.ds(2 * way, 2)]
        half = sources[idx].shape[0] // 2
        return sources[idx].at[pl.ds(way * half, half), :]

    def owner_at(way, step):
        return owner_of(place, way, step)

    def send(idx, way, step):
        dst = piece(idx, owner_at(way, step), way)
        return pltpu.make_async_remote_copy(
            src_ref=source(idx, way) if step == 0 else dst, dst_ref=dst, send_sem=send_sem.at[idx, way, step],
            recv_sem=recv_sem.at[idx, way, step], device_id={'fsdp': targets[way]}, device_id_type=MESH)

    def landed(idx, way, step):
        dst = piece(idx, owner_at(way, step + 1), way)
        return pltpu.make_async_remote_copy(
            src_ref=dst, dst_ref=dst, send_sem=send_sem.at[idx, way, step], recv_sem=recv_sem.at[idx, way, step],
            device_id={'fsdp': targets[way]}, device_id_type=MESH)

    def own(idx, way):
        return pltpu.make_async_copy(source(idx, way), piece(idx, me, way), local_sem.at[idx, way])

    def start_ring(ids):
        for idx in ids:
            for way in WAYS:
                send(idx, way, 0).start()

    def forward(ids, step):
        for idx in ids:
            for way in WAYS:
                landed(idx, way, step - 1).wait_recv()
                send(idx, way, step).start()

    def to_member(src, dst, send_one, recv_one, hop):
        return pltpu.make_async_remote_copy(
            src_ref=src, dst_ref=dst, send_sem=send_one, recv_sem=recv_one,
            device_id={'model': (me_model + hop) % 4}, device_id_type=MESH)

    block_src, block_dst = (dh_part, y_part, dh_attn), (dh_blocks, y_blocks, attn_blocks)

    def block_of(idx, who):
        return block_src[idx].at[:, pl.ds(pl.multiple_of(who * block_rows, block_rows), block_rows), :]

    def block_copy(idx, hop, incoming):
        slot = block_dst[idx].at[member(me_model, hop, incoming)]
        src = slot if incoming else block_of(idx, (me_model + hop) % 4)
        return to_member(src, slot, block_send.at[idx, hop], block_recv.at[idx, hop], hop)

    def block_own(idx):
        return pltpu.make_async_copy(block_of(idx, me_model), block_dst[idx].at[me_model], block_local.at[idx])

    def blocks_start(idx):
        for hop in MATES:
            block_copy(idx, hop, False).start()
        block_own(idx).start()

    def blocks_wait(idx):
        block_own(idx).wait()
        for hop in MATES:
            block_copy(idx, hop, True).wait_recv()
            block_copy(idx, hop, False).wait_send()

    def mid_slot(who):
        return d_full.at[:, pl.ds(pl.multiple_of(who * block_rows, block_rows), block_rows), :]

    def mid_copy(hop, incoming):
        slot = mid_slot(member(me_model, hop, incoming))
        return to_member(slot if incoming else d_mid, slot, mid_send.at[hop], mid_recv.at[hop], hop)

    def mid_own():
        return pltpu.make_async_copy(d_mid, mid_slot(me_model), mid_local)

    def columns(peer):
        return d_mid.at[:, :, pl.ds(pl.multiple_of(peer * slice_width, slice_width), slice_width)]

    def slice_copy(hop, incoming):
        peer = (me + hop) % 8
        slot = mid_cols.at[(me + 8 - hop) % 8 if incoming else me]
        return pltpu.make_async_remote_copy(
            src_ref=slot if incoming else columns(peer), dst_ref=slot, send_sem=slice_send.at[hop],
            recv_sem=slice_recv.at[hop], device_id={'fsdp': peer}, device_id_type=MESH)

    def slice_own():
        return pltpu.make_async_copy(columns(me), mid_cols.at[me], slice_local)

    cols_in, cols_all = (h_cols, mid_cols), (h_spread, mid_spread)

    def cols_copy(idx, hop, incoming):
        slot = cols_all[idx].at[:, :, member(me_model, hop, incoming)]
        return to_member(slot if incoming else cols_in[idx], slot, cols_send.at[idx, hop], cols_recv.at[idx, hop], hop)

    def cols_own(idx):
        return pltpu.make_async_copy(cols_in[idx], cols_all[idx].at[:, :, me_model], cols_local.at[idx])

    def finish_ring(ids):
        for idx in ids:
            for way in WAYS:
                landed(idx, way, 6).wait_recv()
                own(idx, way).wait()

    def cols_wait(idx):
        cols_own(idx).wait()
        for hop in MATES:
            cols_copy(idx, hop, True).wait_recv()
            cols_copy(idx, hop, False).wait_send()

    def mix_copy(hop, incoming):
        slot = mix.at[member(me_model, hop, incoming)]
        return to_member(slot if incoming else gains, slot, mix_send.at[hop], mix_recv.at[hop], hop)

    def mix_own():
        return pltpu.make_async_copy(gains, mix.at[me_model], mix_local)

    def fetch(idx):
        return pltpu.make_async_copy((w_out_in, w_qkv_in)[idx], (w_out, w_qkv)[idx], fetch_sem.at[idx])

    def norm_back(parts, saved, gain, base, result, first_row):
        row_sum[...] = jnp.zeros_like(row_sum)

        @functools.partial(tiles, block_rows, GROUP)
        def _(at):
            for seq in range(seqs):
                d_h = sum_blocks(parts, seq, at)
                val = saved[seq, at, :].astype(f32)
                inv_rms = lax.rsqrt(jnp.mean(val * val, axis=-1, keepdims=True) + NORM_EPS)
                scaled = d_h * gain[...]
                slope = jnp.sum(scaled * val, axis=-1, keepdims=True) * (inv_rms * inv_rms * inv_rms) * (1.0 / d_model)
                result[seq, at, :] = (base[seq, at, :].astype(f32) + (scaled * inv_rms - val * slope)).astype(bf16)
                per_row = d_h * val * inv_rms
                row_sum[...] += per_row[:8] + per_row[8:]
        total = jnp.sum(row_sum[...], axis=0, keepdims=True)
        width = gains.shape[1]
        for row in range(d_model // width):
            gains[first_row + row:first_row + row + 1, :] = total[:, row * width:(row + 1) * width]

    def attention_back():
        cos_two, sin_two = wide_tables(cos_ref, sin_ref)
        d_attn[...] = across(d_full[...].reshape(seqs * seq_len, d_model), w_out[...]).astype(bf16)
        for seq in range(seqs):
            for head in range(heads):
                idx = seq * heads + head
                rows = slice(seq * seq_len, (seq + 1) * seq_len)
                d_out = d_attn[rows, head * head_dim:(head + 1) * head_dim]
                weight = prob[idx]
                d_prob = across(d_out, value[idx])
                row_dot = jnp.sum(d_prob * weight, axis=-1, keepdims=True)
                d_scores = (weight * (d_prob - row_dot) * head_dim ** -0.5).astype(bf16)
                d_query = jnp.dot(d_scores, key[idx], preferred_element_type=f32)
                d_key = along(d_scores, query[idx])
                d_value = along(weight.astype(bf16), d_out)
                for place_in, part in enumerate((d_query, d_key)):
                    turned = part * cos_two + pltpu.roll(part, head_dim // 2, 1) * sin_two
                    start = (3 * head + place_in) * head_dim
                    d_qkv[rows, start:start + head_dim] = turned.astype(bf16)
                d_qkv[rows, (3 * head + 2) * head_dim:(3 * head + 3) * head_dim] = d_value.astype(bf16)

        @functools.partial(tiles, d_model, TILE)
        def _(cols):
            dh_attn[:, :, cols] = across(d_qkv[...], w_qkv[cols, :]).reshape(seqs, seq_len, TILE)

    bigs, smalls, products = (act_all, attn_all, gate_all, up_all), (dy_spread, mid_spread, h_spread, attn_spread), (dw_down, dw_out, dw_gate, dw_up)

    def span(tile):
        return pl.ds(tile * TILE, TILE)

    def small_copy(which):
        return pltpu.make_async_copy(smalls[which], small.at[which], small_sem.at[which])

    def big_copy(kind, tile, slot):
        return pltpu.make_async_copy(bigs[kind].at[:, span(tile)], big.at[slot], big_sem.at[slot])

    def product_copy(kind, tile, slot):
        if kind < 2:
            return pltpu.make_async_copy(tall.at[slot], products[kind].at[span(tile), :], product_sem.at[slot])
        return pltpu.make_async_copy(flat.at[slot], products[kind].at[:, span(tile)], product_sem.at[slot])

    def begin(jobs, done=()):
        for slot, job in enumerate(done):
            product_copy(*job, slot).wait()
        for slot, job in enumerate(jobs):
            big_copy(*job, slot).start()

    def multiply(jobs):
        for slot, (kind, tile) in enumerate(jobs):
            big_copy(kind, tile, slot).wait()
            side = small[min(kind, 2)].reshape(big.shape[1], slice_width)
            if kind < 2:
                tall[slot] = along(big[slot], side)
            else:
                flat[slot] = along(side, big[slot])
            product_copy(kind, tile, slot).start()

    def accumulate(step):
        for way in WAYS:
            owner = owner_at(way, step)
            side = small[3, owner, way].reshape(seq_len, slice_width)

            @functools.partial(tiles, qkv_acc.shape[1], TILE)
            def _(cols):
                if step == 0:
                    block = d_qkv[way * seq_len:(way + 1) * seq_len, cols]
                else:
                    block = qkv_all[pl.ds(pl.multiple_of((2 * owner + way) * seq_len, seq_len), seq_len), cols]
                qkv_acc[:, cols] += along(side, block)

    early = {3: ((0, 0), (0, 1)), 5: ((0, 2), (0, 3)), 6: ((1, 0),)}
    late = {1: ((2, 0), (2, 1)), 2: ((2, 2),), 3: ((2, 3),), 4: ((3, 0), (3, 1)), 5: ((3, 2),), 6: ((3, 3),)}
    small_copy(0).start()
    small_copy(3).start()
    qkv_acc[...] = jnp.zeros_like(qkv_acc)
    start_ring((0, 1))
    blocks_start(0)
    blocks_start(1)
    for idx in range(4):
        for way in WAYS:
            own(idx, way).start()
    for idx in WAYS:
        fetch(idx).start()
    for hop in MATES:
        cols_copy(0, hop, False).start()
    cols_own(0).start()
    for step in LATER:
        forward((0, 1), step)
        if step == 2:
            blocks_wait(0)
            norm_back(dh_blocks, mid_ref, gain_mlp, dy_ref, d_mid, 16)
        if step == 3:
            for hop in MATES:
                mid_copy(hop, False).start()
            mid_own().start()
            slice_own().start()
            for hop in OTHERS:
                slice_copy(hop, False).start()
        if step == 5:
            blocks_wait(1)

            @functools.partial(tiles, block_rows, GROUP)
            def _(at):
                for seq in range(seqs):
                    y_ref[seq, at, :] = (mid_ref[seq, at, :].astype(f32) + sum_blocks(y_blocks, seq, at)).astype(bf16)
    start_ring((2, 3))
    past = ()
    for step in LATER:
        if step == 3:
            small_copy(0).wait()
            finish_ring((0, 1))
        if step == 5:
            cols_wait(0)
            small_copy(2).start()
        if step == 6:
            cols_wait(1)
            small_copy(1).start()
        if step in early:
            begin(early[step], past)
            past = early[step]
        forward((2, 3), step)
        if step == 6:
            small_copy(1).wait()
        if step in early:
            multiply(early[step])
        if step == 1:
            mid_own().wait()
            for hop in MATES:
                mid_copy(hop, True).wait_recv()
                mid_copy(hop, False).wait_send()
            for idx in WAYS:
                fetch(idx).wait()
            attention_back()
        if step == 2:
            blocks_start(2)
            slice_own().wait()
            for hop in OTHERS:
                slice_copy(hop, True).wait_recv()
                slice_copy(hop, False).wait_send()
            for hop in MATES:
                cols_copy(1, hop, False).start()
            cols_own(1).start()
        if step == 4:
            blocks_wait(2)
            norm_back(attn_blocks, x_ref, gain_attn, d_mid, dx_ref, 0)
        if step == 5:
            mix_own().start()
            for hop in MATES:
                mix_copy(hop, False).start()
    start_ring((4,))
    mix_own().wait()
    for hop in MATES:
        mix_copy(hop, True).wait_recv()
        mix_copy(hop, False).wait_send()
    start_ring((5,))
    for idx in (4, 5):
        for way in WAYS:
            own(idx, way).start()
    small_copy(3).wait()
    accumulate(0)
    for step in LATER:
        if step == 1:
            small_copy(2).wait()
            finish_ring((2, 3))
        if step in late:
            begin(late[step], past)
            past = late[step]
        forward((4, 5), step)
        if step in late:
            multiply(late[step])
        accumulate(step)
    begin((), past)
    finish_ring((4, 5))
    accumulate(7)
    result = pltpu.make_async_copy(qkv_acc, dw_qkv, fetch_sem.at[0])
    result.start()
    for idx in range(6):
        for way in WAYS:
            for step in STEPS:
                send(idx, way, step).wait_send()
    result.wait()


def ring_back(collective_id, *args):
    act, attn, d_gate, d_up, dh_part, y_part, h_cols, w_out, w_qkv, mid = args[:10]
    tokens = act.shape[0]
    seqs, seq_len, d_model = dh_part.shape
    bf16, f32 = jnp.bfloat16, jnp.float32
    qkv_cols = w_qkv.shape[1]
    sent = 7 * (3 * act.size + attn.size + tokens * qkv_cols) * 2
    vmem = pl.BlockSpec(memory_space=pltpu.VMEM)
    hbm = pl.BlockSpec(memory_space=pl.ANY)
    shape = jax.ShapeDtypeStruct
    gain_shape = (32, d_model // 16)
    side = d_model // 8
    spread = shape(h_cols.shape[:2] + (4,) + h_cols.shape[2:], bf16)
    blocks = pltpu.VMEM((4,) + mid.shape, f32)
    return pl.pallas_call(
        back_kernel,
        out_shape=[shape((side, qkv_cols), f32), shape((act.shape[1], side), f32), shape((attn.shape[1], side), f32), shape((side, act.shape[1]), f32),
                   shape((side, act.shape[1]), f32)]
        + [shape((8 * tokens, array.shape[1]), bf16) for array in (act, attn, d_gate, d_up)]
        + [shape((8, 4) + gain_shape, f32), shape((4,) + gain_shape, f32),
           shape(h_cols.shape, bf16), spread, spread, shape(mid.shape, bf16), shape(mid.shape, bf16)],
        in_specs=[hbm] * 9 + [vmem] * (len(args) - 11) + [hbm] * 2,
        out_specs=[hbm] * 14 + [vmem] * 2,
        scratch_shapes=[pltpu.VMEM(w_out.shape, bf16), pltpu.VMEM(w_qkv.shape, bf16), pltpu.VMEM(mid.shape, bf16),
                        pltpu.VMEM(dh_part.shape, bf16), pltpu.VMEM((tokens, w_out.shape[0]), bf16),
                        pltpu.VMEM((tokens, qkv_cols), bf16), pltpu.VMEM(dh_part.shape, f32), pltpu.VMEM(gain_shape, f32),
                        pltpu.VMEM((8, d_model), f32), blocks, blocks, blocks,
                        DMA((6, 2, 7)), DMA((6, 2, 7)), DMA((6, 2)), TRIO_MATES, TRIO_MATES, TRIO,
                        MATE_SEMS, MATE_SEMS, DMA, OTHER_SEMS, OTHER_SEMS, DMA, PAIR_MATES, PAIR_MATES, PAIR,
                        MATE_SEMS, MATE_SEMS, DMA, PAIR,
                        pltpu.VMEM((4,) + spread.shape, bf16), pltpu.VMEM((2, 8 * tokens, TILE), bf16),
                        pltpu.VMEM((2, TILE, side), f32), pltpu.VMEM((2, side, TILE), f32), pltpu.VMEM((8 * tokens, qkv_cols), bf16),
                        pltpu.VMEM((side, qkv_cols), f32), MATE_SEMS, PAIR, PAIR],
        compiler_params=pltpu.CompilerParams(collective_id=collective_id, has_side_effects=True,
                                             vmem_limit_bytes=60 * 1024 * 1024),
        cost_estimate=pl.CostEstimate(flops=sent * 3000, bytes_accessed=2 * sent, transcendentals=0),
        name=f'ring_back_{collective_id}',
    )(*args)


def solution(mesh):
    act_spec = P('fsdp', 'model', None)
    rows_spec = P('fsdp', 'model')
    cols_spec = P('model', 'fsdp')
    f32 = jnp.float32

    def device_fn(x_loc, dy_loc, gain_attn, gain_mlp, wqkv_sh, wout_sh, wgate_sh, wup_sh, wdown_sh, rope_cos, rope_sin):
        gain_a, gain_m = gain_attn.reshape(1, -1), gain_mlp.reshape(1, -1)
        rope_cos_t, rope_sin_t = rope_cos.T, rope_sin.T
        (w_qkv, w_out, _, _, h_mlp_cols, h_attn_cols, dy_cols, query, key_rot, value, prob, attn_flat, gated_act, d_gate, d_up,
         mlp_part, dh_part, mid) = ring_front(
            1, wqkv_sh, wout_sh, wdown_sh, wgate_sh, wup_sh, x_loc, dy_loc, gain_a, gain_m, rope_cos_t, rope_sin_t)
        whole = (x_loc.shape[0], rope_cos.shape[0], x_loc.shape[2])
        (dw_qkv, dw_down, dw_out, dw_gate, dw_up, _, _, _, _, gains_all, _, _, _, _, y_loc, dx_loc) = ring_back(
            2, gated_act, attn_flat, d_gate, d_up, dh_part.reshape(whole), mlp_part.reshape(whole), h_mlp_cols, w_out, w_qkv,
            mid, x_loc, dy_loc, gain_m, gain_a, query, key_rot, value, prob, rope_cos_t, rope_sin_t, dy_cols, h_attn_cols)
        gain_grads = [part.reshape(-1) for part in jnp.split(jnp.sum(gains_all, axis=(0, 1)), 2)]
        return (y_loc, dx_loc, gain_grads[0], gain_grads[1], dw_qkv, dw_out, dw_gate, dw_up, dw_down)

    in_specs = (act_spec, act_spec, P(), P(), rows_spec, cols_spec, rows_spec, rows_spec, cols_spec, P(), P())
    out_specs = (act_spec, act_spec, P(), P(), rows_spec, cols_spec, rows_spec, rows_spec, cols_spec)
    return jax.shard_map(device_fn, mesh=mesh, in_specs=in_specs, out_specs=out_specs, check_vma=False)
```
